32 devices in a mesh: gy: 8 (over z, y), gz: 4 (over x, core).
Axes of the slice: x: 2, y: 2, z: 4, core: 2. Of those that a mesh axis runs over, the one named last changes fastest.
Arguments:
- wavefunction: float32 [2, 8, 1024, 1024], P(None, None, 'gy', 'gz'), may hold values from -6 to 6
- absorber: float32 [8, 1024, 1024], P(None, 'gy', 'gz'), may hold values from 0.05 to 1.5
- row_inverse: float32 [2, 1024, 128], P(None, 'gy'), may hold values from -1 to 1
- column_inverse: float32 [2, 1024, 256], replicated, may hold values from -1 to 1
- link_terms: float32 [2, 2, 2], replicated, may hold values from 0.65 to 0.7
- shell_blocks: int32 [4, 8, 56], P('gz'), may hold values from 0 to 63, as said below
- owner_map: int32 [4, 8, 56, 1], P('gz'), may hold values from 0 to 7; in each aligned block of 56 rows (0 to 55, 56 to 111, ..., all dimensions but the last counted through in order) at most 14 rows name the same one
- volkov_phase: float32 [128, 128], replicated, may hold values from -3.140625 to 3.140625
Outputs:
- damped: float32 [2, 8, 1024, 1024], P(None, None, 'gy', 'gz')
- spectrum: float32 [2, 64, 512, 128], P(None, 'gy', 'gz')
The draws below stay inside these ranges and needn't reach their ends.
Inputs may be any that keep to these rules, and one draw needn't show every extreme that they name: `shell_blocks`: the ids listed for one device are distinct. `owner_map`: at most 14 of one device's listed blocks name the same owner.
All inputs are finite; a program needn't handle non-finite values.
Results may differ from the reference program's by a relative error of at most 0.0003.
Values sent between devices are 32-bit elements; how exact they have to be, the bound alone decides.
No kernel may reach another device: no remote copies, remote signals or barrier semaphores. Data moves between devices by JAX's collectives and lax.ppermute only.
A program may use at most 64 MiB of HBM per device.

```python
import math
import jax
import jax.numpy as jnp
import numpy as np
from jax import lax

NX = 8
CY = 128
CZ = 256
BY = 2
KY = 128
KZ = 128
BPD = 64
SHELL_DEV = 56
CAP = 14
NY = 1024
NZ = 1024
N_GY = 8
N_GZ = 4


def draw_inverse(base_key, groups, length):
    subkeys = jax.random.split(base_key, 7)
    modulus = jax.random.uniform(subkeys[0], (groups, length), jnp.float32, 0.4, 0.8)
    phases = jax.random.uniform(subkeys[1], (groups, length), jnp.float32, -jnp.pi, jnp.pi)
    corner_phase = jax.random.uniform(subkeys[3], (groups, 2), jnp.float32, -jnp.pi, jnp.pi)
    edge_modulus = jax.random.uniform(subkeys[4], (groups, 2), jnp.float32, 0.004, 0.01)
    edge_phase = jax.random.uniform(subkeys[6], (groups, 2), jnp.float32, -jnp.pi, jnp.pi)
    spread = jax.random.uniform(subkeys[2], (2, groups, length, length), jnp.float32, -0.1, 0.1)
    corner_modulus = jax.random.uniform(subkeys[5], (groups, 2), jnp.float32, 0.95, 0.99)
    identity = jnp.eye(length, dtype=jnp.float32)
    off_diagonal = spread * (1.0 - identity)
    real_part = off_diagonal[0] + (modulus * jnp.cos(phases))[:, :, None] * identity
    imag_part = off_diagonal[1] + (modulus * jnp.sin(phases))[:, :, None] * identity
    places = jnp.arange(length, dtype=jnp.int32)
    first = places == 0
    last = places == length - 1
    lower_corner = (last[:, None] & first[None, :])[None]
    upper_corner = (first[:, None] & last[None, :])[None]
    head_diagonal = (first[:, None] & first[None, :])[None]
    tail_diagonal = (last[:, None] & last[None, :])[None]
    corner_real = corner_modulus * jnp.cos(corner_phase)
    corner_imag = corner_modulus * jnp.sin(corner_phase)
    edge_real = edge_modulus * jnp.cos(edge_phase)
    edge_imag = edge_modulus * jnp.sin(edge_phase)
    real_part = jnp.where(lower_corner, corner_real[:, 0, None, None], real_part)
    real_part = jnp.where(upper_corner, corner_real[:, 1, None, None], real_part)
    real_part = jnp.where(head_diagonal, edge_real[:, 0, None, None], real_part)
    real_part = jnp.where(tail_diagonal, edge_real[:, 1, None, None], real_part)
    imag_part = jnp.where(lower_corner, corner_imag[:, 0, None, None], imag_part)
    imag_part = jnp.where(upper_corner, corner_imag[:, 1, None, None], imag_part)
    imag_part = jnp.where(head_diagonal, edge_imag[:, 0, None, None], imag_part)
    imag_part = jnp.where(tail_diagonal, edge_imag[:, 1, None, None], imag_part)
    return jnp.stack([real_part, imag_part]).reshape(2, groups * length, length)


def draw_row_inverse(key, part):
    return draw_inverse(jax.random.fold_in(key, 11), NY // CY, CY)


def draw_column_inverse(key, part):
    return draw_inverse(jax.random.fold_in(key, 23), NZ // CZ, CZ)


def draw_shell_blocks(key, part):
    devices = NZ // CZ * (NY // CY)
    subkeys = jax.random.split(jax.random.fold_in(key, 31), devices)
    chosen = jax.vmap(lambda member_key: jax.random.permutation(member_key, BPD)[:SHELL_DEV])(subkeys)
    return chosen.reshape(NZ // CZ, NY // CY, SHELL_DEV).astype(jnp.int32)


def steps_of(stream_key, dims, cuts, smallest, largest):
    loudness = 1.0
    for dim, blocks in cuts:
        heights = jax.random.uniform(jax.random.fold_in(jax.random.fold_in(stream_key, 6), dim), (blocks,), jnp.float32, smallest / len(cuts), largest / len(cuts))
        loudness = loudness * jnp.repeat(jnp.exp(heights), dims[dim] // blocks).reshape((-1,) + (1,) * (len(dims) - 1 - dim))
    return loudness


def deal_out(stream_key, own, number, rows, amount, top, most, lean):
    ranking = jax.random.permutation(stream_key, amount)
    packed, common = portions_of(amount, rows * top, most, lean, True), portions_of(amount, rows * top, most, lean, False)
    places = jnp.arange(amount)

    def named(sizes, rotation):
        used = int((sizes > 0).sum())
        fixed = max(1, used // 4)
        moved = fixed + (places - fixed + rotation * (used - fixed)) % max(1, amount - fixed)
        return jnp.zeros((amount,), jnp.int32).at[ranking[jnp.where(places < fixed, places, moved)]].set(jnp.asarray(sizes, jnp.int32))

    sizes = jnp.where(number % 4 == 0, named(packed, number // 4), named(common, number - number // 4 - 1))
    mixed = jax.random.permutation(jax.random.fold_in(own, 3), amount)
    source_of, sink = mixed[0:amount // 2 * 2:2], mixed[1:amount // 2 * 2:2]
    room = jnp.minimum(sizes[source_of] - 1, most - sizes[sink]) // 2
    room = jnp.where((source_of == ranking[0]) | (sink == ranking[0]) | (sizes[sink] == 0), 0, jnp.maximum(room, 0))
    moved = jax.random.randint(jax.random.fold_in(own, 4), (amount // 2,), 0, 1 << 20) % (room + 1)
    sizes = sizes.at[source_of].add(-moved).at[sink].add(moved)
    members = jnp.searchsorted(jnp.cumsum(sizes), jnp.arange(rows * top), side="right").astype(jnp.int32)
    table = members.reshape(top, rows).T
    table = table[jax.random.permutation(jax.random.fold_in(own, 1), rows)]
    rotation = jax.random.randint(jax.random.fold_in(own, 2), (rows, 1), 0, top)
    return jnp.take_along_axis(table, (jnp.arange(top)[None, :] + rotation) % top, axis=1)


def portions_of(amount, total, reach, lean, full):
    portions = [(1 << 20) // math.isqrt(grade ** lean) + 1 for grade in range(1, amount + 1)]
    largest = reach if full else min(reach, max(-(-total // amount), total * portions[0] // sum(portions)))
    least = 1 if total - largest >= amount - 1 else 0
    holding, rest = [largest] + [least] * (amount - 1), total - largest - least * (amount - 1)
    while rest > 0:
        candidates = [i for i in range(1, amount) if holding[i] < largest] or [i for i in range(1, amount) if holding[i] < reach]
        pool, remaining = sum([portions[i] for i in candidates]), rest
        for i in candidates:
            more = min(reach - holding[i], max(1, remaining * portions[i] // pool), rest)
            holding[i] = holding[i] + more
            rest = rest - more
    return np.array(holding)


def centred(own_key, extent, scale, reach, shards=(), held_as=jnp.bfloat16):
    entries = jax.random.normal(own_key, extent, jnp.float32) * scale
    if len(shards) > 0:
        entries = steps_of(own_key, extent, shards, -0.22, 0.18) * entries
    return jnp.clip(entries, min=-reach, max=reach).astype(held_as)


def setup_inputs(seed: int = 0) -> dict:
    splits = jax.random.split(jax.random.key(seed), 9)
    wavefunction = centred(splits[0], (2, NX, NY, NZ), 1.0, 6.0, ((2, 8), (3, 4)), jnp.float32)
    absorber = jnp.clip(jnp.exp(math.log(1.5) - 3.4011974 * jax.random.uniform(splits[1], (NX, NY, NZ), jnp.float32) ** steps_of(splits[1], (NX, NY, NZ), ((1, 8), (2, 4)), -0.2, 0.2)), 0.05, 1.5)
    row_inverse = draw_row_inverse(jax.random.fold_in(splits[8], 71), 0)
    column_inverse = draw_column_inverse(jax.random.fold_in(splits[8], 71), 0)
    link_terms = jnp.clip(jax.random.uniform(splits[4], (2, 2, 2), jnp.float32, 0.65, 0.7), 0.65, 0.7)
    shell_blocks = draw_shell_blocks(jax.random.fold_in(splits[8], 71), 0)
    owner_map_keys = jax.random.split(jax.random.fold_in(splits[6], 1), N_GZ * N_GY * SHELL_DEV // SHELL_DEV)
    owner_map_turns = jax.random.permutation(jax.random.fold_in(splits[6], 3), N_GZ * N_GY * SHELL_DEV // SHELL_DEV)
    owner_map = jax.vmap(lambda own, number: deal_out(jax.random.fold_in(splits[6], 2), own, number, SHELL_DEV, N_GY, 1, CAP, 2))(owner_map_keys, owner_map_turns).reshape((N_GZ, N_GY, SHELL_DEV, 1))
    volkov_phase = jnp.clip(jax.random.uniform(splits[7], (KY, KZ), jnp.float32, -3.140625, 3.140625), -3.140625, 3.140625)
    return {"wavefunction": wavefunction, "absorber": absorber, "row_inverse": row_inverse, "column_inverse": column_inverse, "link_terms": link_terms, "shell_blocks": shell_blocks, "owner_map": owner_map, "volkov_phase": volkov_phase}


precise = lax.Precision.HIGHEST

def complex_mul(former, latter):
    return (former[0] * latter[0] - former[1] * latter[1], former[0] * latter[1] + former[1] * latter[0])

def complex_div(former, latter):
    modulus = latter[0] * latter[0] + latter[1] * latter[1]
    return ((former[0] * latter[0] + former[1] * latter[1]) / modulus, (former[1] * latter[0] - former[0] * latter[1]) / modulus)

def complex_add(former, latter):
    return (former[0] + latter[0], former[1] + latter[1])

def complex_sub(former, latter):
    return (former[0] - latter[0], former[1] - latter[1])

def complex_einsum(pattern, former, latter):
    real_part = jnp.einsum(pattern, former[0], latter[0], precision=precise) - jnp.einsum(pattern, former[1], latter[1], precision=precise)
    imag_part = jnp.einsum(pattern, former[0], latter[1], precision=precise) + jnp.einsum(pattern, former[1], latter[0], precision=precise)
    return (real_part, imag_part)

def phase_table(positions, count):
    wavenum = jnp.arange(count, dtype=jnp.int32)
    turns = positions[..., None] * wavenum % count
    parity = (positions[..., None] % 2).astype(jnp.float32)
    phases = 2.0 * math.pi / count * turns.astype(jnp.float32) - math.pi * parity
    return (jnp.cos(phases), -jnp.sin(phases))

def edge_terms(inverse, prev_link, next_link):
    length = inverse[0].shape[-1]
    left_spike = complex_mul(prev_link, (inverse[0][..., 0], inverse[1][..., 0]))
    right_spike = complex_mul(next_link, (inverse[0][..., length - 1], inverse[1][..., length - 1]))
    edges = ((left_spike[0][..., 0], left_spike[1][..., 0]), (left_spike[0][..., length - 1], left_spike[1][..., length - 1]), (right_spike[0][..., 0], right_spike[1][..., 0]), (right_spike[0][..., length - 1], right_spike[1][..., length - 1]))
    return (left_spike, right_spike, edges)

def chain_local(edges, head_part, tail_part):
    unity = (jnp.ones((), jnp.float32), jnp.zeros((), jnp.float32))

    def forward(carry, inputs):
        coupling, carried = carry
        spikes, head_now, tail_now = inputs
        pivot_value = complex_sub(unity, complex_mul(spikes[0], coupling))
        gain_term = complex_div(spikes[1], pivot_value)
        coupling_next = complex_add(spikes[3], complex_mul(gain_term, complex_mul(spikes[2], coupling)))
        carried_next = complex_add(complex_mul(gain_term, carried), complex_add(tail_now, complex_mul(complex_mul(gain_term, coupling), head_now)))
        return ((coupling_next, carried_next), (coupling, carried, pivot_value))
    zero_lines = (jnp.zeros_like(head_part[0][0]), jnp.zeros_like(head_part[0][0]))
    initial = ((jnp.zeros((), jnp.float32), jnp.zeros((), jnp.float32)), zero_lines)
    final_state, (coupling_prev, carried_prev, pivots) = lax.scan(forward, initial, (edges, head_part, tail_part))

    def backward(head_next, inputs):
        spikes, head_now, carried_now, coupling_now, pivot_value = inputs
        offset = complex_div(complex_add(head_now, complex_mul(spikes[0], carried_now)), pivot_value)
        factor = complex_div(spikes[2], pivot_value)
        head_value = complex_add(offset, complex_mul(factor, head_next))
        left_value = complex_add(carried_now, complex_mul(coupling_now, head_value))
        return (head_value, (left_value, head_next))
    final_head, (left_values, right_values) = lax.scan(backward, zero_lines, (edges, head_part, carried_prev, coupling_prev, pivots), reverse=True)
    return (left_values, right_values)

def reference(wavefunction, absorber, row_inverse, column_inverse, link_terms, shell_blocks, owner_map, volkov_phase):
    row_count = NY // CY
    column_count = NZ // CZ
    row_groups = (row_inverse[0].reshape(row_count, CY, CY), row_inverse[1].reshape(row_count, CY, CY))
    column_groups = (column_inverse[0].reshape(column_count, CZ, CZ), column_inverse[1].reshape(column_count, CZ, CZ))
    row_left, row_right, row_edges = edge_terms(row_groups, (link_terms[0, 0, 0], link_terms[0, 0, 1]), (link_terms[0, 1, 0], link_terms[0, 1, 1]))
    column_left, column_right, column_edges = edge_terms(column_groups, (link_terms[1, 0, 0], link_terms[1, 0, 1]), (link_terms[1, 1, 0], link_terms[1, 1, 1]))
    weight_norm = 1.0 / math.sqrt(CY * CZ)
    volkov = (jnp.cos(volkov_phase), jnp.sin(volkov_phase))

    def plane_step(inputs):
        field, damping = inputs
        blocks = (field[0].reshape(row_count, CY, NZ), field[1].reshape(row_count, CY, NZ))
        solved = complex_einsum('jab,jbz->jaz', row_groups, blocks)
        head_part = (solved[0][:, 0], solved[1][:, 0])
        tail_part = (solved[0][:, CY - 1], solved[1][:, CY - 1])
        left_value, right_value = chain_local(row_edges, head_part, tail_part)
        lifted = complex_add(solved, complex_add(complex_mul((row_left[0][:, :, None], row_left[1][:, :, None]), (left_value[0][:, None, :], left_value[1][:, None, :])), complex_mul((row_right[0][:, :, None], row_right[1][:, :, None]), (right_value[0][:, None, :], right_value[1][:, None, :]))))
        field_y = (lifted[0].reshape(NY, column_count, CZ), lifted[1].reshape(NY, column_count, CZ))
        solved_z = complex_einsum('jab,yjb->yja', column_groups, field_y)
        head_z = (solved_z[0][:, :, 0].T, solved_z[1][:, :, 0].T)
        tail_z = (solved_z[0][:, :, CZ - 1].T, solved_z[1][:, :, CZ - 1].T)
        left_z, right_z = chain_local(column_edges, head_z, tail_z)
        lifted_z = complex_add(solved_z, complex_add(complex_mul((column_left[0][None], column_left[1][None]), (left_z[0].T[:, :, None], left_z[1].T[:, :, None])), complex_mul((column_right[0][None], column_right[1][None]), (right_z[0].T[:, :, None], right_z[1].T[:, :, None]))))
        field_z = (lifted_z[0].reshape(NY, NZ), lifted_z[1].reshape(NY, NZ))
        kept = jnp.exp(-damping)
        damped = (field_z[0] * kept, field_z[1] * kept)
        lost_stack = jnp.stack([field_z[0] - damped[0], field_z[1] - damped[1]])

        def group_spectrum(position):
            pieces = lax.dynamic_slice_in_dim(lost_stack, (position * CZ).astype(jnp.int32), CZ, axis=2)
            blocks_all = pieces.reshape(2, row_count, BPD, BY, CZ)
            chosen_ids = shell_blocks[position]
            picked = blocks_all[:, jnp.arange(row_count, dtype=jnp.int32)[:, None], chosen_ids]
            z_table = phase_table(position * CZ + jnp.arange(CZ, dtype=jnp.int32), KZ)
            moved = complex_einsum('gmbz,zq->gmbq', (picked[0], picked[1]), z_table)
            rows_y = jnp.arange(row_count, dtype=jnp.int32)[:, None, None] * CY + chosen_ids[:, :, None] * BY + jnp.arange(BY, dtype=jnp.int32)[None, None, :]
            y_table = phase_table(rows_y, KY)
            terms = complex_einsum('gmbk,gmbq->gmkq', y_table, moved)
            targets = owner_map[position, :, :, 0].reshape(-1)
            summed = tuple((jax.ops.segment_sum(member.reshape(row_count * SHELL_DEV, KY, KZ), targets, num_segments=row_count) for member in terms))
            phased = complex_mul(volkov, summed)
            return jnp.stack([phased[0], phased[1]]) * weight_norm
        spectra = lax.map(group_spectrum, jnp.arange(column_count, dtype=jnp.int32))
        return (jnp.stack([damped[0], damped[1]]), spectra)
    planes_out, spectra = lax.map(plane_step, (jnp.moveaxis(wavefunction, 1, 0), absorber))
    damped_all = jnp.moveaxis(planes_out, 0, 1)
    spectrum = spectra.transpose(2, 3, 0, 1, 4, 5).reshape(2, row_count * NX, column_count * KY, KZ)
    return (damped_all, spectrum)
```

```python
import math

import jax
import jax.numpy as jnp
import numpy as np
from jax import lax
from jax.experimental import pallas as pl
from jax.experimental.pallas import tpu as pltpu
from jax.sharding import PartitionSpec as P

BY = 2
KY = 128
KZ = 128
EDGE = 8
CHUNKS = 1

f32 = jnp.float32
bf16 = jnp.bfloat16
NN = (((1,), (0,)), ((), ()))
NT = (((1,), (1,)), ((), ()))
TN = (((0,), (0,)), ((), ()))


def mm(a, b, dims=NN):
    return lax.dot_general(a, b, dims, preferred_element_type=f32)


def split(a):
    hi = a.astype(bf16)
    return hi, (a - hi.astype(f32)).astype(bf16)


def mm3(a, b, dims=NN):
    return mm(a[0], b[0], dims) + mm(a[0], b[1], dims) + mm(a[1], b[0], dims)


def cmul(a, b):
    return (a[0] * b[0] - a[1] * b[1], a[0] * b[1] + a[1] * b[0])


def cdiv(a, b):
    modulus = b[0] * b[0] + b[1] * b[1]
    return ((a[0] * b[0] + a[1] * b[1]) / modulus, (a[1] * b[0] - a[0] * b[1]) / modulus)


def cadd(a, b):
    return (a[0] + b[0], a[1] + b[1])


def put(hi_ref, lo_ref, rows, cols, value):
    hi, lo = split(value)
    hi_ref[rows, cols] = hi
    lo_ref[rows, cols] = lo


def spikes_of(transposed, link, sweep):
    last = transposed[0].shape[0] - 1
    left = cmul(
        (link[sweep, 0, 0], link[sweep, 0, 1]), (transposed[0][0:1], transposed[1][0:1])
    )
    right = cmul(
        (link[sweep, 1, 0], link[sweep, 1, 1]),
        (transposed[0][last : last + 1], transposed[1][last : last + 1]),
    )
    return left, right


def edge_rows(left, right, lanes):
    last = left[0].shape[1] - 1
    rows = []
    for spike in (left, right):
        for at in (0, last):
            for part in spike:
                rows.append(jnp.broadcast_to(part[:, at : at + 1], (1, lanes)))
    return rows


def solve_rows_kernel(link, w, y, thi, tlo, pay, spk, yh, yl, ps):
    x = pl.program_id(0)
    planes = pl.num_programs(0)
    n = y.shape[1]
    width = w.shape[3]

    @pl.when(x == 0)
    def _():
        yr = y[0]
        yi = y[1]
        put(yh, yl, slice(0, n), slice(0, n), yr)
        put(yh, yl, slice(0, n), slice(n, 2 * n), -yi)
        put(yh, yl, slice(n, 2 * n), slice(0, n), yi)
        put(yh, yl, slice(n, 2 * n), slice(n, 2 * n), yr)
        left, right = spikes_of((yr.T, yi.T), link, 0)
        for at, row in enumerate((left[0], left[1], right[0], right[1])):
            spk[at : at + 1, :] = row
        spk[4:8, :] = jnp.zeros((4, n), f32)
        count = ps.shape[0] - EDGE
        for at, row in enumerate(edge_rows(left, right, width)):
            ps[count + at : count + at + 1, :] = row

    wx = split(w[...].reshape(2 * n, width))
    t = mm3((yh[...], yl[...]), wx)
    hi, lo = split(t)
    thi[0, :, 0:width] = hi[0:n]
    thi[0, :, width : 2 * width] = hi[n : 2 * n]
    tlo[0, :, 0:width] = lo[0:n]
    tlo[0, :, width : 2 * width] = lo[n : 2 * n]
    nx = (ps.shape[0] - EDGE) // 4
    for at, row in enumerate((0, n, n - 1, 2 * n - 1)):
        ps[pl.ds(at * nx + x, 1), :] = t[row : row + 1]

    @pl.when(x == planes - 1)
    def _():
        value = ps[...]
        for g in range(pay.shape[0]):
            pay[g] = value


def solve_columns_kernel(link, thi, tlo, col, s, base, zh, zl, zsp, zed, zv, eh, el, sem):
    x = pl.program_id(0)
    wz = zv.shape[1]
    nx = base.shape[0] // 4

    @pl.when(x == 0)
    def _():
        rank = lax.axis_index("gz")
        copy = pltpu.make_async_copy(col.at[:, pl.ds(rank * wz, wz), :], zv, sem)
        copy.start()
        copy.wait()
        zr = zv[0]
        zi = zv[1]
        rt = zr.T
        it = zi.T
        put(zh, zl, slice(0, wz), slice(0, wz), rt)
        put(zh, zl, slice(0, wz), slice(wz, 2 * wz), it)
        put(zh, zl, slice(wz, 2 * wz), slice(0, wz), -it)
        put(zh, zl, slice(wz, 2 * wz), slice(wz, 2 * wz), rt)
        left, right = spikes_of((rt, it), link, 1)
        for at, spike in enumerate((left, right)):
            zsp[2 * at : 2 * at + 1, 0:wz] = spike[0]
            zsp[2 * at : 2 * at + 1, wz : 2 * wz] = spike[1]
            zsp[2 * at + 1 : 2 * at + 2, 0:wz] = -spike[1]
            zsp[2 * at + 1 : 2 * at + 2, wz : 2 * wz] = spike[0]
        zsp[4:8, :] = jnp.zeros((4, 2 * wz), f32)
        for at, row in enumerate(edge_rows(left, right, zed.shape[1])):
            zed[at : at + 1, :] = row
        zero = jnp.zeros((12, wz), f32)
        real = jnp.concatenate([zr[0:1], zi[0:1], zr[wz - 1 : wz], zi[wz - 1 : wz], zero], 0)
        imag = jnp.concatenate([-zi[0:1], zr[0:1], -zi[wz - 1 : wz], zr[wz - 1 : wz], zero], 0)
        put(eh, el, slice(0, 16), slice(0, wz), real)
        put(eh, el, slice(0, 16), slice(wz, 2 * wz), imag)

    t = (thi[0], tlo[0])
    s[0] = mm3(t, (zh[...], zl[...]))
    edges = mm3((eh[...], el[...]), t, NT)
    for at in range(4):
        base[pl.ds(at * nx + x, 1), :] = edges[at : at + 1]


def chain(gathered, nx, own, keep):
    groups = gathered.shape[0]
    lanes = gathered.shape[2]
    zero = jnp.zeros((nx, lanes), f32)

    def read(j):
        block = gathered[j]
        rows = [block[at * nx : (at + 1) * nx] for at in range(4)]
        edges = [
            jnp.broadcast_to(block[4 * nx + at : 4 * nx + at + 1], (nx, lanes))
            for at in range(EDGE)
        ]
        head, tail = (rows[0], rows[1]), (rows[2], rows[3])
        return head, tail, [(edges[2 * at], edges[2 * at + 1]) for at in range(4)]

    def forward(j, carry):
        coupling, carried = (carry[0], carry[1]), (carry[2], carry[3])
        head, tail, (lead_left, tail_left, lead_right, tail_right) = read(j)
        product = cmul(lead_left, coupling)
        pivot = (1.0 - product[0], -product[1])
        gain = cdiv(tail_left, pivot)
        for at, value in enumerate(coupling + carried + pivot):
            keep[j, at * nx : (at + 1) * nx, :] = value
        coupling_next = cadd(tail_right, cmul(gain, cmul(lead_right, coupling)))
        carried_next = cadd(
            cmul(gain, carried), cadd(tail, cmul(cmul(gain, coupling), head))
        )
        return coupling_next + carried_next

    def solved(j, head_next):
        head, _, (lead_left, _, lead_right, _) = read(j)
        kept = keep[j]
        values = [kept[at * nx : (at + 1) * nx] for at in range(6)]
        coupling, carried, pivot = (
            (values[0], values[1]),
            (values[2], values[3]),
            (values[4], values[5]),
        )
        offset = cdiv(cadd(head, cmul(lead_left, carried)), pivot)
        factor = cdiv(lead_right, pivot)
        value = cadd(offset, cmul(factor, head_next))
        return value, cadd(carried, cmul(coupling, value))

    lax.fori_loop(0, groups, forward, (zero, zero, zero, zero))
    following = lax.fori_loop(
        0,
        groups - 1 - own,
        lambda lap, head_next: solved(groups - 1 - lap, head_next)[0],
        (zero, zero),
    )
    return solved(own, following)[1], following


def row_chain_kernel(gathered, zh, zl, base, zed, spk, lam, pay, keep):
    nx = base.shape[0] // 4
    left, right = chain(gathered, nx, lax.axis_index("gy"), keep)
    stacked = jnp.concatenate(
        [jnp.concatenate([left[0], left[1]], 1), jnp.concatenate([right[0], right[1]], 1)], 0
    )
    moved = mm3(split(stacked), (zh[...], zl[...]))
    lam[...] = moved
    wz = moved.shape[1] // 2
    spikes = (
        (spk[0:1, :], spk[1:2, :]),
        (spk[2:3, :], spk[3:4, :]),
    )
    for at, z in enumerate((0, wz - 1)):
        value = (base[2 * at * nx : (2 * at + 1) * nx, :], base[(2 * at + 1) * nx : (2 * at + 2) * nx, :])
        for side in range(2):
            rows = slice(side * nx, (side + 1) * nx)
            factor = (moved[rows, z : z + 1], moved[rows, wz + z : wz + z + 1])
            value = cadd(value, cmul(factor, spikes[side]))
        pay[2 * at * nx : (2 * at + 1) * nx, :] = value[0]
        pay[(2 * at + 1) * nx : (2 * at + 2) * nx, :] = value[1]
    pay[4 * nx : 4 * nx + EDGE, :] = zed[...]


def route_kernel(listed, owners, place, *, tail):
    me = lax.axis_index("gy")
    groups, count = owners.shape
    rows = place.shape[1] // groups
    ny = place.shape[2] // 2
    ids = listed[pl.ds(me, 1), :]
    own = owners[pl.ds(me, 1), :]
    hot = (lax.broadcasted_iota(jnp.int32, (groups, count), 0) == own).astype(f32)
    upper = (
        lax.broadcasted_iota(jnp.int32, (count, count), 0)
        < lax.broadcasted_iota(jnp.int32, (count, count), 1)
    ).astype(bf16)
    earlier = mm(hot.astype(bf16), upper)
    rank = jnp.sum(hot * earlier, axis=0, keepdims=True).astype(jnp.int32)
    at = lax.broadcasted_iota(jnp.int32, (groups * rows, count), 0)
    n = lax.broadcasted_iota(jnp.int32, (ny, count), 0)
    for side in range(place.shape[0]):
        total = jnp.zeros((groups * rows, ny), f32)
        for b in range(BY):
            row = rank * BY + b
            if tail is not None and side:
                row = row + jnp.where(row >= tail, 4, 0)
            here = (at == own * rows + row).astype(f32).astype(bf16)
            there = (n == ids * BY + b).astype(f32).astype(bf16)
            total = total + mm(here, there, NT)
        place[side, :, 0:ny] = total.astype(bf16)
        place[side, :, ny : 2 * ny] = total.astype(bf16)


def table_kernel(listed, owners, table, phase, yt, vol, q, *, tail, norm):
    me = lax.axis_index("gy")
    groups, count = owners.shape
    rows = yt.shape[3] // groups
    ny = table.shape[2]
    mine = (owners[...] == me).astype(f32)
    upper = (
        lax.broadcasted_iota(jnp.int32, (count, count), 0)
        < lax.broadcasted_iota(jnp.int32, (count, count), 1)
    ).astype(f32).astype(bf16)
    rank = mm(mine.astype(bf16), upper).astype(jnp.int32)
    at = lax.broadcasted_iota(jnp.int32, (rows, count), 0)
    n = lax.broadcasted_iota(jnp.int32, (ny, count), 0)
    for side in range(yt.shape[0]):
        for g in range(groups):
            total = jnp.zeros((rows, ny), f32)
            for b in range(BY):
                row = rank[g : g + 1] * BY + b
                if tail is not None and side:
                    row = row + jnp.where(row >= tail, 4, 0)
                here = jnp.where(at == row, jnp.broadcast_to(mine[g : g + 1], at.shape), 0.0)
                there = (n == listed[g : g + 1, :] * BY + b).astype(f32).astype(bf16)
                total = total + mm(here.astype(bf16), there, NT)
            q[g * rows : (g + 1) * rows, :] = total.astype(bf16)
        for part in range(2):
            yt[side, part] = mm(table[part], q[...], NT).astype(bf16)
    vol[0] = jnp.cos(phase[...]) * norm
    vol[1] = jnp.sin(phase[...]) * norm


def finish_kernel(gathered, s, absorber, lam, zsp, spk, place, *rest, tail, first):
    damped, out, keep, am, bm = rest[-5:]
    step = pl.program_id(0)
    planes = lam.shape[0] // 2
    wz = lam.shape[1] // 2
    nx = planes

    @pl.when(step == 0)
    def _():
        left, right = chain(gathered, nx, lax.axis_index("gz"), keep)
        for x in range(planes):
            al = lam[x : x + 1, :]
            ar = lam[nx + x : nx + x + 1, :]

            def turned(row):
                return jnp.concatenate([-row[:, wz : 2 * wz], row[:, 0:wz]], 1)

            b = jnp.concatenate([al, turned(al), ar, turned(ar), zsp[0:4, :]], 0)
            a = jnp.concatenate(
                [spk[0:4, :]] + [v[x : x + 1] for v in (left[0], left[1], right[0], right[1])], 0
            )
            bhi = b.astype(bf16).astype(f32)
            ahi = a.astype(bf16).astype(f32)
            bm[x] = jnp.concatenate([bhi, b - bhi, bhi, jnp.zeros_like(b)], 0).astype(bf16)
            am[x] = jnp.concatenate([ahi, ahi, a - ahi, jnp.zeros_like(a)], 0).astype(bf16)

    sides = s.shape[0]
    groups = out.shape[0]
    rows = place.shape[1] // groups
    parts = []
    for side in range(sides):
        x = first + step * sides + side
        field = s[side] + mm(am[x], bm[x], TN)
        kept = jnp.exp(-absorber[side])
        fr = field[:, 0:wz]
        fi = field[:, wz : 2 * wz]
        dr = fr * kept
        di = fi * kept
        damped[0, side] = dr
        damped[1, side] = di
        lr = fr - dr
        li = fi - di
        folded = jnp.concatenate(
            [
                sum(lr[:, k * KZ : (k + 1) * KZ] for k in range(wz // KZ)),
                sum(li[:, k * KZ : (k + 1) * KZ] for k in range(wz // KZ)),
            ],
            1,
        )
        hi, lo = split(folded)
        parts.append(
            mm(place[side % place.shape[0]], jnp.concatenate([hi, lo], 0)).reshape(
                groups, rows, 2 * KZ
            )
        )
    if tail is None:
        for side in range(sides):
            out[:, side * rows : (side + 1) * rows, :] = parts[side]
    else:
        out[:, 0:tail, :] = parts[0][:, 0:tail]
        out[:, tail : 2 * tail, :] = parts[1][:, 0:tail]
        out[:, 2 * tail : 2 * tail + 8, :] = parts[0][:, tail:rows] + parts[1][:, tail:rows]


def transform_kernel(got, yt, ez, vol, *rest, tail):
    out = rest[-1]
    sides = out.shape[1]
    groups = got.shape[0]
    rows = yt.shape[3] // groups
    half = yt.shape[2] // 2
    for side in range(sides):
        if tail is None:
            block = got[:, side * rows : (side + 1) * rows, :]
        else:
            block = jnp.concatenate(
                [
                    got[:, side * tail : (side + 1) * tail, :],
                    got[:, 2 * tail : 2 * tail + 8, :],
                ],
                1,
            )
        u = mm3((yt[side % yt.shape[0], 0], yt[side % yt.shape[0], 1]), split(block.reshape(groups * rows, 2 * KZ)))
        ur = u[0:half, 0:KZ] - u[half:, KZ:]
        ui = u[0:half, KZ:] + u[half:, 0:KZ]
        v = mm3(split(jnp.concatenate([ur, ui], 1)), (ez[0], ez[1]))
        vr = v[:, 0:KZ]
        vi = v[:, KZ:]
        out[0, side] = vol[0] * vr - vol[1] * vi
        out[1, side] = vol[0] * vi + vol[1] * vr


def halves(table):
    exact = np.asarray(table, np.float64)
    hi = exact.astype(jnp.bfloat16)
    lo = (exact - hi.astype(np.float64)).astype(jnp.bfloat16)
    return np.stack([hi, lo])


def transform_tables():
    n = np.arange(KY)
    angle = 2.0 * np.pi / KY * (np.outer(n, n) % KY) - np.pi * (n % 2)[None, :]
    ytab = halves(np.concatenate([np.cos(angle), -np.sin(angle)], 0))
    n = np.arange(KZ)
    angle = 2.0 * np.pi / KZ * (np.outer(n, n) % KZ) - np.pi * (n % 2)[:, None]
    er, ei = np.cos(angle), -np.sin(angle)
    ztab = halves(np.block([[er, ei], [-ei, er]]))
    return ytab, ztab


def whole(shape):
    zeros = (0,) * len(shape)
    return pl.BlockSpec(tuple(shape), lambda *_: zeros)


def body(
    wavefunction,
    absorber,
    row_inverse,
    column_inverse,
    link_terms,
    shell_blocks,
    owner_map,
    volkov_phase,
):
    nx, wy, wz = wavefunction.shape[1:]
    groups = lax.axis_size("gy")
    shell = shell_blocks.shape[2]
    capacity = 2 * ((shell + groups - 1) // groups)
    sent = capacity * BY
    pair = sent % 8 == 4 and nx % 2 == 0
    sides = 2 if nx % 2 == 0 else 1
    tail = sent - 4 if pair else None
    rows = (sent + 7) // 8 * 8
    per_step = 2 * sent if pair else sides * rows
    smem = pl.BlockSpec(memory_space=pltpu.SMEM)
    listed = shell_blocks[0]
    owners = owner_map[0, :, :, 0]
    ytab, ztab = transform_tables()
    norm = 1.0 / math.sqrt(wy * wz)

    thi, tlo, pay, spk = pl.pallas_call(
        solve_rows_kernel,
        grid=(nx,),
        in_specs=[
            smem,
            pl.BlockSpec((2, 1, wy, wz), lambda x: (0, x, 0, 0)),
            whole((2, wy, wy)),
        ],
        out_specs=[
            pl.BlockSpec((1, wy, 2 * wz), lambda x: (x, 0, 0)),
            pl.BlockSpec((1, wy, 2 * wz), lambda x: (x, 0, 0)),
            whole((groups, 4 * nx + EDGE, wz)),
            whole((8, wy)),
        ],
        out_shape=[
            jax.ShapeDtypeStruct((nx, wy, 2 * wz), bf16),
            jax.ShapeDtypeStruct((nx, wy, 2 * wz), bf16),
            jax.ShapeDtypeStruct((groups, 4 * nx + EDGE, wz), f32),
            jax.ShapeDtypeStruct((8, wy), f32),
        ],
        scratch_shapes=[
            pltpu.VMEM((2 * wy, 2 * wy), bf16),
            pltpu.VMEM((2 * wy, 2 * wy), bf16),
            pltpu.VMEM((4 * nx + EDGE, wz), f32),
        ],
        name="solve_rows",
    )(link_terms, wavefunction, row_inverse)

    gathered = lax.all_to_all(pay, "gy", split_axis=0, concat_axis=0, tiled=True)

    s, base, zh, zl, zsp, zed = pl.pallas_call(
        solve_columns_kernel,
        grid=(nx,),
        in_specs=[
            smem,
            pl.BlockSpec((1, wy, 2 * wz), lambda x: (x, 0, 0)),
            pl.BlockSpec((1, wy, 2 * wz), lambda x: (x, 0, 0)),
            pl.BlockSpec(memory_space=pl.ANY),
        ],
        out_specs=[
            pl.BlockSpec((1, wy, 2 * wz), lambda x: (x, 0, 0)),
            whole((4 * nx, wy)),
            whole((2 * wz, 2 * wz)),
            whole((2 * wz, 2 * wz)),
            whole((8, 2 * wz)),
            whole((EDGE, wy)),
        ],
        out_shape=[
            jax.ShapeDtypeStruct((nx, wy, 2 * wz), f32),
            jax.ShapeDtypeStruct((4 * nx, wy), f32),
            jax.ShapeDtypeStruct((2 * wz, 2 * wz), bf16),
            jax.ShapeDtypeStruct((2 * wz, 2 * wz), bf16),
            jax.ShapeDtypeStruct((8, 2 * wz), f32),
            jax.ShapeDtypeStruct((EDGE, wy), f32),
        ],
        scratch_shapes=[
            pltpu.VMEM((2, wz, wz), f32),
            pltpu.VMEM((16, 2 * wz), bf16),
            pltpu.VMEM((16, 2 * wz), bf16),
            pltpu.SemaphoreType.DMA,
        ],
        name="solve_columns",
    )(link_terms, thi, tlo, column_inverse)

    place = pl.pallas_call(
        lambda *refs: route_kernel(*refs, tail=tail),
        out_shape=jax.ShapeDtypeStruct((2 if pair else 1, groups * rows, 2 * wy), bf16),
        name="route",
    )(listed, owners)

    lam, payz = pl.pallas_call(
        row_chain_kernel,
        out_shape=[
            jax.ShapeDtypeStruct((2 * nx, 2 * wz), f32),
            jax.ShapeDtypeStruct((4 * nx + EDGE, wy), f32),
        ],
        scratch_shapes=[pltpu.VMEM((groups, 6 * nx, wz), f32)],
        name="row_chain",
    )(gathered, zh, zl, base, zed, spk)

    edges = lax.all_gather(payz, "gz")

    yt, vol = pl.pallas_call(
        lambda *refs: table_kernel(*refs, tail=tail, norm=norm),
        out_shape=[
            jax.ShapeDtypeStruct((2 if pair else 1, 2, 2 * KY, groups * rows), bf16),
            jax.ShapeDtypeStruct((2, KY, KZ), f32),
        ],
        scratch_shapes=[pltpu.VMEM((groups * rows, KY), bf16)],
        name="tables",
    )(listed, owners, jnp.asarray(ytab), volkov_phase)

    steps = nx // sides // CHUNKS
    columns = edges.shape[0]
    sends = []
    damped = None
    for chunk in range(CHUNKS):
        start = chunk * steps

        def at(index, start=start):
            return lambda i: tuple(start + i if d == index else 0 for d in range(3))

        carried = [] if damped is None else [damped]
        damped, out = pl.pallas_call(
            lambda *refs, start=start: finish_kernel(*refs, tail=tail, first=start * sides),
            grid=(steps,),
            in_specs=[
                whole((columns, 4 * nx + EDGE, wy)),
                pl.BlockSpec((sides, wy, 2 * wz), at(0)),
                pl.BlockSpec((sides, wy, wz), at(0)),
                whole((2 * nx, 2 * wz)),
                whole((8, 2 * wz)),
                whole((8, wy)),
                whole(place.shape),
            ]
            + [pl.BlockSpec(memory_space=pl.ANY)] * len(carried),
            out_specs=[
                pl.BlockSpec((2, sides, wy, wz), lambda i, start=start: (0, start + i, 0, 0)),
                pl.BlockSpec((groups, per_step, 2 * KZ), lambda i: (0, i, 0)),
            ],
            out_shape=[
                jax.ShapeDtypeStruct((2, nx, wy, wz), f32),
                jax.ShapeDtypeStruct((groups, steps * per_step, 2 * KZ), f32),
            ],
            scratch_shapes=[
                pltpu.VMEM((columns, 6 * nx, wy), f32),
                pltpu.VMEM((nx, 32, wy), bf16),
                pltpu.VMEM((nx, 32, 2 * wz), bf16),
            ],
            input_output_aliases={7: 0} if carried else {},
            name="finish",
        )(edges, s, absorber, lam, zsp, spk, place, *carried)
        sends.append(out)

    spectrum = None
    for chunk, out in enumerate(sends):
        start = chunk * steps
        got = lax.all_to_all(out, "gy", split_axis=0, concat_axis=0, tiled=True)
        carried = [] if spectrum is None else [spectrum]
        spectrum = pl.pallas_call(
            lambda *refs: transform_kernel(*refs, tail=tail),
            grid=(steps,),
            in_specs=[
                pl.BlockSpec((groups, per_step, 2 * KZ), lambda i: (0, i, 0)),
                whole(yt.shape),
                whole(ztab.shape),
                whole((2, KY, KZ)),
            ]
            + [pl.BlockSpec(memory_space=pl.ANY)] * len(carried),
            out_specs=pl.BlockSpec(
                (2, sides, KY, KZ), lambda i, start=start: (0, start + i, 0, 0)
            ),
            out_shape=jax.ShapeDtypeStruct((2, nx, KY, KZ), f32),
            input_output_aliases={4: 0} if carried else {},
            name="transform",
        )(got, yt, jnp.asarray(ztab), vol, *carried)
    return damped, spectrum


def solution(mesh):
    placed = (
        P(None, None, "gy", "gz"),
        P(None, "gy", "gz"),
        P(None, "gy", None),
        P(),
        P(),
        P("gz", None, None),
        P("gz", None, None, None),
        P(),
    )
    return jax.shard_map(
        body,
        mesh=mesh,
        in_specs=placed,
        out_specs=(P(None, None, "gy", "gz"), P(None, "gy", "gz", None)),
        check_vma=False,
    )
```

```python
import math

import jax
import jax.numpy as jnp
import numpy as np
from jax import lax
from jax.experimental import pallas as pl
from jax.experimental.pallas import tpu as pltpu
from jax.sharding import PartitionSpec as P

BY = 2
KY = 128
KZ = 128
EDGE = 8
ORDER = lambda step: step
MBLOCK = 4

f32 = jnp.float32
bf16 = jnp.bfloat16
NN = (((1,), (0,)), ((), ()))
NT = (((1,), (1,)), ((), ()))
TN = (((0,), (0,)), ((), ()))


def mm(a, b, dims=NN):
    return lax.dot_general(a, b, dims, preferred_element_type=f32)


def split(a):
    hi = a.astype(bf16)
    return hi, (a - hi.astype(f32)).astype(bf16)


def mm3(a, b, dims=NN):
    return mm(a[0], b[0], dims) + mm(a[0], b[1], dims) + mm(a[1], b[0], dims)


def cmul(a, b):
    return (a[0] * b[0] - a[1] * b[1], a[0] * b[1] + a[1] * b[0])


def cdiv(a, b):
    modulus = b[0] * b[0] + b[1] * b[1]
    return ((a[0] * b[0] + a[1] * b[1]) / modulus, (a[1] * b[0] - a[0] * b[1]) / modulus)


def cadd(a, b):
    return (a[0] + b[0], a[1] + b[1])


def put(hi_ref, lo_ref, rows, cols, value):
    hi, lo = split(value)
    hi_ref[rows, cols] = hi
    lo_ref[rows, cols] = lo


def spikes_of(transposed, link, sweep):
    last = transposed[0].shape[0] - 1
    left = cmul(
        (link[sweep, 0, 0], link[sweep, 0, 1]), (transposed[0][0:1], transposed[1][0:1])
    )
    right = cmul(
        (link[sweep, 1, 0], link[sweep, 1, 1]),
        (transposed[0][last : last + 1], transposed[1][last : last + 1]),
    )
    return left, right


def edge_rows(left, right, lanes):
    last = left[0].shape[1] - 1
    rows = []
    for spike in (left, right):
        for at in (0, last):
            for part in spike:
                rows.append(jnp.broadcast_to(part[:, at : at + 1], (1, lanes)))
    return rows

VM = pl.BlockSpec(memory_space=pltpu.VMEM)
SM = pl.BlockSpec(memory_space=pltpu.SMEM)
AN = pl.BlockSpec(memory_space=pl.ANY)
LIMIT = pltpu.CompilerParams(vmem_limit_bytes=20 << 20)


def far(*values):
    return [pltpu.with_memory_space_constraint(value, pltpu.HBM) for value in values]


def paired_by_bits(groups):
    return groups & (groups - 1) == 0


def slot_of(owner, me, groups):
    return owner ^ me if paired_by_bits(groups) else (owner - me + groups) % groups


def source_of(step, me, groups):
    return me ^ step if paired_by_bits(groups) else (me - step + groups) % groups


def exchange(value, step, groups):
    pairs = [
        (i, i ^ step if paired_by_bits(groups) else (i + step) % groups) for i in range(groups)
    ]
    return lax.ppermute(value, "gy", pairs)


def row_edges_kernel(link, w, y, pay, spk, wv, yv, ps, sems, ysem):
    groups = pay.shape[0]
    nx, n, width = wv.shape[1:]
    ycopy = pltpu.make_async_copy(y, yv, ysem)
    ycopy.start()
    copies = []
    for x in range(nx):
        copy = pltpu.make_async_copy(w.at[:, x], wv.at[:, x], sems.at[x])
        copy.start()
        copies.append(copy)
    ycopy.wait()
    rt = yv[0].T
    it = yv[1].T
    left, right = spikes_of((rt, it), link, 0)
    for at, row in enumerate((left[0], left[1], right[0], right[1])):
        spk[at : at + 1, :] = row
    spk[4:8, :] = jnp.zeros((4, n), f32)
    for at, row in enumerate(edge_rows(left, right, width)):
        ps[4 * nx + at : 4 * nx + at + 1, :] = row
    lanes = 128
    coef = [
        (
            jnp.broadcast_to(rt[:, row : row + 1], (n, lanes)),
            jnp.broadcast_to(it[:, row : row + 1], (n, lanes)),
        )
        for row in (0, n - 1)
    ]
    for x in range(nx):
        copies[x].wait()
        for k in range(width // lanes):
            cols = slice(k * lanes, (k + 1) * lanes)
            wr = wv[0, x, :, cols]
            wi = wv[1, x, :, cols]
            for side, (cr, ci) in enumerate(coef):
                real = jnp.sum(cr * wr - ci * wi, axis=0, keepdims=True)
                imag = jnp.sum(cr * wi + ci * wr, axis=0, keepdims=True)
                at = 2 * side * nx + x
                ps[at : at + 1, cols] = real
                ps[at + nx : at + nx + 1, cols] = imag
    for g in range(groups):
        pay[g] = ps[...]


def route(listed, owners, place, tail):
    me = lax.axis_index("gy")
    groups, count = owners.shape
    rows = place.shape[1] // groups
    ny = place.shape[2] // 2
    ids = listed[pl.ds(me, 1), :]
    own = owners[pl.ds(me, 1), :]
    slot = slot_of(own, me, groups)
    hot = (lax.broadcasted_iota(jnp.int32, (groups, count), 0) == own).astype(f32)
    upper = (
        lax.broadcasted_iota(jnp.int32, (count, count), 0)
        < lax.broadcasted_iota(jnp.int32, (count, count), 1)
    ).astype(f32).astype(bf16)
    earlier = mm(hot.astype(bf16), upper)
    rank = jnp.sum(hot * earlier, axis=0, keepdims=True).astype(jnp.int32)
    at = lax.broadcasted_iota(jnp.int32, (groups * rows, count), 0)
    n = lax.broadcasted_iota(jnp.int32, (ny, count), 0)
    for side in range(place.shape[0]):
        total = jnp.zeros((groups * rows, ny), f32)
        for b in range(BY):
            row = rank * BY + b
            if tail is not None and side:
                row = row + jnp.where(row >= tail, 4, 0)
            here = (at == slot * rows + row).astype(f32).astype(bf16)
            there = (n == ids * BY + b).astype(f32).astype(bf16)
            total = total + mm(here, there, NT)
        place[side, :, 0:ny] = total.astype(bf16)
        place[side, :, ny : 2 * ny] = total.astype(bf16)


def solve_kernel(
    link, w, y, col, listed, owners,
    s, base, edge, zsp, zed, zzh, zzl, placed,
    yv, zv, iv, ov, yh, yl, th, tl, zh, zl, place, ysem, sem, isem, osem, sems, *, tail
):
    nx, n, wz = w.shape[1:]
    rank = lax.axis_index("gz")
    loads = [
        pltpu.make_async_copy(y, yv, ysem),
        pltpu.make_async_copy(col.at[:, pl.ds(rank * wz, wz), :], zv, sem),
        pltpu.make_async_copy(listed, iv, isem),
        pltpu.make_async_copy(owners, ov, osem),
    ]
    for load in loads:
        load.start()
    loads[0].wait()
    yr = yv[0]
    yi = yv[1]
    for part, value in ((0, (yr, -yi)), (1, (yi, yr))):
        for half in range(2):
            hi, lo = split(value[half])
            yh[part * n : (part + 1) * n, half * n : (half + 1) * n] = hi
            yl[part * n : (part + 1) * n, half * n : (half + 1) * n] = lo
    loads[1].wait()
    zr = zv[0]
    zi = zv[1]
    rt = zr.T
    it = zi.T
    put(zh, zl, slice(0, wz), slice(0, wz), rt)
    put(zh, zl, slice(0, wz), slice(wz, 2 * wz), it)
    put(zh, zl, slice(wz, 2 * wz), slice(0, wz), -it)
    put(zh, zl, slice(wz, 2 * wz), slice(wz, 2 * wz), rt)
    loads[2].wait()
    loads[3].wait()
    route(iv, ov, place, tail)
    sends = [
        pltpu.make_async_copy(zh, zzh, sems.at[0]),
        pltpu.make_async_copy(zl, zzl, sems.at[1]),
        pltpu.make_async_copy(place, placed, sems.at[2]),
    ]
    for send in sends:
        send.start()
    for at, (row, turned) in enumerate(((0, False), (0, True), (wz - 1, False), (wz - 1, True))):
        edge[at : at + 1, 0:wz] = (zi if turned else zr)[row : row + 1]
        edge[at : at + 1, wz : 2 * wz] = zr[row : row + 1] if turned else -zi[row : row + 1]
    edge[4:8, :] = jnp.zeros((4, 2 * wz), f32)
    left, right = spikes_of((rt, it), link, 1)
    for at, spike in enumerate((left, right)):
        zsp[2 * at : 2 * at + 1, 0:wz] = spike[0]
        zsp[2 * at : 2 * at + 1, wz : 2 * wz] = spike[1]
        zsp[2 * at + 1 : 2 * at + 2, 0:wz] = -spike[1]
        zsp[2 * at + 1 : 2 * at + 2, wz : 2 * wz] = spike[0]
    zsp[4:8, :] = jnp.zeros((4, 2 * wz), f32)
    for at, row in enumerate(edge_rows(left, right, zed.shape[1])):
        zed[at : at + 1, :] = row
    for x in range(nx):
        wx = split(w[:, x].reshape(2 * n, wz))
        hi, lo = split(mm3((yh[...], yl[...]), wx))
        rows = slice(x * n, (x + 1) * n)
        th[rows, 0:wz] = hi[0:n]
        th[rows, wz : 2 * wz] = hi[n : 2 * n]
        tl[rows, 0:wz] = lo[0:n]
        tl[rows, wz : 2 * wz] = lo[n : 2 * n]
    block = MBLOCK * n
    for m in range(nx // MBLOCK):
        rows = slice(m * block, (m + 1) * block)
        s[rows, :] = mm3((th[rows, :], tl[rows, :]), (zh[...], zl[...]))
    lane = lax.broadcasted_iota(jnp.int32, (n, 128), 1)
    picked = jnp.zeros((n, 128), f32)
    for at, column in enumerate((0, wz, wz - 1, 2 * wz - 1)):
        for x in range(nx):
            value = s[x * n : (x + 1) * n, column : column + 1]
            picked = jnp.where(lane == at * nx + x, value, picked)
    base[...] = picked.T[0 : 4 * nx]
    for send in sends:
        send.wait()


def chain(gathered, nx, own, keep):
    groups = gathered.shape[0]
    lanes = gathered.shape[2]
    zero = jnp.zeros((nx, lanes), f32)

    def read(j):
        block = gathered[j]
        rows = [block[at * nx : (at + 1) * nx] for at in range(4)]
        edges = [
            jnp.broadcast_to(block[4 * nx + at : 4 * nx + at + 1], (nx, lanes))
            for at in range(EDGE)
        ]
        head, tail = (rows[0], rows[1]), (rows[2], rows[3])
        return head, tail, [(edges[2 * at], edges[2 * at + 1]) for at in range(4)]

    def forward(j, carry):
        coupling, carried = (carry[0], carry[1]), (carry[2], carry[3])
        head, tail, (lead_left, tail_left, lead_right, tail_right) = read(j)
        product = cmul(lead_left, coupling)
        pivot = (1.0 - product[0], -product[1])
        gain = cdiv(tail_left, pivot)
        for at, value in enumerate(coupling + carried + pivot):
            keep[j, at * nx : (at + 1) * nx, :] = value
        coupling_next = cadd(tail_right, cmul(gain, cmul(lead_right, coupling)))
        carried_next = cadd(
            cmul(gain, carried), cadd(tail, cmul(cmul(gain, coupling), head))
        )
        return coupling_next + carried_next

    def solved(j, head_next):
        head, _, (lead_left, _, lead_right, _) = read(j)
        kept = keep[j]
        values = [kept[at * nx : (at + 1) * nx] for at in range(6)]
        coupling, carried, pivot = (
            (values[0], values[1]),
            (values[2], values[3]),
            (values[4], values[5]),
        )
        offset = cdiv(cadd(head, cmul(lead_left, carried)), pivot)
        factor = cdiv(lead_right, pivot)
        value = cadd(offset, cmul(factor, head_next))
        return value, cadd(carried, cmul(coupling, value))

    lax.fori_loop(0, groups, forward, (zero, zero, zero, zero))
    following = lax.fori_loop(
        0,
        groups - 1 - own,
        lambda lap, head_next: solved(groups - 1 - lap, head_next)[0],
        (zero, zero),
    )
    return solved(own, following)[1], following


def row_chain_kernel(gathered, base, edge, zed, spk, lam, pay, keep):
    nx = base.shape[0] // 4
    left, right = chain(gathered, nx, lax.axis_index("gy"), keep)
    stacked = jnp.concatenate(
        [jnp.concatenate([left[0], left[1]], 1), jnp.concatenate([right[0], right[1]], 1)], 0
    )
    lam[...] = stacked
    spikes = ((spk[0:1, :], spk[1:2, :]), (spk[2:3, :], spk[3:4, :]))
    for at in range(2):
        value = [base[(2 * at + part) * nx : (2 * at + part + 1) * nx, :] for part in range(2)]
        moved = [
            jnp.sum(stacked * edge[2 * at + part : 2 * at + part + 1, :], axis=1, keepdims=True)
            for part in range(2)
        ]
        for side in range(2):
            rows = slice(side * nx, (side + 1) * nx)
            value = cadd(value, cmul((moved[0][rows], moved[1][rows]), spikes[side]))
        pay[2 * at * nx : (2 * at + 1) * nx, :] = value[0]
        pay[(2 * at + 1) * nx : (2 * at + 2) * nx, :] = value[1]
    pay[4 * nx : 4 * nx + EDGE, :] = zed[...]


def table_kernel(listed, owners, table, phase, *rest, tail, norm):
    yt, ylast, vol, q, rank, mine = rest
    me = lax.axis_index("gy")
    groups, count = owners.shape
    rows = q.shape[0] // groups
    ny = table.shape[2]
    mine[...] = (owners[...] == me).astype(f32)
    upper = (
        lax.broadcasted_iota(jnp.int32, (count, count), 0)
        < lax.broadcasted_iota(jnp.int32, (count, count), 1)
    ).astype(f32).astype(bf16)
    rank[...] = mm(mine[...].astype(bf16), upper).astype(jnp.int32)
    at = lax.broadcasted_iota(jnp.int32, (rows, count), 0)
    n = lax.broadcasted_iota(jnp.int32, (ny, count), 0)
    order = steps_of(groups)
    for side in range(yt.shape[0]):
        for place, step in enumerate([0] + order):
            g = source_of(step, me, groups)
            own = jnp.broadcast_to(mine[pl.ds(g, 1), :], at.shape)
            total = jnp.zeros((rows, ny), f32)
            for b in range(BY):
                row = rank[pl.ds(g, 1), :] * BY + b
                if tail is not None and side:
                    row = row + jnp.where(row >= tail, 4, 0)
                here = jnp.where(at == row, own, 0.0)
                there = (n == listed[pl.ds(g, 1), :] * BY + b).astype(f32).astype(bf16)
                total = total + mm(here.astype(bf16), there, NT)
            q[place * rows : (place + 1) * rows, :] = total
        first = q[0 : (groups - 1) * rows, :].astype(bf16)
        last = q[(groups - 1) * rows : groups * rows, :].astype(bf16)
        for part in range(2):
            yt[side, part] = mm(table[part], first, NT).astype(bf16)
        hi = mm(table[0], last, NT)
        lo = mm(table[1], last, NT)
        ylast[side] = jnp.concatenate([hi, hi, lo], 1).astype(bf16)
    vol[0] = jnp.cos(phase[...]) * norm
    vol[1] = jnp.sin(phase[...]) * norm


def corrections(gathered, lam, zsp, spk, keep, am, bm):
    nx = lam.shape[0] // 2
    wz = lam.shape[1] // 2
    left, right = chain(gathered, nx, lax.axis_index("gz"), keep)
    swapped = jnp.concatenate([-lam[:, wz : 2 * wz], lam[:, 0:wz]], 1)
    for x in range(nx):
        b = jnp.concatenate(
            [
                lam[x : x + 1, :],
                swapped[x : x + 1],
                lam[nx + x : nx + x + 1, :],
                swapped[nx + x : nx + x + 1],
                zsp[0:4, :],
            ],
            0,
        )
        a = jnp.concatenate(
            [spk[0:4, :]] + [v[x : x + 1] for v in (left[0], left[1], right[0], right[1])], 0
        )
        bhi = b.astype(bf16).astype(f32)
        ahi = a.astype(bf16).astype(f32)
        bm[x] = jnp.concatenate([bhi, b - bhi, bhi, jnp.zeros_like(b)], 0).astype(bf16)
        am[x] = jnp.concatenate([ahi, ahi, a - ahi, jnp.zeros_like(a)], 0).astype(bf16)


def lost_kernel(
    gathered, s, lam, zsp, spk, absorber, zzh, zzl, placed, *rest, tail
):
    groups = len(rest) - 11
    sent = rest[:groups]
    am, bm, keep, moved, av, zh, zl, place, asems, zsems, psem = rest[groups:]
    nx, n, wz = av.shape
    loads = [
        pltpu.make_async_copy(zzh, zh, zsems.at[0]),
        pltpu.make_async_copy(zzl, zl, zsems.at[1]),
        pltpu.make_async_copy(placed, place, psem),
    ]
    for load in loads:
        load.start()
    copies = []
    for x in range(nx):
        copies.append(pltpu.make_async_copy(absorber.at[x], av.at[x], asems.at[x]))
        copies[x].start()
    loads[0].wait()
    loads[1].wait()
    moved[...] = mm3(split(lam[...]), (zh[...], zl[...]))
    corrections(gathered, moved, zsp, spk, keep, am, bm)
    loads[2].wait()
    rows = place.shape[1] // groups
    sides = 1 if tail is None else 2
    width = rows if tail is None else 2 * tail + 8
    for step in range(nx // sides):
        parts = []
        for side in range(sides):
            x = step * sides + side
            copies[x].wait()
            field = s[x * n : (x + 1) * n, :] + mm(am[x], bm[x], TN)
            kept = jnp.exp(-av[x])
            folded = []
            for part in range(2):
                value = field[:, part * wz : (part + 1) * wz]
                value = value - value * kept
                folded.append(sum(value[:, k * KZ : (k + 1) * KZ] for k in range(wz // KZ)))
            hi, lo = split(jnp.concatenate(folded, 1))
            parts.append(mm(place[side], jnp.concatenate([hi, lo], 0)))
        at = step * width
        for g in range(groups):
            top = g * rows
            if tail is None:
                sent[g][at : at + rows, :] = parts[0][top : top + rows]
            else:
                sent[g][at : at + tail, :] = parts[0][top : top + tail]
                sent[g][at + tail : at + 2 * tail, :] = parts[1][top : top + tail]
                sent[g][at + 2 * tail : at + 2 * tail + 8, :] = (
                    parts[0][top + tail : top + rows] + parts[1][top + tail : top + rows]
                )


def damp_kernel(s, absorber, am, bm, damped, dv, sems):
    nx, n, wz = absorber.shape
    copies = []
    for x in range(nx):
        field = s[x * n : (x + 1) * n, :] + mm(am[x], bm[x], TN)
        kept = jnp.exp(-absorber[x])
        for part in range(2):
            dv[x, part] = field[:, part * wz : (part + 1) * wz] * kept
            copies.append(
                pltpu.make_async_copy(dv.at[x, part], damped.at[part, x], sems.at[x, part])
            )
            copies[-1].start()
    for copy in copies:
        copy.wait()


def plane_rows(block, x, rows, tail):
    if tail is None:
        return block[x * rows : (x + 1) * rows, :]
    at = x // 2 * (2 * tail + 8)
    side = x % 2
    return jnp.concatenate(
        [
            block[at + side * tail : at + (side + 1) * tail, :],
            block[at + 2 * tail : at + 2 * tail + 8, :],
        ],
        0,
    )


def combine(u):
    half = u.shape[0] // 2
    real = u[0:half, 0:KZ] - u[half:, KZ:]
    imag = u[0:half, KZ:] + u[half:, 0:KZ]
    return real, imag


def early_kernel(yt, ez, *rest, tail):
    count = len(rest) - 2
    got, (out, moved) = rest[:count], rest[count:]
    rows = yt.shape[3] // count
    sides = 1 if tail is None else 2
    for g in range(count):
        moved[g] = mm3(split(got[g][...]), (ez[0], ez[1]))
    for x in range(out.shape[0]):
        block = jnp.concatenate([plane_rows(moved[g], x, rows, tail) for g in range(count)], 0)
        side = x % sides
        real, imag = combine(mm3((yt[side, 0], yt[side, 1]), split(block)))
        out[x, :, 0:KZ] = real
        out[x, :, KZ:] = imag


def late_kernel(ylast, ez, got, early, vol, out, moved, ov, sems, *, tail):
    rows = ylast.shape[2] // 3
    sides = 1 if tail is None else 2
    moved[...] = mm3(split(got[...]), (ez[0], ez[1]))
    copies = []
    for x in range(early.shape[0]):
        hi, lo = split(plane_rows(moved, x, rows, tail))
        real, imag = combine(mm(ylast[x % sides], jnp.concatenate([hi, lo, hi], 0)))
        real = real + early[x, :, 0:KZ]
        imag = imag + early[x, :, KZ:]
        ov[x, 0] = vol[0] * real - vol[1] * imag
        ov[x, 1] = vol[0] * imag + vol[1] * real
        for part in range(2):
            copies.append(pltpu.make_async_copy(ov.at[x, part], out.at[part, x], sems.at[x, part]))
            copies[-1].start()
    for copy in copies:
        copy.wait()


def steps_of(groups):
    if paired_by_bits(groups):
        return sorted(range(1, groups), key=ORDER)
    return list(range(1, groups))


def halves(table):
    exact = np.asarray(table, np.float64)
    hi = exact.astype(jnp.bfloat16)
    lo = (exact - hi.astype(np.float64)).astype(jnp.bfloat16)
    return np.stack([hi, lo])


def transform_tables():
    n = np.arange(KY)
    angle = 2.0 * np.pi / KY * (np.outer(n, n) % KY) - np.pi * (n % 2)[None, :]
    ytab = halves(np.concatenate([np.cos(angle), -np.sin(angle)], 0))
    n = np.arange(KZ)
    angle = 2.0 * np.pi / KZ * (np.outer(n, n) % KZ) - np.pi * (n % 2)[:, None]
    er, ei = np.cos(angle), -np.sin(angle)
    ztab = halves(np.block([[er, ei], [-ei, er]]))
    return ytab, ztab


def sds(*shape, dtype=f32):
    return jax.ShapeDtypeStruct(shape, dtype)


def body(
    wavefunction,
    absorber,
    row_inverse,
    column_inverse,
    link_terms,
    shell_blocks,
    owner_map,
    volkov_phase,
):
    nx, wy, wz = wavefunction.shape[1:]
    groups = lax.axis_size("gy")
    columns = lax.axis_size("gz")
    shell = shell_blocks.shape[2]
    capacity = 2 * ((shell + groups - 1) // groups)
    sent = capacity * BY
    paired = sent % 8 == 4 and nx % 2 == 0
    tail = sent - 4 if paired else None
    rows = (sent + 7) // 8 * 8
    sides = 2 if paired else 1
    per_plane = sent if paired else rows
    listed = shell_blocks[0]
    owners = owner_map[0, :, :, 0]
    ytab, ztab = transform_tables()
    norm = 1.0 / math.sqrt(wy * wz)

    pay, spk = pl.pallas_call(
        row_edges_kernel,
        in_specs=[SM, AN, AN],
        out_specs=[VM] * 2,
        out_shape=[sds(groups, 4 * nx + EDGE, wz), sds(8, wy)],
        scratch_shapes=[
            pltpu.VMEM((2, nx, wy, wz), f32),
            pltpu.VMEM((2, wy, wy), f32),
            pltpu.VMEM((4 * nx + EDGE, wz), f32),
            pltpu.SemaphoreType.DMA((nx,)),
            pltpu.SemaphoreType.DMA,
        ],
        name="row_edges",
    )(link_terms, wavefunction, row_inverse)

    gathered = lax.all_to_all(pay, "gy", split_axis=0, concat_axis=0, tiled=True)

    s, base, edge, zsp, zed, zzh, zzl, placed = pl.pallas_call(
        lambda *refs: solve_kernel(*refs, tail=tail),
        in_specs=[SM, VM, AN, AN, AN, AN],
        out_specs=[VM] * 5 + [AN] * 3,
        out_shape=[
            sds(nx * wy, 2 * wz),
            sds(4 * nx, wy),
            sds(8, 2 * wz),
            sds(8, 2 * wz),
            sds(EDGE, wy),
            pltpu.HBM((2 * wz, 2 * wz), bf16),
            pltpu.HBM((2 * wz, 2 * wz), bf16),
            pltpu.HBM((sides, groups * rows, 2 * wy), bf16),
        ],
        scratch_shapes=[
            pltpu.VMEM((2, wy, wy), f32),
            pltpu.VMEM((2, wz, wz), f32),
            pltpu.VMEM(listed.shape, jnp.int32),
            pltpu.VMEM(owners.shape, jnp.int32),
            pltpu.VMEM((2 * wy, 2 * wy), bf16),
            pltpu.VMEM((2 * wy, 2 * wy), bf16),
            pltpu.VMEM((nx * wy, 2 * wz), bf16),
            pltpu.VMEM((nx * wy, 2 * wz), bf16),
            pltpu.VMEM((2 * wz, 2 * wz), bf16),
            pltpu.VMEM((2 * wz, 2 * wz), bf16),
            pltpu.VMEM((sides, groups * rows, 2 * wy), bf16),
            pltpu.SemaphoreType.DMA,
            pltpu.SemaphoreType.DMA,
            pltpu.SemaphoreType.DMA,
            pltpu.SemaphoreType.DMA,
            pltpu.SemaphoreType.DMA((3,)),
        ],
        compiler_params=LIMIT,
        name="solve",
    )(link_terms, wavefunction, *far(row_inverse, column_inverse, listed, owners))

    lam, payz = pl.pallas_call(
        row_chain_kernel,
        in_specs=[VM] * 5,
        out_specs=[VM] * 2,
        out_shape=[sds(2 * nx, 2 * wz), sds(4 * nx + EDGE, wy)],
        scratch_shapes=[pltpu.VMEM((groups, 6 * nx, wz), f32)],
        compiler_params=LIMIT,
        name="row_chain",
    )(gathered, base, edge, zed, spk)

    edges = lax.all_gather(payz, "gz")

    height = nx * per_plane
    *sent, am, bm = pl.pallas_call(
        lambda *refs: lost_kernel(*refs, tail=tail),
        in_specs=[VM] * 5 + [AN] * 4,
        out_specs=[VM] * (groups + 2),
        out_shape=[sds(height, 2 * KZ)] * groups
        + [sds(nx, 32, wy, dtype=bf16), sds(nx, 32, 2 * wz, dtype=bf16)],
        scratch_shapes=[
            pltpu.VMEM((columns, 6 * nx, wy), f32),
            pltpu.VMEM((2 * nx, 2 * wz), f32),
            pltpu.VMEM((nx, wy, wz), f32),
            pltpu.VMEM((2 * wz, 2 * wz), bf16),
            pltpu.VMEM((2 * wz, 2 * wz), bf16),
            pltpu.VMEM((sides, groups * rows, 2 * wy), bf16),
            pltpu.SemaphoreType.DMA((nx,)),
            pltpu.SemaphoreType.DMA((2,)),
            pltpu.SemaphoreType.DMA,
        ],
        compiler_params=LIMIT,
        name="lost",
    )(edges, s, lam, zsp, spk, *far(absorber, zzh, zzl, placed))

    order = steps_of(groups)
    got = [sent[0]] + [exchange(sent[step], step, groups) for step in order]

    yt, ylast, vol = pl.pallas_call(
        lambda *refs: table_kernel(*refs, tail=tail, norm=norm),
        in_specs=[VM] * 4,
        out_specs=[VM] * 3,
        out_shape=[
            sds(sides, 2, 2 * KY, (groups - 1) * rows, dtype=bf16),
            sds(sides, 2 * KY, 3 * rows, dtype=bf16),
            sds(2, KY, KZ),
        ],
        scratch_shapes=[
            pltpu.VMEM((groups * rows, KY), f32),
            pltpu.VMEM(owners.shape, jnp.int32),
            pltpu.VMEM(owners.shape, f32),
        ],
        compiler_params=LIMIT,
        name="tables",
    )(listed, owners, jnp.asarray(ytab), volkov_phase)

    damped = pl.pallas_call(
        damp_kernel,
        in_specs=[VM] * 4,
        out_specs=AN,
        out_shape=sds(2, nx, wy, wz),
        scratch_shapes=[
            pltpu.VMEM((nx, 2, wy, wz), f32),
            pltpu.SemaphoreType.DMA((nx, 2)),
        ],
        compiler_params=LIMIT,
        name="damp",
    )(s, absorber, am, bm)

    early = pl.pallas_call(
        lambda *refs: early_kernel(*refs, tail=tail),
        in_specs=[VM] * (groups + 1),
        out_specs=VM,
        out_shape=sds(nx, KY, 2 * KZ),
        scratch_shapes=[pltpu.VMEM((groups - 1, height, 2 * KZ), f32)],
        compiler_params=LIMIT,
        name="early",
    )(yt, jnp.asarray(ztab), *got[:-1])

    spectrum = pl.pallas_call(
        lambda *refs: late_kernel(*refs, tail=tail),
        in_specs=[VM] * 5,
        out_specs=AN,
        out_shape=sds(2, nx, KY, KZ),
        scratch_shapes=[
            pltpu.VMEM((height, 2 * KZ), f32),
            pltpu.VMEM((nx, 2, KY, KZ), f32),
            pltpu.SemaphoreType.DMA((nx, 2)),
        ],
        compiler_params=LIMIT,
        name="late",
    )(ylast, jnp.asarray(ztab), got[-1], early, vol)
    return damped, spectrum


def solution(mesh):
    placed = (
        P(None, None, "gy", "gz"),
        P(None, "gy", "gz"),
        P(None, "gy", None),
        P(),
        P(),
        P("gz", None, None),
        P("gz", None, None, None),
        P(),
    )
    return jax.shard_map(
        body,
        mesh=mesh,
        in_specs=placed,
        out_specs=(P(None, None, "gy", "gz"), P(None, "gy", "gz", None)),
        check_vma=False,
    )
```

```python
import math

import jax
import jax.numpy as jnp
import numpy as np
from jax import lax
from jax.experimental import pallas as pl
from jax.experimental.pallas import tpu as pltpu
from jax.sharding import PartitionSpec as P

BY = 2
KY = 128
KZ = 128
EDGE = 8
ORDER = lambda step: (4, 2, 5, 3, 6, 1, 7).index(step) if step < 8 else step
MBLOCK = 4

f32 = jnp.float32
bf16 = jnp.bfloat16
NN = (((1,), (0,)), ((), ()))
NT = (((1,), (1,)), ((), ()))
TN = (((0,), (0,)), ((), ()))


def mm(a, b, dims=NN):
    return lax.dot_general(a, b, dims, preferred_element_type=f32)


def split(a):
    hi = a.astype(bf16)
    return hi, (a - hi.astype(f32)).astype(bf16)


def mm3(a, b, dims=NN):
    return mm(a[0], b[0], dims) + mm(a[0], b[1], dims) + mm(a[1], b[0], dims)


def cmul(a, b):
    return (a[0] * b[0] - a[1] * b[1], a[0] * b[1] + a[1] * b[0])


def cdiv(a, b):
    modulus = b[0] * b[0] + b[1] * b[1]
    return ((a[0] * b[0] + a[1] * b[1]) / modulus, (a[1] * b[0] - a[0] * b[1]) / modulus)


def cadd(a, b):
    return (a[0] + b[0], a[1] + b[1])


def put(hi_ref, lo_ref, rows, cols, value):
    hi, lo = split(value)
    hi_ref[rows, cols] = hi
    lo_ref[rows, cols] = lo


def spikes_of(transposed, link, sweep):
    last = transposed[0].shape[0] - 1
    left = cmul(
        (link[sweep, 0, 0], link[sweep, 0, 1]), (transposed[0][0:1], transposed[1][0:1])
    )
    right = cmul(
        (link[sweep, 1, 0], link[sweep, 1, 1]),
        (transposed[0][last : last + 1], transposed[1][last : last + 1]),
    )
    return left, right


def edge_rows(left, right, lanes):
    last = left[0].shape[1] - 1
    rows = []
    for spike in (left, right):
        for at in (0, last):
            for part in spike:
                rows.append(jnp.broadcast_to(part[:, at : at + 1], (1, lanes)))
    return rows

VM = pl.BlockSpec(memory_space=pltpu.VMEM)
SM = pl.BlockSpec(memory_space=pltpu.SMEM)
AN = pl.BlockSpec(memory_space=pl.ANY)
LIMIT = pltpu.CompilerParams(vmem_limit_bytes=20 << 20)


def far(*values):
    return [pltpu.with_memory_space_constraint(value, pltpu.HBM) for value in values]


def paired_by_bits(groups):
    return groups & (groups - 1) == 0


def slot_of(owner, me, groups):
    return owner ^ me if paired_by_bits(groups) else (owner - me + groups) % groups


def source_of(step, me, groups):
    return me ^ step if paired_by_bits(groups) else (me - step + groups) % groups


def exchange(value, step, groups):
    pairs = [
        (i, i ^ step if paired_by_bits(groups) else (i + step) % groups) for i in range(groups)
    ]
    return lax.ppermute(value, "gy", pairs)


def row_edges_kernel(link, w, y, ps, spk, wv, yv, sems, ysem):
    nx, n, width = wv.shape[1:]
    ycopy = pltpu.make_async_copy(y, yv, ysem)
    ycopy.start()
    copies = []
    for x in range(nx):
        copies.append(pltpu.make_async_copy(w.at[:, x], wv.at[:, x], sems.at[x]))
        copies[x].start()
    ycopy.wait()
    rt = yv[0].T
    it = yv[1].T
    left, right = spikes_of((rt, it), link, 0)
    for at, row in enumerate((left[0], left[1], right[0], right[1])):
        spk[at : at + 1, :] = row
    spk[4:8, :] = jnp.zeros((4, n), f32)
    for at, row in enumerate(edge_rows(left, right, width)):
        ps[0, 4 * nx + at : 4 * nx + at + 1, :] = row
    lanes = 128
    coef = [
        (
            jnp.broadcast_to(rt[:, row : row + 1], (n, lanes)),
            jnp.broadcast_to(it[:, row : row + 1], (n, lanes)),
        )
        for row in (0, n - 1)
    ]
    for x in range(nx):
        copies[x].wait()
        for k in range(width // lanes):
            cols = slice(k * lanes, (k + 1) * lanes)
            wr = wv[0, x, :, cols]
            wi = wv[1, x, :, cols]
            for side, (cr, ci) in enumerate(coef):
                real = jnp.sum(cr * wr - ci * wi, axis=0, keepdims=True)
                imag = jnp.sum(cr * wi + ci * wr, axis=0, keepdims=True)
                at = 2 * side * nx + x
                ps[0, at : at + 1, cols] = real
                ps[0, at + nx : at + nx + 1, cols] = imag


def join_kernel(mine, theirs, after, out):
    count = mine.shape[0]
    out[0:count] = mine[...]
    out[count : 2 * count] = theirs[...]


def route(listed, owners, place, tail):
    me = lax.axis_index("gy")
    groups, count = owners.shape
    rows = place.shape[1] // groups
    ny = place.shape[2] // 2
    ids = listed[pl.ds(me, 1), :]
    own = owners[pl.ds(me, 1), :]
    slot = slot_of(own, me, groups)
    hot = (lax.broadcasted_iota(jnp.int32, (groups, count), 0) == own).astype(f32)
    upper = (
        lax.broadcasted_iota(jnp.int32, (count, count), 0)
        < lax.broadcasted_iota(jnp.int32, (count, count), 1)
    ).astype(f32).astype(bf16)
    earlier = mm(hot.astype(bf16), upper)
    rank = jnp.sum(hot * earlier, axis=0, keepdims=True).astype(jnp.int32)
    at = lax.broadcasted_iota(jnp.int32, (groups * rows, count), 0)
    n = lax.broadcasted_iota(jnp.int32, (ny, count), 0)
    for side in range(place.shape[0]):
        total = jnp.zeros((groups * rows, ny), f32)
        for b in range(BY):
            row = rank * BY + b
            if tail is not None and side:
                row = row + jnp.where(row >= tail, 4, 0)
            here = (at == slot * rows + row).astype(f32).astype(bf16)
            there = (n == ids * BY + b).astype(f32).astype(bf16)
            total = total + mm(here, there, NT)
        place[side, :, 0:ny] = total.astype(bf16)
        place[side, :, ny : 2 * ny] = total.astype(bf16)


def solve_rows_kernel(w, y, th, tl, yh, yl):
    nx, n, wz = w.shape[1:]
    yr = y[0]
    yi = y[1]
    for part, value in ((0, (yr, -yi)), (1, (yi, yr))):
        for half in range(2):
            hi, lo = split(value[half])
            yh[part * n : (part + 1) * n, half * n : (half + 1) * n] = hi
            yl[part * n : (part + 1) * n, half * n : (half + 1) * n] = lo
    for x in range(nx):
        wx = split(w[:, x].reshape(2 * n, wz))
        hi, lo = split(mm3((yh[...], yl[...]), wx))
        rows = slice(x * n, (x + 1) * n)
        th[rows, 0:wz] = hi[0:n]
        th[rows, wz : 2 * wz] = hi[n : 2 * n]
        tl[rows, 0:wz] = lo[0:n]
        tl[rows, wz : 2 * wz] = lo[n : 2 * n]


def prepare_kernel(
    link, col, listed, owners, after, edge, zsp, zed, zh, zl, place, zv, iv, ov, sems, *, tail
):
    wz = zv.shape[1]
    rank = lax.axis_index("gz")
    loads = [
        pltpu.make_async_copy(col.at[:, pl.ds(rank * wz, wz), :], zv, sems.at[0]),
        pltpu.make_async_copy(listed, iv, sems.at[1]),
        pltpu.make_async_copy(owners, ov, sems.at[2]),
    ]
    for load in loads:
        load.start()
    for load in loads:
        load.wait()
    zr = zv[0]
    zi = zv[1]
    rt = zr.T
    it = zi.T
    put(zh, zl, slice(0, wz), slice(0, wz), rt)
    put(zh, zl, slice(0, wz), slice(wz, 2 * wz), it)
    put(zh, zl, slice(wz, 2 * wz), slice(0, wz), -it)
    put(zh, zl, slice(wz, 2 * wz), slice(wz, 2 * wz), rt)
    for at, (row, turned) in enumerate(((0, False), (0, True), (wz - 1, False), (wz - 1, True))):
        edge[at : at + 1, 0:wz] = (zi if turned else zr)[row : row + 1]
        edge[at : at + 1, wz : 2 * wz] = zr[row : row + 1] if turned else -zi[row : row + 1]
    edge[4:8, :] = jnp.zeros((4, 2 * wz), f32)
    left, right = spikes_of((rt, it), link, 1)
    for at, spike in enumerate((left, right)):
        zsp[2 * at : 2 * at + 1, 0:wz] = spike[0]
        zsp[2 * at : 2 * at + 1, wz : 2 * wz] = spike[1]
        zsp[2 * at + 1 : 2 * at + 2, 0:wz] = -spike[1]
        zsp[2 * at + 1 : 2 * at + 2, wz : 2 * wz] = spike[0]
    zsp[4:8, :] = jnp.zeros((4, 2 * wz), f32)
    for at, row in enumerate(edge_rows(left, right, zed.shape[1])):
        zed[at : at + 1, :] = row
    route(iv, ov, place, tail)


def solve_columns_kernel(th, tl, zh, zl, after, s, base):
    n = base.shape[1]
    nx = base.shape[0] // 4
    wz = s.shape[1] // 2
    block = MBLOCK * n
    for m in range(nx // MBLOCK):
        rows = slice(m * block, (m + 1) * block)
        s[rows, :] = mm3((th[rows, :], tl[rows, :]), (zh[...], zl[...]))
    lane = lax.broadcasted_iota(jnp.int32, (n, 128), 1)
    picked = jnp.zeros((n, 128), f32)
    for at, column in enumerate((0, wz, wz - 1, 2 * wz - 1)):
        for x in range(nx):
            value = s[x * n : (x + 1) * n, column : column + 1]
            picked = jnp.where(lane == at * nx + x, value, picked)
    base[...] = picked.T[0 : 4 * nx]


def chain(gathered, nx, own, keep, index=lambda j: j):
    groups = gathered.shape[0]
    lanes = gathered.shape[2]
    zero = jnp.zeros((nx, lanes), f32)

    def read(j):
        block = gathered[index(j)]
        rows = [block[at * nx : (at + 1) * nx] for at in range(4)]
        edges = [
            jnp.broadcast_to(block[4 * nx + at : 4 * nx + at + 1], (nx, lanes))
            for at in range(EDGE)
        ]
        head, tail = (rows[0], rows[1]), (rows[2], rows[3])
        return head, tail, [(edges[2 * at], edges[2 * at + 1]) for at in range(4)]

    def forward(j, carry):
        coupling, carried = (carry[0], carry[1]), (carry[2], carry[3])
        head, tail, (lead_left, tail_left, lead_right, tail_right) = read(j)
        product = cmul(lead_left, coupling)
        pivot = (1.0 - product[0], -product[1])
        gain = cdiv(tail_left, pivot)
        for at, value in enumerate(coupling + carried + pivot):
            keep[j, at * nx : (at + 1) * nx, :] = value
        coupling_next = cadd(tail_right, cmul(gain, cmul(lead_right, coupling)))
        carried_next = cadd(
            cmul(gain, carried), cadd(tail, cmul(cmul(gain, coupling), head))
        )
        return coupling_next + carried_next

    def solved(j, head_next):
        head, _, (lead_left, _, lead_right, _) = read(j)
        kept = keep[j]
        values = [kept[at * nx : (at + 1) * nx] for at in range(6)]
        coupling, carried, pivot = (
            (values[0], values[1]),
            (values[2], values[3]),
            (values[4], values[5]),
        )
        offset = cdiv(cadd(head, cmul(lead_left, carried)), pivot)
        factor = cdiv(lead_right, pivot)
        value = cadd(offset, cmul(factor, head_next))
        return value, cadd(carried, cmul(coupling, value))

    lax.fori_loop(0, groups, forward, (zero, zero, zero, zero))
    following = lax.fori_loop(
        0,
        groups - 1 - own,
        lambda lap, head_next: solved(groups - 1 - lap, head_next)[0],
        (zero, zero),
    )
    return solved(own, following)[1], following


def reversed_bits(value, count):
    out = 0
    while count > 1:
        out = 2 * out + value % 2
        value = value // 2
        count = count // 2
    return out


def row_chain_kernel(*refs):
    *parts, base, edge, zed, spk, lam, pay, keep, gathered = refs
    nx = base.shape[0] // 4
    own = lax.axis_index("gy")
    bits = len(parts) > 1
    groups = gathered.shape[0]
    for at in range(groups):
        part = parts[at // parts[0].shape[0]]
        place = reversed_bits(at, groups) if bits else at
        gathered[place] = part[at % parts[0].shape[0]]
    left, right = chain(gathered, nx, own, keep, (lambda j: j ^ own) if bits else (lambda j: j))
    stacked = jnp.concatenate(
        [jnp.concatenate([left[0], left[1]], 1), jnp.concatenate([right[0], right[1]], 1)], 0
    )
    lam[...] = stacked
    spikes = ((spk[0:1, :], spk[1:2, :]), (spk[2:3, :], spk[3:4, :]))
    for at in range(2):
        value = [base[(2 * at + part) * nx : (2 * at + part + 1) * nx, :] for part in range(2)]
        moved = [
            jnp.sum(stacked * edge[2 * at + part : 2 * at + part + 1, :], axis=1, keepdims=True)
            for part in range(2)
        ]
        for side in range(2):
            rows = slice(side * nx, (side + 1) * nx)
            value = cadd(value, cmul((moved[0][rows], moved[1][rows]), spikes[side]))
        pay[2 * at * nx : (2 * at + 1) * nx, :] = value[0]
        pay[(2 * at + 1) * nx : (2 * at + 2) * nx, :] = value[1]
    pay[4 * nx : 4 * nx + EDGE, :] = zed[...]


def table_kernel(listed, owners, table, phase, *rest, tail, norm):
    yt, ylast, vol, q, rank, mine = rest
    me = lax.axis_index("gy")
    groups, count = owners.shape
    rows = q.shape[0] // groups
    ny = table.shape[2]
    mine[...] = (owners[...] == me).astype(f32)
    upper = (
        lax.broadcasted_iota(jnp.int32, (count, count), 0)
        < lax.broadcasted_iota(jnp.int32, (count, count), 1)
    ).astype(f32).astype(bf16)
    rank[...] = mm(mine[...].astype(bf16), upper).astype(jnp.int32)
    at = lax.broadcasted_iota(jnp.int32, (rows, count), 0)
    n = lax.broadcasted_iota(jnp.int32, (ny, count), 0)
    order = steps_of(groups)
    for side in range(yt.shape[0]):
        for place, step in enumerate([0] + order):
            g = source_of(step, me, groups)
            own = jnp.broadcast_to(mine[pl.ds(g, 1), :], at.shape)
            total = jnp.zeros((rows, ny), f32)
            for b in range(BY):
                row = rank[pl.ds(g, 1), :] * BY + b
                if tail is not None and side:
                    row = row + jnp.where(row >= tail, 4, 0)
                here = jnp.where(at == row, own, 0.0)
                there = (n == listed[pl.ds(g, 1), :] * BY + b).astype(f32).astype(bf16)
                total = total + mm(here.astype(bf16), there, NT)
            q[place * rows : (place + 1) * rows, :] = total
        first = q[0 : (groups - 1) * rows, :].astype(bf16)
        last = q[(groups - 1) * rows : groups * rows, :].astype(bf16)
        for part in range(2):
            yt[side, part] = mm(table[part], first, NT).astype(bf16)
        hi = mm(table[0], last, NT)
        lo = mm(table[1], last, NT)
        ylast[side] = jnp.concatenate([hi, hi, lo], 1).astype(bf16)
    vol[0] = jnp.cos(phase[...]) * norm
    vol[1] = jnp.sin(phase[...]) * norm


def corrections(gathered, lam, zsp, spk, keep, am, bm):
    nx = lam.shape[0] // 2
    wz = lam.shape[1] // 2
    left, right = chain(gathered, nx, lax.axis_index("gz"), keep)
    swapped = jnp.concatenate([-lam[:, wz : 2 * wz], lam[:, 0:wz]], 1)
    for x in range(nx):
        b = jnp.concatenate(
            [
                lam[x : x + 1, :],
                swapped[x : x + 1],
                lam[nx + x : nx + x + 1, :],
                swapped[nx + x : nx + x + 1],
                zsp[0:4, :],
            ],
            0,
        )
        a = jnp.concatenate(
            [spk[0:4, :]] + [v[x : x + 1] for v in (left[0], left[1], right[0], right[1])], 0
        )
        bhi = b.astype(bf16).astype(f32)
        ahi = a.astype(bf16).astype(f32)
        bm[x] = jnp.concatenate([bhi, b - bhi, bhi, jnp.zeros_like(b)], 0).astype(bf16)
        am[x] = jnp.concatenate([ahi, ahi, a - ahi, jnp.zeros_like(a)], 0).astype(bf16)


def lost_kernel(gathered, s, lam, zsp, spk, absorber, zh, zl, place, *rest, tail):
    groups = len(rest) - 4
    sent = rest[:groups]
    am, bm, keep, moved = rest[groups:]
    nx, n, wz = absorber.shape
    moved[...] = mm3(split(lam[...]), (zh[...], zl[...]))
    corrections(gathered, moved, zsp, spk, keep, am, bm)
    rows = place.shape[1] // groups
    sides = 1 if tail is None else 2
    width = rows if tail is None else 2 * tail + 8
    for step in range(nx // sides):
        parts = []
        for side in range(sides):
            x = step * sides + side
            field = s[x * n : (x + 1) * n, :] + mm(am[x], bm[x], TN)
            kept = jnp.exp(-absorber[x])
            folded = []
            for part in range(2):
                value = field[:, part * wz : (part + 1) * wz]
                value = value - value * kept
                folded.append(sum(value[:, k * KZ : (k + 1) * KZ] for k in range(wz // KZ)))
            hi, lo = split(jnp.concatenate(folded, 1))
            parts.append(mm(place[side], jnp.concatenate([hi, lo], 0)))
        at = step * width
        for g in range(groups):
            top = g * rows
            if tail is None:
                sent[g][at : at + rows, :] = parts[0][top : top + rows]
            else:
                sent[g][at : at + tail, :] = parts[0][top : top + tail]
                sent[g][at + tail : at + 2 * tail, :] = parts[1][top : top + tail]
                sent[g][at + 2 * tail : at + 2 * tail + 8, :] = (
                    parts[0][top + tail : top + rows] + parts[1][top + tail : top + rows]
                )


def damp_kernel(s, absorber, am, bm, damped, dv, sems):
    nx, n, wz = absorber.shape
    copies = []
    for x in range(nx):
        field = s[x * n : (x + 1) * n, :] + mm(am[x], bm[x], TN)
        kept = jnp.exp(-absorber[x])
        for part in range(2):
            dv[x, part] = field[:, part * wz : (part + 1) * wz] * kept
            copies.append(
                pltpu.make_async_copy(dv.at[x, part], damped.at[part, x], sems.at[x, part])
            )
            copies[-1].start()
    for copy in copies:
        copy.wait()


def plane_rows(block, x, rows, tail):
    if tail is None:
        return block[x * rows : (x + 1) * rows, :]
    at = x // 2 * (2 * tail + 8)
    side = x % 2
    return jnp.concatenate(
        [
            block[at + side * tail : at + (side + 1) * tail, :],
            block[at + 2 * tail : at + 2 * tail + 8, :],
        ],
        0,
    )


def combine(u):
    half = u.shape[0] // 2
    real = u[0:half, 0:KZ] - u[half:, KZ:]
    imag = u[0:half, KZ:] + u[half:, 0:KZ]
    return real, imag


def early_kernel(yt, ez, *rest, tail):
    count = len(rest) - 2
    got, (out, moved) = rest[:count], rest[count:]
    rows = yt.shape[3] // count
    sides = 1 if tail is None else 2
    for g in range(count):
        moved[g] = mm3(split(got[g][...]), (ez[0], ez[1]))
    for x in range(out.shape[0]):
        block = jnp.concatenate([plane_rows(moved[g], x, rows, tail) for g in range(count)], 0)
        side = x % sides
        real, imag = combine(mm3((yt[side, 0], yt[side, 1]), split(block)))
        out[x, :, 0:KZ] = real
        out[x, :, KZ:] = imag


def late_kernel(ylast, ez, got, early, vol, out, moved, ov, sems, *, tail):
    rows = ylast.shape[2] // 3
    sides = 1 if tail is None else 2
    moved[...] = mm3(split(got[...]), (ez[0], ez[1]))
    copies = []
    for x in range(early.shape[0]):
        hi, lo = split(plane_rows(moved, x, rows, tail))
        real, imag = combine(mm(ylast[x % sides], jnp.concatenate([hi, lo, hi], 0)))
        real = real + early[x, :, 0:KZ]
        imag = imag + early[x, :, KZ:]
        ov[x, 0] = vol[0] * real - vol[1] * imag
        ov[x, 1] = vol[0] * imag + vol[1] * real
        for part in range(2):
            copies.append(pltpu.make_async_copy(ov.at[x, part], out.at[part, x], sems.at[x, part]))
            copies[-1].start()
    for copy in copies:
        copy.wait()


def steps_of(groups):
    if paired_by_bits(groups):
        return sorted(range(1, groups), key=ORDER)
    return list(range(1, groups))


def halves(table):
    exact = np.asarray(table, np.float64)
    hi = exact.astype(jnp.bfloat16)
    lo = (exact - hi.astype(np.float64)).astype(jnp.bfloat16)
    return np.stack([hi, lo])


def transform_tables():
    n = np.arange(KY)
    angle = 2.0 * np.pi / KY * (np.outer(n, n) % KY) - np.pi * (n % 2)[None, :]
    ytab = halves(np.concatenate([np.cos(angle), -np.sin(angle)], 0))
    n = np.arange(KZ)
    angle = 2.0 * np.pi / KZ * (np.outer(n, n) % KZ) - np.pi * (n % 2)[:, None]
    er, ei = np.cos(angle), -np.sin(angle)
    ztab = halves(np.block([[er, ei], [-ei, er]]))
    return ytab, ztab


def widen(blocks, after, groups):
    if not paired_by_bits(groups) or 2 * blocks[0].shape[0] >= groups:
        return blocks
    shape = blocks[0].shape
    joined = pl.pallas_call(
        join_kernel,
        in_specs=[VM, VM, AN],
        out_specs=VM,
        out_shape=sds(2 * shape[0], *shape[1:]),
        compiler_params=LIMIT,
        name="join",
    )(*blocks, after)
    return [joined, exchange(joined, groups // (4 * shape[0]), groups)]


def sds(*shape, dtype=f32):
    return jax.ShapeDtypeStruct(shape, dtype)


def body(
    wavefunction,
    absorber,
    row_inverse,
    column_inverse,
    link_terms,
    shell_blocks,
    owner_map,
    volkov_phase,
):
    nx, wy, wz = wavefunction.shape[1:]
    groups = lax.axis_size("gy")
    columns = lax.axis_size("gz")
    shell = shell_blocks.shape[2]
    capacity = 2 * ((shell + groups - 1) // groups)
    sent = capacity * BY
    paired = sent % 8 == 4 and nx % 2 == 0
    tail = sent - 4 if paired else None
    rows = (sent + 7) // 8 * 8
    sides = 2 if paired else 1
    per_plane = sent if paired else rows
    listed = shell_blocks[0]
    owners = owner_map[0, :, :, 0]
    ytab, ztab = transform_tables()
    norm = 1.0 / math.sqrt(wy * wz)

    pay, spk, wv, yv = pl.pallas_call(
        row_edges_kernel,
        in_specs=[SM, AN, AN],
        out_specs=[VM] * 4,
        out_shape=[
            sds(1, 4 * nx + EDGE, wz),
            sds(8, wy),
            sds(2, nx, wy, wz),
            sds(2, wy, wy),
        ],
        scratch_shapes=[pltpu.SemaphoreType.DMA((nx,)), pltpu.SemaphoreType.DMA],
        compiler_params=LIMIT,
        name="row_edges",
    )(*far(link_terms, wavefunction, row_inverse))

    bits = paired_by_bits(groups)
    gathered = [pay, exchange(pay, groups // 2, groups)] if bits else [lax.all_gather(pay[0], "gy")]
    th, tl = pl.pallas_call(
        solve_rows_kernel,
        in_specs=[VM] * 2,
        out_specs=[VM] * 2,
        out_shape=[sds(nx * wy, 2 * wz, dtype=bf16)] * 2,
        scratch_shapes=[pltpu.VMEM((2 * wy, 2 * wy), bf16)] * 2,
        compiler_params=LIMIT,
        name="solve_rows",
    )(wv, yv)

    first = gathered[-1]
    gathered = widen(gathered, th, groups)
    edge, zsp, zed, zh, zl, place = pl.pallas_call(
        lambda *refs: prepare_kernel(*refs, tail=tail),
        in_specs=[SM] + [AN] * 4,
        out_specs=[VM] * 6,
        out_shape=[
            sds(8, 2 * wz),
            sds(8, 2 * wz),
            sds(EDGE, wy),
            sds(2 * wz, 2 * wz, dtype=bf16),
            sds(2 * wz, 2 * wz, dtype=bf16),
            sds(sides, groups * rows, 2 * wy, dtype=bf16),
        ],
        scratch_shapes=[
            pltpu.VMEM((2, wz, wz), f32),
            pltpu.VMEM(listed.shape, jnp.int32),
            pltpu.VMEM(owners.shape, jnp.int32),
            pltpu.SemaphoreType.DMA((3,)),
        ],
        compiler_params=LIMIT,
        name="prepare",
    )(*far(link_terms, column_inverse, listed, owners), first)

    second = gathered[-1]
    gathered = widen(gathered, edge, groups)
    s, base = pl.pallas_call(
        solve_columns_kernel,
        in_specs=[VM] * 4 + [AN],
        out_specs=[VM] * 2,
        out_shape=[sds(nx * wy, 2 * wz), sds(4 * nx, wy)],
        compiler_params=LIMIT,
        name="solve_columns",
    )(th, tl, zh, zl, second)

    while bits and 2 * gathered[0].shape[0] < groups:
        gathered = widen(gathered, base, groups)

    lam, payz = pl.pallas_call(
        row_chain_kernel,
        in_specs=[VM] * (4 + len(gathered)),
        out_specs=[VM] * 2,
        out_shape=[sds(2 * nx, 2 * wz), sds(4 * nx + EDGE, wy)],
        scratch_shapes=[
            pltpu.VMEM((groups, 6 * nx, wz), f32),
            pltpu.VMEM((groups, 4 * nx + EDGE, wz), f32),
        ],
        compiler_params=LIMIT,
        name="row_chain",
    )(*gathered, base, edge, zed, spk)

    edges = lax.all_gather(payz, "gz")

    height = nx * per_plane
    *sent, am, bm = pl.pallas_call(
        lambda *refs: lost_kernel(*refs, tail=tail),
        in_specs=[VM] * 9,
        out_specs=[VM] * (groups + 2),
        out_shape=[sds(height, 2 * KZ)] * groups
        + [sds(nx, 32, wy, dtype=bf16), sds(nx, 32, 2 * wz, dtype=bf16)],
        scratch_shapes=[
            pltpu.VMEM((columns, 6 * nx, wy), f32),
            pltpu.VMEM((2 * nx, 2 * wz), f32),
        ],
        compiler_params=LIMIT,
        name="lost",
    )(edges, s, lam, zsp, spk, absorber, zh, zl, place)

    order = steps_of(groups)
    got = [sent[0]] + [exchange(sent[step], step, groups) for step in order]

    yt, ylast, vol = pl.pallas_call(
        lambda *refs: table_kernel(*refs, tail=tail, norm=norm),
        in_specs=[VM] * 4,
        out_specs=[VM] * 3,
        out_shape=[
            sds(sides, 2, 2 * KY, (groups - 1) * rows, dtype=bf16),
            sds(sides, 2 * KY, 3 * rows, dtype=bf16),
            sds(2, KY, KZ),
        ],
        scratch_shapes=[
            pltpu.VMEM((groups * rows, KY), f32),
            pltpu.VMEM(owners.shape, jnp.int32),
            pltpu.VMEM(owners.shape, f32),
        ],
        compiler_params=LIMIT,
        name="tables",
    )(listed, owners, jnp.asarray(ytab), volkov_phase)

    damped = pl.pallas_call(
        damp_kernel,
        in_specs=[VM] * 4,
        out_specs=AN,
        out_shape=sds(2, nx, wy, wz),
        scratch_shapes=[
            pltpu.VMEM((nx, 2, wy, wz), f32),
            pltpu.SemaphoreType.DMA((nx, 2)),
        ],
        compiler_params=LIMIT,
        name="damp",
    )(s, absorber, am, bm)

    early = pl.pallas_call(
        lambda *refs: early_kernel(*refs, tail=tail),
        in_specs=[VM] * (groups + 1),
        out_specs=VM,
        out_shape=sds(nx, KY, 2 * KZ),
        scratch_shapes=[pltpu.VMEM((groups - 1, height, 2 * KZ), f32)],
        compiler_params=LIMIT,
        name="early",
    )(yt, jnp.asarray(ztab), *got[:-1])

    spectrum = pl.pallas_call(
        lambda *refs: late_kernel(*refs, tail=tail),
        in_specs=[VM] * 5,
        out_specs=AN,
        out_shape=sds(2, nx, KY, KZ),
        scratch_shapes=[
            pltpu.VMEM((height, 2 * KZ), f32),
            pltpu.VMEM((nx, 2, KY, KZ), f32),
            pltpu.SemaphoreType.DMA((nx, 2)),
        ],
        compiler_params=LIMIT,
        name="late",
    )(ylast, jnp.asarray(ztab), got[-1], early, vol)
    return damped, spectrum


def solution(mesh):
    placed = (
        P(None, None, "gy", "gz"),
        P(None, "gy", "gz"),
        P(None, "gy", None),
        P(),
        P(),
        P("gz", None, None),
        P("gz", None, None, None),
        P(),
    )
    return jax.shard_map(
        body,
        mesh=mesh,
        in_specs=placed,
        out_specs=(P(None, None, "gy", "gz"), P(None, "gy", "gz", None)),
        check_vma=False,
    )
```

```python
import math

import jax
import jax.numpy as jnp
import numpy as np
from jax import lax
from jax.experimental import pallas as pl
from jax.experimental.pallas import tpu as pltpu
from jax.sharding import PartitionSpec as P

BY = 2
KY = 128
KZ = 128
EDGE = 8
ORDER = lambda step: step
MBLOCK = 4

f32 = jnp.float32
bf16 = jnp.bfloat16
NN = (((1,), (0,)), ((), ()))
NT = (((1,), (1,)), ((), ()))
TN = (((0,), (0,)), ((), ()))


def mm(a, b, dims=NN):
    return lax.dot_general(a, b, dims, preferred_element_type=f32)


def split(a):
    hi = a.astype(bf16)
    return hi, (a - hi.astype(f32)).astype(bf16)


def mm3(a, b, dims=NN):
    return mm(a[0], b[0], dims) + mm(a[0], b[1], dims) + mm(a[1], b[0], dims)


def cmul(a, b):
    return (a[0] * b[0] - a[1] * b[1], a[0] * b[1] + a[1] * b[0])


def cdiv(a, b):
    modulus = b[0] * b[0] + b[1] * b[1]
    return ((a[0] * b[0] + a[1] * b[1]) / modulus, (a[1] * b[0] - a[0] * b[1]) / modulus)


def cadd(a, b):
    return (a[0] + b[0], a[1] + b[1])


def put(hi_ref, lo_ref, rows, cols, value):
    hi, lo = split(value)
    hi_ref[rows, cols] = hi
    lo_ref[rows, cols] = lo


def spikes_of(transposed, link, sweep):
    last = transposed[0].shape[0] - 1
    left = cmul(
        (link[sweep, 0, 0], link[sweep, 0, 1]), (transposed[0][0:1], transposed[1][0:1])
    )
    right = cmul(
        (link[sweep, 1, 0], link[sweep, 1, 1]),
        (transposed[0][last : last + 1], transposed[1][last : last + 1]),
    )
    return left, right


def edge_rows(left, right, lanes):
    last = left[0].shape[1] - 1
    rows = []
    for spike in (left, right):
        for at in (0, last):
            for part in spike:
                rows.append(jnp.broadcast_to(part[:, at : at + 1], (1, lanes)))
    return rows

VM = pl.BlockSpec(memory_space=pltpu.VMEM)
SM = pl.BlockSpec(memory_space=pltpu.SMEM)
AN = pl.BlockSpec(memory_space=pl.ANY)
LIMIT = pltpu.CompilerParams(vmem_limit_bytes=20 << 20)


def far(*values):
    return [pltpu.with_memory_space_constraint(value, pltpu.HBM) for value in values]


def paired_by_bits(groups):
    return groups & (groups - 1) == 0


def slot_of(owner, me, groups):
    return owner ^ me if paired_by_bits(groups) else (owner - me + groups) % groups


def source_of(step, me, groups):
    return me ^ step if paired_by_bits(groups) else (me - step + groups) % groups


def exchange(value, step, groups, axis="gy"):
    pairs = [
        (i, i ^ step if paired_by_bits(groups) else (i + step) % groups) for i in range(groups)
    ]
    return lax.ppermute(value, axis, pairs)


def inner_of(groups):
    bits = groups.bit_length() - 1
    return 1 << (bits // 2)


def row_edges_kernel(
    link, w, y, col, listed, owners, ps, spk, wv, yv, zv, iv, ov, sems, ysem, zsems
):
    nx, n, width = wv.shape[1:]
    ycopy = pltpu.make_async_copy(y, yv, ysem)
    ycopy.start()
    copies = []
    for x in range(nx):
        copies.append(pltpu.make_async_copy(w.at[:, x], wv.at[:, x], sems.at[x]))
        copies[x].start()
    wz = zv.shape[1]
    rank = lax.axis_index("gz")
    loads = [
        pltpu.make_async_copy(col.at[:, pl.ds(rank * wz, wz), :], zv, zsems.at[0]),
        pltpu.make_async_copy(listed, iv, zsems.at[1]),
        pltpu.make_async_copy(owners, ov, zsems.at[2]),
    ]
    for load in loads:
        load.start()
    ycopy.wait()
    rt = yv[0].T
    it = yv[1].T
    left, right = spikes_of((rt, it), link, 0)
    for at, row in enumerate((left[0], left[1], right[0], right[1])):
        spk[at : at + 1, :] = row
    spk[4:8, :] = jnp.zeros((4, n), f32)
    lanes = ps.shape[2]
    count = width // lanes * nx
    for at, row in enumerate(edge_rows(left, right, lanes)):
        ps[0, 4 * count + at : 4 * count + at + 1, :] = row
    coef = [
        (
            jnp.broadcast_to(rt[:, row : row + 1], (n, lanes)),
            jnp.broadcast_to(it[:, row : row + 1], (n, lanes)),
        )
        for row in (0, n - 1)
    ]
    for x in range(nx):
        copies[x].wait()
        for k in range(width // lanes):
            cols = slice(k * lanes, (k + 1) * lanes)
            wr = wv[0, x, :, cols]
            wi = wv[1, x, :, cols]
            for side, (cr, ci) in enumerate(coef):
                real = jnp.sum(cr * wr - ci * wi, axis=0, keepdims=True)
                imag = jnp.sum(cr * wi + ci * wr, axis=0, keepdims=True)
                at = 2 * side * count + k * nx + x
                ps[0, at : at + 1, :] = real
                ps[0, at + count : at + count + 1, :] = imag
    for load in loads:
        load.wait()


def join_kernel(*refs):
    *parts, _, out = refs
    for at, part in enumerate(parts):
        out[at] = part[0]


def route(listed, owners, place, tail):
    me = lax.axis_index("gy")
    groups, count = owners.shape
    rows = place.shape[1] // groups
    ny = place.shape[2] // 2
    ids = listed[pl.ds(me, 1), :]
    own = owners[pl.ds(me, 1), :]
    slot = slot_of(own, me, groups)
    hot = (lax.broadcasted_iota(jnp.int32, (groups, count), 0) == own).astype(f32)
    upper = (
        lax.broadcasted_iota(jnp.int32, (count, count), 0)
        < lax.broadcasted_iota(jnp.int32, (count, count), 1)
    ).astype(f32).astype(bf16)
    earlier = mm(hot.astype(bf16), upper)
    rank = jnp.sum(hot * earlier, axis=0, keepdims=True).astype(jnp.int32)
    at = lax.broadcasted_iota(jnp.int32, (groups * rows, count), 0)
    n = lax.broadcasted_iota(jnp.int32, (ny, count), 0)
    for side in range(place.shape[0]):
        total = jnp.zeros((groups * rows, ny), f32)
        for b in range(BY):
            row = rank * BY + b
            if tail is not None and side:
                row = row + jnp.where(row >= tail, 4, 0)
            here = (at == slot * rows + row).astype(f32).astype(bf16)
            there = (n == ids * BY + b).astype(f32).astype(bf16)
            total = total + mm(here, there, NT)
        place[side, :, 0:ny] = total.astype(bf16)
        place[side, :, ny : 2 * ny] = total.astype(bf16)


def solve_rows_kernel(w, y, th, tl, yh, yl):
    nx, n, wz = w.shape[1:]
    yr = y[0]
    yi = y[1]
    for part, value in ((0, (yr, -yi)), (1, (yi, yr))):
        for half in range(2):
            hi, lo = split(value[half])
            yh[part * n : (part + 1) * n, half * n : (half + 1) * n] = hi
            yl[part * n : (part + 1) * n, half * n : (half + 1) * n] = lo
    for x in range(nx):
        wx = split(w[:, x].reshape(2 * n, wz))
        hi, lo = split(mm3((yh[...], yl[...]), wx))
        rows = slice(x * n, (x + 1) * n)
        th[rows, 0:wz] = hi[0:n]
        th[rows, wz : 2 * wz] = hi[n : 2 * n]
        tl[rows, 0:wz] = lo[0:n]
        tl[rows, wz : 2 * wz] = lo[n : 2 * n]


def prepare_kernel(link, zv, iv, ov, after, edge, zsp, zed, zh, zl, place, *, tail):
    wz = zv.shape[1]
    zr = zv[0]
    zi = zv[1]
    rt = zr.T
    it = zi.T
    put(zh, zl, slice(0, wz), slice(0, wz), rt)
    put(zh, zl, slice(0, wz), slice(wz, 2 * wz), it)
    put(zh, zl, slice(wz, 2 * wz), slice(0, wz), -it)
    put(zh, zl, slice(wz, 2 * wz), slice(wz, 2 * wz), rt)
    for at, (row, turned) in enumerate(((0, False), (0, True), (wz - 1, False), (wz - 1, True))):
        edge[at : at + 1, 0:wz] = (zi if turned else zr)[row : row + 1]
        edge[at : at + 1, wz : 2 * wz] = zr[row : row + 1] if turned else -zi[row : row + 1]
    edge[4:8, :] = jnp.zeros((4, 2 * wz), f32)
    left, right = spikes_of((rt, it), link, 1)
    for at, spike in enumerate((left, right)):
        zsp[2 * at : 2 * at + 1, 0:wz] = spike[0]
        zsp[2 * at : 2 * at + 1, wz : 2 * wz] = spike[1]
        zsp[2 * at + 1 : 2 * at + 2, 0:wz] = -spike[1]
        zsp[2 * at + 1 : 2 * at + 2, wz : 2 * wz] = spike[0]
    zsp[4:8, :] = jnp.zeros((4, 2 * wz), f32)
    for at, row in enumerate(edge_rows(left, right, zed.shape[1])):
        zed[at : at + 1, :] = row
    route(iv, ov, place, tail)


def solve_columns_kernel(th, tl, zh, zl, s, base):
    n = base.shape[1]
    nx = base.shape[0] // 4
    wz = s.shape[1] // 2
    block = MBLOCK * n
    for m in range(nx // MBLOCK):
        rows = slice(m * block, (m + 1) * block)
        s[rows, :] = mm3((th[rows, :], tl[rows, :]), (zh[...], zl[...]))
    lane = lax.broadcasted_iota(jnp.int32, (n, 128), 1)
    picked = jnp.zeros((n, 128), f32)
    for at, column in enumerate((0, wz, wz - 1, 2 * wz - 1)):
        for x in range(nx):
            value = s[x * n : (x + 1) * n, column : column + 1]
            picked = jnp.where(lane == at * nx + x, value, picked)
    base[...] = picked.T[0 : 4 * nx]


def chain(gathered, nx, own, keep, index=lambda j: j):
    groups = gathered.shape[0]
    lanes = gathered.shape[2]
    zero = jnp.zeros((nx, lanes), f32)

    def read(j):
        block = gathered[index(j)]
        rows = [block[at * nx : (at + 1) * nx] for at in range(4)]
        edges = [
            jnp.broadcast_to(block[4 * nx + at : 4 * nx + at + 1], (nx, lanes))
            for at in range(EDGE)
        ]
        head, tail = (rows[0], rows[1]), (rows[2], rows[3])
        return head, tail, [(edges[2 * at], edges[2 * at + 1]) for at in range(4)]

    def forward(j, carry):
        coupling, carried = (carry[0], carry[1]), (carry[2], carry[3])
        head, tail, (lead_left, tail_left, lead_right, tail_right) = read(j)
        product = cmul(lead_left, coupling)
        pivot = (1.0 - product[0], -product[1])
        gain = cdiv(tail_left, pivot)
        for at, value in enumerate(coupling + carried + pivot):
            keep[j, at * nx : (at + 1) * nx, :] = value
        coupling_next = cadd(tail_right, cmul(gain, cmul(lead_right, coupling)))
        carried_next = cadd(
            cmul(gain, carried), cadd(tail, cmul(cmul(gain, coupling), head))
        )
        return coupling_next + carried_next

    def solved(j, head_next):
        head, _, (lead_left, _, lead_right, _) = read(j)
        kept = keep[j]
        values = [kept[at * nx : (at + 1) * nx] for at in range(6)]
        coupling, carried, pivot = (
            (values[0], values[1]),
            (values[2], values[3]),
            (values[4], values[5]),
        )
        offset = cdiv(cadd(head, cmul(lead_left, carried)), pivot)
        factor = cdiv(lead_right, pivot)
        value = cadd(offset, cmul(factor, head_next))
        return value, cadd(carried, cmul(coupling, value))

    lax.fori_loop(0, groups, forward, (zero, zero, zero, zero))
    following = lax.fori_loop(
        0,
        groups - 1 - own,
        lambda lap, head_next: solved(groups - 1 - lap, head_next)[0],
        (zero, zero),
    )
    return solved(own, following)[1], following


def row_chain_kernel(*refs):
    *parts, base, edge, zed, spk, lam, pay, keep, gathered = refs
    nx = base.shape[0] // 4
    own = lax.axis_index("gy")
    bits = len(parts) > 1
    for b, part in enumerate(parts):
        for a in range(part.shape[0]):
            gathered[a * len(parts) + b] = part[a]
    count = (gathered.shape[1] - EDGE) // 4
    sides = chain(gathered, count, own, keep, (lambda j: j ^ own) if bits else (lambda j: j))
    stacked = jnp.concatenate(
        [
            jnp.concatenate(
                [part[k : k + nx] for part in side for k in range(0, count, nx)], 1
            )
            for side in sides
        ],
        0,
    )
    lam[...] = stacked
    spikes = ((spk[0:1, :], spk[1:2, :]), (spk[2:3, :], spk[3:4, :]))
    for at in range(2):
        value = [base[(2 * at + part) * nx : (2 * at + part + 1) * nx, :] for part in range(2)]
        moved = [
            jnp.sum(stacked * edge[2 * at + part : 2 * at + part + 1, :], axis=1, keepdims=True)
            for part in range(2)
        ]
        for side in range(2):
            rows = slice(side * nx, (side + 1) * nx)
            value = cadd(value, cmul((moved[0][rows], moved[1][rows]), spikes[side]))
        pay[2 * at * nx : (2 * at + 1) * nx, :] = value[0]
        pay[(2 * at + 1) * nx : (2 * at + 2) * nx, :] = value[1]
    pay[4 * nx : 4 * nx + EDGE, :] = zed[...]


def table_kernel(listed, owners, table, phase, *rest, tail, norm):
    yt, ylast, vol, q, rank, mine = rest
    me = lax.axis_index("gy")
    groups, count = owners.shape
    rows = q.shape[0] // groups
    ny = table.shape[2]
    mine[...] = (owners[...] == me).astype(f32)
    upper = (
        lax.broadcasted_iota(jnp.int32, (count, count), 0)
        < lax.broadcasted_iota(jnp.int32, (count, count), 1)
    ).astype(f32).astype(bf16)
    rank[...] = mm(mine[...].astype(bf16), upper).astype(jnp.int32)
    at = lax.broadcasted_iota(jnp.int32, (rows, count), 0)
    n = lax.broadcasted_iota(jnp.int32, (ny, count), 0)
    order = steps_of(groups)
    for side in range(yt.shape[0]):
        for place, step in enumerate([0] + order):
            g = source_of(step, me, groups)
            own = jnp.broadcast_to(mine[pl.ds(g, 1), :], at.shape)
            total = jnp.zeros((rows, ny), f32)
            for b in range(BY):
                row = rank[pl.ds(g, 1), :] * BY + b
                if tail is not None and side:
                    row = row + jnp.where(row >= tail, 4, 0)
                here = jnp.where(at == row, own, 0.0)
                there = (n == listed[pl.ds(g, 1), :] * BY + b).astype(f32).astype(bf16)
                total = total + mm(here.astype(bf16), there, NT)
            q[place * rows : (place + 1) * rows, :] = total
        cut = (groups - late_of(groups)) * rows
        first = q[0:cut, :].astype(bf16)
        last = q[cut : groups * rows, :].astype(bf16)
        for part in range(2):
            yt[side, part] = mm(table[part], first, NT).astype(bf16)
        hi = mm(table[0], last, NT)
        lo = mm(table[1], last, NT)
        ylast[side] = jnp.concatenate([hi, hi, lo], 1).astype(bf16)
    vol[0] = jnp.cos(phase[...]) * norm
    vol[1] = jnp.sin(phase[...]) * norm


def ready_kernel(lam, zh, zl, zsp, absorber, bm, kept, moved):
    nx = lam.shape[0] // 2
    wz = lam.shape[1] // 2
    moved[...] = mm3(split(lam[...]), (zh[...], zl[...]))
    swapped = jnp.concatenate([-moved[:, wz : 2 * wz], moved[:, 0:wz]], 1)
    for x in range(nx):
        b = jnp.concatenate(
            [
                moved[x : x + 1, :],
                swapped[x : x + 1],
                moved[nx + x : nx + x + 1, :],
                swapped[nx + x : nx + x + 1],
                zsp[0:4, :],
            ],
            0,
        )
        bhi = b.astype(bf16).astype(f32)
        bm[x] = jnp.concatenate([bhi, b - bhi, bhi, jnp.zeros_like(b)], 0).astype(bf16)
        kept[x] = jnp.exp(-absorber[x])


def lost_kernel(s, spk, keep_part, bm, place, *rest, columns, groups, tail):
    parts = rest[:columns]
    am, keep, gathered = rest[-3:]
    sent = rest[columns : columns + groups]
    more = rest[columns + groups : -3]
    final = steps_of(groups)[-1]
    nx, n, wz = keep_part.shape
    own = lax.axis_index("gz")
    bits = paired_by_bits(columns)
    for step, part in enumerate(parts):
        gathered[step] = part[...]

    def index(j):
        return j ^ own if bits else (own - j + columns) % columns

    left, right = chain(gathered, nx, own, keep, index)
    for x in range(nx):
        a = jnp.concatenate(
            [spk[0:4, :]] + [v[x : x + 1] for v in (left[0], left[1], right[0], right[1])], 0
        )
        ahi = a.astype(bf16).astype(f32)
        am[x] = jnp.concatenate([ahi, ahi, a - ahi, jnp.zeros_like(a)], 0).astype(bf16)
    rows = place.shape[1] // groups
    sides = 1 if tail is None else 2
    width = rows if tail is None else 2 * tail + 8
    for step in range(nx // sides):
        parts = []
        for side in range(sides):
            x = step * sides + side
            field = s[x * n : (x + 1) * n, :] + mm(am[x], bm[x], TN)
            kept = keep_part[x]
            folded = []
            for part in range(2):
                value = field[:, part * wz : (part + 1) * wz]
                value = value - value * kept
                folded.append(sum(value[:, k * KZ : (k + 1) * KZ] for k in range(wz // KZ)))
            hi, lo = split(jnp.concatenate(folded, 1))
            parts.append(mm(place[side], jnp.concatenate([hi, lo], 0)))
        for g in range(groups):
            top = g * rows
            at = step * width
            target = sent[g]
            if g == final and at >= target.shape[0]:
                at = at - target.shape[0]
                target = more[0]
            if tail is None:
                target[at : at + rows, :] = parts[0][top : top + rows]
            else:
                target[at : at + tail, :] = parts[0][top : top + tail]
                target[at + tail : at + 2 * tail, :] = parts[1][top : top + tail]
                target[at + 2 * tail : at + 2 * tail + 8, :] = (
                    parts[0][top + tail : top + rows] + parts[1][top + tail : top + rows]
                )


def damp_kernel(s, keep_part, am, bm, damped, dv, sems):
    nx, n, wz = keep_part.shape
    copies = []
    for x in range(nx):
        field = s[x * n : (x + 1) * n, :] + mm(am[x], bm[x], TN)
        kept = keep_part[x]
        for part in range(2):
            dv[x, part] = field[:, part * wz : (part + 1) * wz] * kept
            copies.append(
                pltpu.make_async_copy(dv.at[x, part], damped.at[part, x], sems.at[x, part])
            )
            copies[-1].start()
    for copy in copies:
        copy.wait()


def plane_rows(block, x, rows, tail):
    if tail is None:
        return block[x * rows : (x + 1) * rows, :]
    at = x // 2 * (2 * tail + 8)
    side = x % 2
    return jnp.concatenate(
        [
            block[at + side * tail : at + (side + 1) * tail, :],
            block[at + 2 * tail : at + 2 * tail + 8, :],
        ],
        0,
    )


def combine(u):
    half = u.shape[0] // 2
    real = u[0:half, 0:KZ] - u[half:, KZ:]
    imag = u[0:half, KZ:] + u[half:, 0:KZ]
    return real, imag


def early_kernel(yt, ez, *rest, tail):
    count = len(rest) - 2
    got, (out, moved) = rest[:count], rest[count:]
    rows = yt.shape[3] // count
    sides = 1 if tail is None else 2
    for g in range(count):
        moved[g] = mm3(split(got[g][...]), (ez[0], ez[1]))
    for x in range(out.shape[0]):
        block = jnp.concatenate([plane_rows(moved[g], x, rows, tail) for g in range(count)], 0)
        side = x % sides
        real, imag = combine(mm3((yt[side, 0], yt[side, 1]), split(block)))
        out[x, :, 0:KZ] = real
        out[x, :, KZ:] = imag


def late_kernel(ylast, ez, early, vol, *rest, tail, first):
    out, moved, ov, sems = rest[-4:]
    sources = moved.shape[0]
    height = moved.shape[1]
    count = ov.shape[0]
    rows = ylast.shape[2] // (3 * sources)
    sides = 1 if tail is None else 2
    top = first * height // count
    for at in range(sources):
        got = rest[at]
        block = got[...] if at == sources - 1 else got[top : top + height, :]
        moved[at] = mm3(split(block), (ez[0], ez[1]))
    copies = []
    for x in range(count):
        block = [plane_rows(moved[at], x, rows, tail) for at in range(sources)]
        hi, lo = split(jnp.concatenate(block, 0))
        real, imag = combine(mm(ylast[x % sides], jnp.concatenate([hi, lo, hi], 0)))
        real = real + early[first + x, :, 0:KZ]
        imag = imag + early[first + x, :, KZ:]
        ov[x, 0] = vol[0] * real - vol[1] * imag
        ov[x, 1] = vol[0] * imag + vol[1] * real
        for part in range(2):
            copies.append(
                pltpu.make_async_copy(ov.at[x, part], out.at[part, first + x], sems.at[x, part])
            )
            copies[-1].start()
    for copy in copies:
        copy.wait()


def late_of(groups):
    return min(2, groups - 1)


def steps_of(groups):
    if paired_by_bits(groups):
        return sorted(range(1, groups), key=ORDER)
    return list(range(1, groups))


def halves(table):
    exact = np.asarray(table, np.float64)
    hi = exact.astype(jnp.bfloat16)
    lo = (exact - hi.astype(np.float64)).astype(jnp.bfloat16)
    return np.stack([hi, lo])


def transform_tables():
    n = np.arange(KY)
    angle = 2.0 * np.pi / KY * (np.outer(n, n) % KY) - np.pi * (n % 2)[None, :]
    ytab = halves(np.concatenate([np.cos(angle), -np.sin(angle)], 0))
    n = np.arange(KZ)
    angle = 2.0 * np.pi / KZ * (np.outer(n, n) % KZ) - np.pi * (n % 2)[:, None]
    er, ei = np.cos(angle), -np.sin(angle)
    ztab = halves(np.block([[er, ei], [-ei, er]]))
    return ytab, ztab


def sds(*shape, dtype=f32):
    return jax.ShapeDtypeStruct(shape, dtype)


def body(
    wavefunction,
    absorber,
    row_inverse,
    column_inverse,
    link_terms,
    shell_blocks,
    owner_map,
    volkov_phase,
):
    nx, wy, wz = wavefunction.shape[1:]
    groups = lax.axis_size("gy")
    columns = lax.axis_size("gz")
    shell = shell_blocks.shape[2]
    capacity = 2 * ((shell + groups - 1) // groups)
    sent = capacity * BY
    paired = sent % 8 == 4 and nx % 2 == 0
    tail = sent - 4 if paired else None
    rows = (sent + 7) // 8 * 8
    sides = 2 if paired else 1
    per_plane = sent if paired else rows
    listed = shell_blocks[0]
    owners = owner_map[0, :, :, 0]
    ytab, ztab = transform_tables()
    norm = 1.0 / math.sqrt(wy * wz)

    tall = 4 * (wz // 128) * nx + EDGE
    pay, spk, wv, yv, zv, iv, ov = pl.pallas_call(
        row_edges_kernel,
        in_specs=[SM] + [AN] * 5,
        out_specs=[VM] * 7,
        out_shape=[
            sds(1, tall, 128),
            sds(8, wy),
            sds(2, nx, wy, wz),
            sds(2, wy, wy),
            sds(2, wz, wz),
            sds(*listed.shape, dtype=jnp.int32),
            sds(*owners.shape, dtype=jnp.int32),
        ],
        scratch_shapes=[
            pltpu.SemaphoreType.DMA((nx,)),
            pltpu.SemaphoreType.DMA,
            pltpu.SemaphoreType.DMA((3,)),
        ],
        compiler_params=LIMIT,
        name="row_edges",
    )(*far(link_terms, wavefunction, row_inverse, column_inverse, listed, owners))

    inner = inner_of(groups) if paired_by_bits(groups) else groups
    outer = groups // inner
    if paired_by_bits(groups):
        lines = [pay] + [exchange(pay, step * inner, groups) for step in range(1, outer)]
    else:
        lines = [lax.all_gather(pay[0], "gy")]

    th, tl = pl.pallas_call(
        solve_rows_kernel,
        in_specs=[VM] * 2,
        out_specs=[VM] * 2,
        out_shape=[sds(nx * wy, 2 * wz, dtype=bf16)] * 2,
        scratch_shapes=[pltpu.VMEM((2 * wy, 2 * wy), bf16)] * 2,
        compiler_params=LIMIT,
        name="solve_rows",
    )(wv, yv)

    first = lines[-1]
    if paired_by_bits(groups):
        joined = pl.pallas_call(
            join_kernel,
            in_specs=[VM] * outer + [AN],
            out_specs=VM,
            out_shape=sds(outer, tall, 128),
            compiler_params=LIMIT,
            name="join",
        )(*lines, th)
        gathered = [joined] + [exchange(joined, step, groups) for step in range(1, inner)]
    else:
        gathered = lines

    edge, zsp, zed, zh, zl, place = pl.pallas_call(
        lambda *refs: prepare_kernel(*refs, tail=tail),
        in_specs=[SM, VM, VM, VM, AN],
        out_specs=[VM] * 6,
        out_shape=[
            sds(8, 2 * wz),
            sds(8, 2 * wz),
            sds(EDGE, wy),
            sds(2 * wz, 2 * wz, dtype=bf16),
            sds(2 * wz, 2 * wz, dtype=bf16),
            sds(sides, groups * rows, 2 * wy, dtype=bf16),
        ],
        compiler_params=LIMIT,
        name="prepare",
    )(*far(link_terms), zv, iv, ov, first)

    s, base = pl.pallas_call(
        solve_columns_kernel,
        in_specs=[VM] * 4,
        out_specs=[VM] * 2,
        out_shape=[sds(nx * wy, 2 * wz), sds(4 * nx, wy)],
        compiler_params=LIMIT,
        name="solve_columns",
    )(th, tl, zh, zl)

    lam, payz = pl.pallas_call(
        row_chain_kernel,
        in_specs=[VM] * (4 + len(gathered)),
        out_specs=[VM] * 2,
        out_shape=[sds(2 * nx, 2 * wz), sds(4 * nx + EDGE, wy)],
        scratch_shapes=[
            pltpu.VMEM((groups, 6 * (wz // 128) * nx, 128), f32),
            pltpu.VMEM((groups, tall, 128), f32),
        ],
        compiler_params=LIMIT,
        name="row_chain",
    )(*gathered, base, edge, zed, spk)

    edges = [payz] + [exchange(payz, step, columns, "gz") for step in range(1, columns)]

    bm, kept = pl.pallas_call(
        ready_kernel,
        in_specs=[VM] * 5,
        out_specs=[VM] * 2,
        out_shape=[sds(nx, 32, 2 * wz, dtype=bf16), sds(nx, wy, wz)],
        scratch_shapes=[pltpu.VMEM((2 * nx, 2 * wz), f32)],
        compiler_params=LIMIT,
        name="ready",
    )(lam, zh, zl, zsp, absorber)

    height = nx * per_plane
    order = steps_of(groups)
    cuts = 2 if nx // sides % 2 == 0 else 1
    *sent, am = pl.pallas_call(
        lambda *refs: lost_kernel(*refs, columns=columns, groups=groups, tail=tail),
        in_specs=[VM] * (5 + columns),
        out_specs=[VM] * (groups + cuts),
        out_shape=[sds(height // (cuts if g == order[-1] else 1), 2 * KZ) for g in range(groups)]
        + [sds(height // cuts, 2 * KZ)] * (cuts - 1)
        + [sds(nx, 32, wy, dtype=bf16)],
        scratch_shapes=[
            pltpu.VMEM((columns, 6 * nx, wy), f32),
            pltpu.VMEM((columns, 4 * nx + EDGE, wy), f32),
        ],
        compiler_params=LIMIT,
        name="lost",
    )(s, spk, kept, bm, place, *edges)

    late = late_of(groups)
    got = [sent[0]] + [exchange(sent[step], step, groups) for step in order[:-1]]
    lasts = [exchange(part, order[-1], groups) for part in [sent[order[-1]]] + sent[groups:]]

    yt, ylast, vol = pl.pallas_call(
        lambda *refs: table_kernel(*refs, tail=tail, norm=norm),
        in_specs=[VM] * 4,
        out_specs=[VM] * 3,
        out_shape=[
            sds(sides, 2, 2 * KY, (groups - late) * rows, dtype=bf16),
            sds(sides, 2 * KY, 3 * late * rows, dtype=bf16),
            sds(2, KY, KZ),
        ],
        scratch_shapes=[
            pltpu.VMEM((groups * rows, KY), f32),
            pltpu.VMEM(owners.shape, jnp.int32),
            pltpu.VMEM(owners.shape, f32),
        ],
        compiler_params=LIMIT,
        name="tables",
    )(listed, owners, jnp.asarray(ytab), volkov_phase)

    damped = pl.pallas_call(
        damp_kernel,
        in_specs=[VM] * 4,
        out_specs=AN,
        out_shape=sds(2, nx, wy, wz),
        scratch_shapes=[
            pltpu.VMEM((nx, 2, wy, wz), f32),
            pltpu.SemaphoreType.DMA((nx, 2)),
        ],
        compiler_params=LIMIT,
        name="damp",
    )(s, kept, am, bm)

    early = pl.pallas_call(
        lambda *refs: early_kernel(*refs, tail=tail),
        in_specs=[VM] * (groups - late + 2),
        out_specs=VM,
        out_shape=sds(nx, KY, 2 * KZ),
        scratch_shapes=[pltpu.VMEM((groups - late, height, 2 * KZ), f32)],
        compiler_params=LIMIT,
        name="early",
    )(yt, jnp.asarray(ztab), *got[: groups - late])

    spectrum = []
    first = 0
    for block in lasts:
        count = block.shape[0] // per_plane
        spectrum = [
            pl.pallas_call(
                lambda *refs, first=first: late_kernel(*refs, tail=tail, first=first),
                in_specs=[VM] * (4 + late) + [AN] * len(spectrum),
                out_specs=AN,
                out_shape=sds(2, nx, KY, KZ),
                scratch_shapes=[
                    pltpu.VMEM((late, *block.shape), f32),
                    pltpu.VMEM((count, 2, KY, KZ), f32),
                    pltpu.SemaphoreType.DMA((count, 2)),
                ],
                input_output_aliases={4 + late: 0} if spectrum else {},
                compiler_params=LIMIT,
                name="late",
            )(ylast, jnp.asarray(ztab), early, vol, *got[groups - late :], block, *far(*spectrum))
        ]
        first = first + count
    (spectrum,) = spectrum
    return damped, spectrum


def solution(mesh):
    placed = (
        P(None, None, "gy", "gz"),
        P(None, "gy", "gz"),
        P(None, "gy", None),
        P(),
        P(),
        P("gz", None, None),
        P("gz", None, None, None),
        P(),
    )
    return jax.shard_map(
        body,
        mesh=mesh,
        in_specs=placed,
        out_specs=(P(None, None, "gy", "gz"), P(None, "gy", "gz", None)),
        check_vma=False,
    )
```

```python
import math

import jax
import jax.numpy as jnp
import numpy as np
from jax import lax
from jax.experimental import pallas as pl
from jax.experimental.pallas import tpu as pltpu
from jax.sharding import PartitionSpec as P


BY = 2
KY = 128
KZ = 128
EDGE = 8
MBLOCK = 4

f32 = jnp.float32
bf16 = jnp.bfloat16
NN = (((1,), (0,)), ((), ()))
NT = (((1,), (1,)), ((), ()))
TN = (((0,), (0,)), ((), ()))


def mm(a, b, dims=NN):
    return lax.dot_general(a, b, dims, preferred_element_type=f32)


def split(a):
    hi = a.astype(bf16)
    return hi, (a - hi.astype(f32)).astype(bf16)


def mm3(a, b, dims=NN):
    return mm(a[0], b[0], dims) + mm(a[0], b[1], dims) + mm(a[1], b[0], dims)


def cmul(a, b):
    return (a[0] * b[0] - a[1] * b[1], a[0] * b[1] + a[1] * b[0])


def cdiv(a, b):
    modulus = b[0] * b[0] + b[1] * b[1]
    return ((a[0] * b[0] + a[1] * b[1]) / modulus, (a[1] * b[0] - a[0] * b[1]) / modulus)


def cadd(a, b):
    return (a[0] + b[0], a[1] + b[1])


def put(hi_ref, lo_ref, rows, cols, value):
    hi, lo = split(value)
    hi_ref[rows, cols] = hi
    lo_ref[rows, cols] = lo


def spikes_of(transposed, link, sweep):
    last = transposed[0].shape[0] - 1
    left = cmul(
        (link[sweep, 0, 0], link[sweep, 0, 1]), (transposed[0][0:1], transposed[1][0:1])
    )
    right = cmul(
        (link[sweep, 1, 0], link[sweep, 1, 1]),
        (transposed[0][last : last + 1], transposed[1][last : last + 1]),
    )
    return left, right


def edge_rows(left, right, lanes):
    last = left[0].shape[1] - 1
    rows = []
    for spike in (left, right):
        for at in (0, last):
            for part in spike:
                rows.append(jnp.broadcast_to(part[:, at : at + 1], (1, lanes)))
    return rows


VM = pl.BlockSpec(memory_space=pltpu.VMEM)
SM = pl.BlockSpec(memory_space=pltpu.SMEM)
AN = pl.BlockSpec(memory_space=pl.ANY)
LIMIT = pltpu.CompilerParams(vmem_limit_bytes=20 << 20)


def far(*values):
    return [pltpu.with_memory_space_constraint(value, pltpu.HBM) for value in values]


def paired_by_bits(groups):
    return groups & (groups - 1) == 0


def slot_of(owner, me, groups):
    return owner ^ me if paired_by_bits(groups) else (owner - me + groups) % groups


def source_of(step, me, groups):
    return me ^ step if paired_by_bits(groups) else (me - step + groups) % groups


def exchange(value, step, groups, axis="gy"):
    pairs = [
        (i, i ^ step if paired_by_bits(groups) else (i + step) % groups) for i in range(groups)
    ]
    return lax.ppermute(value, axis, pairs)


def inner_of(groups):
    bits = groups.bit_length() - 1
    return 1 << (bits // 2)


def row_edges_kernel(
    link, w, y, col, listed, owners, ps, spk, wv, yv, zv, iv, ov, sums, sems, ysem, zsems
):
    nx, n, width = wv.shape[1:]
    ycopy = pltpu.make_async_copy(y, yv, ysem)
    ycopy.start()
    copies = []
    for x in range(nx):
        copies.append(pltpu.make_async_copy(w.at[:, x], wv.at[:, x], sems.at[x]))
        copies[x].start()
    wz = zv.shape[1]
    rank = lax.axis_index("gz")
    loads = [
        pltpu.make_async_copy(col.at[:, pl.ds(rank * wz, wz), :], zv, zsems.at[0]),
        pltpu.make_async_copy(listed, iv, zsems.at[1]),
        pltpu.make_async_copy(owners, ov, zsems.at[2]),
    ]
    for load in loads:
        load.start()
    ycopy.wait()
    rt = yv[0].T
    it = yv[1].T
    left, right = spikes_of((rt, it), link, 0)
    for at, row in enumerate((left[0], left[1], right[0], right[1])):
        spk[at : at + 1, :] = row
    spk[4:8, :] = jnp.zeros((4, n), f32)
    lanes = ps.shape[2]
    count = width // lanes * nx
    for at, row in enumerate(edge_rows(left, right, lanes)):
        ps[0, 4 * count + at : 4 * count + at + 1, :] = row
    coef = [
        (
            jnp.broadcast_to(rt[:, row : row + 1], (n, lanes)),
            jnp.broadcast_to(it[:, row : row + 1], (n, lanes)),
        )
        for row in (0, n - 1)
    ]
    for x in range(nx):
        copies[x].wait()
        for k in range(width // lanes):
            cols = slice(k * lanes, (k + 1) * lanes)
            wr = wv[0, x, :, cols]
            wi = wv[1, x, :, cols]
            for side, (cr, ci) in enumerate(coef):
                real = cr * wr - ci * wi
                imag = cr * wi + ci * wr
                at = 2 * side * count + k * nx + x
                sums[at] = jnp.sum(real.reshape(n // 8, 8, lanes), axis=0)
                sums[at + count] = jnp.sum(imag.reshape(n // 8, 8, lanes), axis=0)
    ps[0, 0 : 4 * count, :] = jnp.sum(sums[...], axis=1)
    for load in loads:
        load.wait()


def join_kernel(*refs):
    *parts, _, out = refs
    for at, part in enumerate(parts):
        out[at] = part[0]


def route(listed, owners, place, tail):
    me = lax.axis_index("gy")
    groups, count = owners.shape
    rows = place.shape[1] // groups
    ny = place.shape[2] // 2
    ids = listed[pl.ds(me, 1), :]
    own = owners[pl.ds(me, 1), :]
    slot = slot_of(own, me, groups)
    hot = (lax.broadcasted_iota(jnp.int32, (groups, count), 0) == own).astype(f32)
    upper = (
        lax.broadcasted_iota(jnp.int32, (count, count), 0)
        < lax.broadcasted_iota(jnp.int32, (count, count), 1)
    ).astype(f32).astype(bf16)
    earlier = mm(hot.astype(bf16), upper)
    rank = jnp.sum(hot * earlier, axis=0, keepdims=True).astype(jnp.int32)
    at = lax.broadcasted_iota(jnp.int32, (groups * rows, count), 0)
    n = lax.broadcasted_iota(jnp.int32, (ny, count), 0)
    for side in range(place.shape[0]):
        total = jnp.zeros((groups * rows, ny), f32)
        for b in range(BY):
            row = rank * BY + b
            if tail is not None and side:
                row = row + jnp.where(row >= tail, 4, 0)
            here = (at == slot * rows + row).astype(f32).astype(bf16)
            there = (n == ids * BY + b).astype(f32).astype(bf16)
            total = total + mm(here, there, NT)
        place[side, :, 0:ny] = total.astype(bf16)
        place[side, :, ny : 2 * ny] = total.astype(bf16)


def solve_rows_kernel(w, y, th, tl, yh, yl):
    nx, n, wz = w.shape[1:]
    yr = y[0]
    yi = y[1]
    for part, value in ((0, (yr, -yi)), (1, (yi, yr))):
        for half in range(2):
            hi, lo = split(value[half])
            yh[part * n : (part + 1) * n, half * n : (half + 1) * n] = hi
            yl[part * n : (part + 1) * n, half * n : (half + 1) * n] = lo
    for x in range(nx):
        wx = split(w[:, x].reshape(2 * n, wz))
        hi, lo = split(mm3((yh[...], yl[...]), wx))
        rows = slice(x * n, (x + 1) * n)
        th[rows, 0:wz] = hi[0:n]
        th[rows, wz : 2 * wz] = hi[n : 2 * n]
        tl[rows, 0:wz] = lo[0:n]
        tl[rows, wz : 2 * wz] = lo[n : 2 * n]


def prepare_kernel(link, zv, iv, ov, after, edge, zsp, zed, zh, zl, place, *, tail):
    wz = zv.shape[1]
    zr = zv[0]
    zi = zv[1]
    rt = zr.T
    it = zi.T
    put(zh, zl, slice(0, wz), slice(0, wz), rt)
    put(zh, zl, slice(0, wz), slice(wz, 2 * wz), it)
    put(zh, zl, slice(wz, 2 * wz), slice(0, wz), -it)
    put(zh, zl, slice(wz, 2 * wz), slice(wz, 2 * wz), rt)
    for at, (row, turned) in enumerate(((0, False), (0, True), (wz - 1, False), (wz - 1, True))):
        edge[at : at + 1, 0:wz] = (zi if turned else zr)[row : row + 1]
        edge[at : at + 1, wz : 2 * wz] = zr[row : row + 1] if turned else -zi[row : row + 1]
    edge[4:8, :] = jnp.zeros((4, 2 * wz), f32)
    left, right = spikes_of((rt, it), link, 1)
    for at, spike in enumerate((left, right)):
        zsp[2 * at : 2 * at + 1, 0:wz] = spike[0]
        zsp[2 * at : 2 * at + 1, wz : 2 * wz] = spike[1]
        zsp[2 * at + 1 : 2 * at + 2, 0:wz] = -spike[1]
        zsp[2 * at + 1 : 2 * at + 2, wz : 2 * wz] = spike[0]
    zsp[4:8, :] = jnp.zeros((4, 2 * wz), f32)
    for at, row in enumerate(edge_rows(left, right, zed.shape[1])):
        zed[at : at + 1, :] = row
    route(iv, ov, place, tail)


def solve_columns_kernel(th, tl, zh, zl, s, base):
    n = base.shape[1]
    nx = base.shape[0] // 4
    wz = s.shape[1] // 2
    block = MBLOCK * n
    for m in range(nx // MBLOCK):
        rows = slice(m * block, (m + 1) * block)
        s[rows, :] = mm3((th[rows, :], tl[rows, :]), (zh[...], zl[...]))
    lane = lax.broadcasted_iota(jnp.int32, (n, 128), 1)
    picked = jnp.zeros((n, 128), f32)
    for at, column in enumerate((0, wz, wz - 1, 2 * wz - 1)):
        for x in range(nx):
            value = s[x * n : (x + 1) * n, column : column + 1]
            picked = jnp.where(lane == at * nx + x, value, picked)
    base[...] = picked.T[0 : 4 * nx]


def chain(gathered, nx, own, keep, index=lambda j: j):
    groups = gathered.shape[0]
    lanes = gathered.shape[2]
    zero = jnp.zeros((nx, lanes), f32)

    def read(j):
        block = gathered[index(j)]
        rows = [block[at * nx : (at + 1) * nx] for at in range(4)]
        edges = [
            jnp.broadcast_to(block[4 * nx + at : 4 * nx + at + 1], (nx, lanes))
            for at in range(EDGE)
        ]
        head, tail = (rows[0], rows[1]), (rows[2], rows[3])
        return head, tail, [(edges[2 * at], edges[2 * at + 1]) for at in range(4)]

    def forward(j, carry):
        coupling, carried = (carry[0], carry[1]), (carry[2], carry[3])
        head, tail, (lead_left, tail_left, lead_right, tail_right) = read(j)
        product = cmul(lead_left, coupling)
        pivot = (1.0 - product[0], -product[1])
        gain = cdiv(tail_left, pivot)
        for at, value in enumerate(coupling + carried + pivot):
            keep[j, at * nx : (at + 1) * nx, :] = value
        coupling_next = cadd(tail_right, cmul(gain, cmul(lead_right, coupling)))
        carried_next = cadd(
            cmul(gain, carried), cadd(tail, cmul(cmul(gain, coupling), head))
        )
        return coupling_next + carried_next

    def solved(j, head_next):
        head, _, (lead_left, _, lead_right, _) = read(j)
        kept = keep[j]
        values = [kept[at * nx : (at + 1) * nx] for at in range(6)]
        coupling, carried, pivot = (
            (values[0], values[1]),
            (values[2], values[3]),
            (values[4], values[5]),
        )
        offset = cdiv(cadd(head, cmul(lead_left, carried)), pivot)
        factor = cdiv(lead_right, pivot)
        value = cadd(offset, cmul(factor, head_next))
        return value, cadd(carried, cmul(coupling, value))

    lax.fori_loop(0, groups, forward, (zero, zero, zero, zero))
    following = lax.fori_loop(
        0,
        groups - 1 - own,
        lambda lap, head_next: solved(groups - 1 - lap, head_next)[0],
        (zero, zero),
    )
    return solved(own, following)[1], following


def row_chain_kernel(*refs):
    *parts, base, edge, zed, spk, lam, pay, keep, gathered = refs
    nx = base.shape[0] // 4
    own = lax.axis_index("gy")
    bits = len(parts) > 1
    for b, part in enumerate(parts):
        for a in range(part.shape[0]):
            gathered[a * len(parts) + b] = part[a]
    count = (gathered.shape[1] - EDGE) // 4
    sides = chain(gathered, count, own, keep, (lambda j: j ^ own) if bits else (lambda j: j))
    stacked = jnp.concatenate(
        [
            jnp.concatenate(
                [part[k : k + nx] for part in side for k in range(0, count, nx)], 1
            )
            for side in sides
        ],
        0,
    )
    lam[...] = stacked
    spikes = ((spk[0:1, :], spk[1:2, :]), (spk[2:3, :], spk[3:4, :]))
    for at in range(2):
        value = [base[(2 * at + part) * nx : (2 * at + part + 1) * nx, :] for part in range(2)]
        moved = [
            jnp.sum(stacked * edge[2 * at + part : 2 * at + part + 1, :], axis=1, keepdims=True)
            for part in range(2)
        ]
        for side in range(2):
            rows = slice(side * nx, (side + 1) * nx)
            value = cadd(value, cmul((moved[0][rows], moved[1][rows]), spikes[side]))
        pay[2 * at * nx : (2 * at + 1) * nx, :] = value[0]
        pay[(2 * at + 1) * nx : (2 * at + 2) * nx, :] = value[1]
    pay[4 * nx : 4 * nx + EDGE, :] = zed[...]


def table_kernel(listed, owners, table, phase, *rest, tail, norm):
    yt, ylast, vol, q, rank, mine = rest
    me = lax.axis_index("gy")
    groups, count = owners.shape
    rows = q.shape[0] // groups
    ny = table.shape[2]
    mine[...] = (owners[...] == me).astype(f32)
    upper = (
        lax.broadcasted_iota(jnp.int32, (count, count), 0)
        < lax.broadcasted_iota(jnp.int32, (count, count), 1)
    ).astype(f32).astype(bf16)
    rank[...] = mm(mine[...].astype(bf16), upper).astype(jnp.int32)
    at = lax.broadcasted_iota(jnp.int32, (rows, count), 0)
    n = lax.broadcasted_iota(jnp.int32, (ny, count), 0)
    order = steps_of(groups)
    for side in range(yt.shape[0]):
        for place, step in enumerate([0] + order):
            g = source_of(step, me, groups)
            own = jnp.broadcast_to(mine[pl.ds(g, 1), :], at.shape)
            total = jnp.zeros((rows, ny), f32)
            for b in range(BY):
                row = rank[pl.ds(g, 1), :] * BY + b
                if tail is not None and side:
                    row = row + jnp.where(row >= tail, 4, 0)
                here = jnp.where(at == row, own, 0.0)
                there = (n == listed[pl.ds(g, 1), :] * BY + b).astype(f32).astype(bf16)
                total = total + mm(here.astype(bf16), there, NT)
            q[place * rows : (place + 1) * rows, :] = total
        cut = (groups - late_of(groups)) * rows
        first = q[0:cut, :].astype(bf16)
        last = q[cut : groups * rows, :].astype(bf16)
        for part in range(2):
            yt[side, part] = mm(table[part], first, NT).astype(bf16)
        hi = mm(table[0], last, NT)
        lo = mm(table[1], last, NT)
        ylast[side] = jnp.concatenate([hi, hi, lo], 1).astype(bf16)
    vol[0] = jnp.cos(phase[...]) * norm
    vol[1] = jnp.sin(phase[...]) * norm


def ready_kernel(lam, zh, zl, zsp, absorber, bm, kept, moved):
    nx = lam.shape[0] // 2
    wz = lam.shape[1] // 2
    moved[...] = mm3(split(lam[...]), (zh[...], zl[...]))
    swapped = jnp.concatenate([-moved[:, wz : 2 * wz], moved[:, 0:wz]], 1)
    for x in range(nx):
        b = jnp.concatenate(
            [
                moved[x : x + 1, :],
                swapped[x : x + 1],
                moved[nx + x : nx + x + 1, :],
                swapped[nx + x : nx + x + 1],
                zsp[0:4, :],
            ],
            0,
        )
        bhi = b.astype(bf16).astype(f32)
        bm[x] = jnp.concatenate([bhi, b - bhi, bhi, jnp.zeros_like(b)], 0).astype(bf16)
        kept[x] = jnp.exp(-absorber[x])


def lost_kernel(s, spk, keep_part, bm, place, *rest, columns, groups, tail):
    parts = rest[:columns]
    am, keep, gathered = rest[-3:]
    sent = rest[columns : columns + groups]
    more = rest[columns + groups : -3]
    final = steps_of(groups)[-1]
    nx, n, wz = keep_part.shape
    own = lax.axis_index("gz")
    bits = paired_by_bits(columns)
    for step, part in enumerate(parts):
        gathered[step] = part[...]

    def index(j):
        return j ^ own if bits else (own - j + columns) % columns

    left, right = chain(gathered, nx, own, keep, index)
    for x in range(nx):
        a = jnp.concatenate(
            [spk[0:4, :]] + [v[x : x + 1] for v in (left[0], left[1], right[0], right[1])], 0
        )
        ahi = a.astype(bf16).astype(f32)
        am[x] = jnp.concatenate([ahi, ahi, a - ahi, jnp.zeros_like(a)], 0).astype(bf16)
    rows = place.shape[1] // groups
    sides = 1 if tail is None else 2
    width = rows if tail is None else 2 * tail + 8
    for step in range(nx // sides):
        parts = []
        for side in range(sides):
            x = step * sides + side
            field = s[x * n : (x + 1) * n, :] + mm(am[x], bm[x], TN)
            kept = keep_part[x]
            folded = []
            for part in range(2):
                value = field[:, part * wz : (part + 1) * wz]
                value = value - value * kept
                folded.append(sum(value[:, k * KZ : (k + 1) * KZ] for k in range(wz // KZ)))
            hi, lo = split(jnp.concatenate(folded, 1))
            parts.append(mm(place[side], jnp.concatenate([hi, lo], 0)))
        for g in range(groups):
            top = g * rows
            at = step * width
            target = sent[g]
            if g == final and at >= target.shape[0]:
                at = at - target.shape[0]
                target = more[0]
            if tail is None:
                target[at : at + rows, :] = parts[0][top : top + rows]
            else:
                target[at : at + tail, :] = parts[0][top : top + tail]
                target[at + tail : at + 2 * tail, :] = parts[1][top : top + tail]
                target[at + 2 * tail : at + 2 * tail + 8, :] = (
                    parts[0][top + tail : top + rows] + parts[1][top + tail : top + rows]
                )


def damp_kernel(s, keep_part, am, bm, damped, dv, sems):
    nx, n, wz = keep_part.shape
    copies = []
    for x in range(nx):
        field = s[x * n : (x + 1) * n, :] + mm(am[x], bm[x], TN)
        kept = keep_part[x]
        for part in range(2):
            dv[x, part] = field[:, part * wz : (part + 1) * wz] * kept
            copies.append(
                pltpu.make_async_copy(dv.at[x, part], damped.at[part, x], sems.at[x, part])
            )
            copies[-1].start()
    for copy in copies:
        copy.wait()


def plane_rows(block, x, rows, tail):
    if tail is None:
        return block[x * rows : (x + 1) * rows, :]
    at = x // 2 * (2 * tail + 8)
    side = x % 2
    return jnp.concatenate(
        [
            block[at + side * tail : at + (side + 1) * tail, :],
            block[at + 2 * tail : at + 2 * tail + 8, :],
        ],
        0,
    )


def combine(u):
    half = u.shape[0] // 2
    real = u[0:half, 0:KZ] - u[half:, KZ:]
    imag = u[0:half, KZ:] + u[half:, 0:KZ]
    return real, imag


def early_kernel(yt, ez, *rest, tail):
    count = len(rest) - 2
    got, (out, moved) = rest[:count], rest[count:]
    rows = yt.shape[3] // count
    sides = 1 if tail is None else 2
    for g in range(count):
        moved[g] = mm3(split(got[g][...]), (ez[0], ez[1]))
    for x in range(out.shape[0]):
        block = jnp.concatenate([plane_rows(moved[g], x, rows, tail) for g in range(count)], 0)
        side = x % sides
        real, imag = combine(mm3((yt[side, 0], yt[side, 1]), split(block)))
        out[x, :, 0:KZ] = real
        out[x, :, KZ:] = imag


def late_kernel(ylast, ez, early, vol, *rest, tail, first):
    out, moved, ov, sems = rest[-4:]
    sources = moved.shape[0]
    height = moved.shape[1]
    count = ov.shape[0]
    rows = ylast.shape[2] // (3 * sources)
    sides = 1 if tail is None else 2
    top = first * height // count
    for at in range(sources):
        got = rest[at]
        block = got[...] if at == sources - 1 else got[top : top + height, :]
        moved[at] = mm3(split(block), (ez[0], ez[1]))
    copies = []
    for x in range(count):
        block = [plane_rows(moved[at], x, rows, tail) for at in range(sources)]
        hi, lo = split(jnp.concatenate(block, 0))
        real, imag = combine(mm(ylast[x % sides], jnp.concatenate([hi, lo, hi], 0)))
        real = real + early[first + x, :, 0:KZ]
        imag = imag + early[first + x, :, KZ:]
        ov[x, 0] = vol[0] * real - vol[1] * imag
        ov[x, 1] = vol[0] * imag + vol[1] * real
        for part in range(2):
            copies.append(
                pltpu.make_async_copy(ov.at[x, part], out.at[part, first + x], sems.at[x, part])
            )
            copies[-1].start()
    for copy in copies:
        copy.wait()


def late_of(groups):
    return min(2, groups - 1)


def steps_of(groups):
    return list(range(1, groups))


def halves(table):
    exact = np.asarray(table, np.float64)
    hi = exact.astype(jnp.bfloat16)
    lo = (exact - hi.astype(np.float64)).astype(jnp.bfloat16)
    return np.stack([hi, lo])


def transform_tables():
    n = np.arange(KY)
    angle = 2.0 * np.pi / KY * (np.outer(n, n) % KY) - np.pi * (n % 2)[None, :]
    ytab = halves(np.concatenate([np.cos(angle), -np.sin(angle)], 0))
    n = np.arange(KZ)
    angle = 2.0 * np.pi / KZ * (np.outer(n, n) % KZ) - np.pi * (n % 2)[:, None]
    er, ei = np.cos(angle), -np.sin(angle)
    ztab = halves(np.block([[er, ei], [-ei, er]]))
    return ytab, ztab


def sds(*shape, dtype=f32):
    return jax.ShapeDtypeStruct(shape, dtype)


def body(
    wavefunction,
    absorber,
    row_inverse,
    column_inverse,
    link_terms,
    shell_blocks,
    owner_map,
    volkov_phase,
):
    nx, wy, wz = wavefunction.shape[1:]
    groups = lax.axis_size("gy")
    columns = lax.axis_size("gz")
    shell = shell_blocks.shape[2]
    capacity = 2 * ((shell + groups - 1) // groups)
    sent = capacity * BY
    paired = sent % 8 == 4 and nx % 2 == 0
    tail = sent - 4 if paired else None
    rows = (sent + 7) // 8 * 8
    sides = 2 if paired else 1
    per_plane = sent if paired else rows
    listed = shell_blocks[0]
    owners = owner_map[0, :, :, 0]
    ytab, ztab = transform_tables()
    norm = 1.0 / math.sqrt(wy * wz)

    tall = 4 * (wz // 128) * nx + EDGE
    pay, spk, wv, yv, zv, iv, ov = pl.pallas_call(
        row_edges_kernel,
        in_specs=[SM] + [AN] * 5,
        out_specs=[VM] * 7,
        out_shape=[
            sds(1, tall, 128),
            sds(8, wy),
            sds(2, nx, wy, wz),
            sds(2, wy, wy),
            sds(2, wz, wz),
            sds(*listed.shape, dtype=jnp.int32),
            sds(*owners.shape, dtype=jnp.int32),
        ],
        scratch_shapes=[
            pltpu.VMEM((tall - EDGE, 8, 128), f32),
            pltpu.SemaphoreType.DMA((nx,)),
            pltpu.SemaphoreType.DMA,
            pltpu.SemaphoreType.DMA((3,)),
        ],
        compiler_params=LIMIT,
        name="row_edges",
    )(*far(link_terms, wavefunction, row_inverse, column_inverse, listed, owners))

    inner = inner_of(groups) if paired_by_bits(groups) else groups
    outer = groups // inner
    if paired_by_bits(groups):
        lines = [pay]
        for step in range(1, outer):
            lines.append(exchange(pay, step * inner, groups))
    else:
        lines = [lax.all_gather(pay[0], "gy")]

    th, tl = pl.pallas_call(
        solve_rows_kernel,
        in_specs=[VM] * 2,
        out_specs=[VM] * 2,
        out_shape=[sds(nx * wy, 2 * wz, dtype=bf16)] * 2,
        scratch_shapes=[pltpu.VMEM((2 * wy, 2 * wy), bf16)] * 2,
        compiler_params=LIMIT,
        name="solve_rows",
    )(wv, yv)

    first = lines[-1]
    if paired_by_bits(groups):
        joined = pl.pallas_call(
            join_kernel,
            in_specs=[VM] * outer + [AN],
            out_specs=VM,
            out_shape=sds(outer, tall, 128),
            compiler_params=LIMIT,
            name="join",
        )(*lines, th)
        gathered = [joined] + [exchange(joined, step, groups) for step in range(1, inner)]
    else:
        gathered = lines

    edge, zsp, zed, zh, zl, place = pl.pallas_call(
        lambda *refs: prepare_kernel(*refs, tail=tail),
        in_specs=[SM, VM, VM, VM, AN],
        out_specs=[VM] * 6,
        out_shape=[
            sds(8, 2 * wz),
            sds(8, 2 * wz),
            sds(EDGE, wy),
            sds(2 * wz, 2 * wz, dtype=bf16),
            sds(2 * wz, 2 * wz, dtype=bf16),
            sds(sides, groups * rows, 2 * wy, dtype=bf16),
        ],
        compiler_params=LIMIT,
        name="prepare",
    )(*far(link_terms), zv, iv, ov, first)

    s, base = pl.pallas_call(
        solve_columns_kernel,
        in_specs=[VM] * 4,
        out_specs=[VM] * 2,
        out_shape=[sds(nx * wy, 2 * wz), sds(4 * nx, wy)],
        compiler_params=LIMIT,
        name="solve_columns",
    )(th, tl, zh, zl)

    lam, payz = pl.pallas_call(
        row_chain_kernel,
        in_specs=[VM] * (4 + len(gathered)),
        out_specs=[VM] * 2,
        out_shape=[sds(2 * nx, 2 * wz), sds(4 * nx + EDGE, wy)],
        scratch_shapes=[
            pltpu.VMEM((groups, 6 * (wz // 128) * nx, 128), f32),
            pltpu.VMEM((groups, tall, 128), f32),
        ],
        compiler_params=LIMIT,
        name="row_chain",
    )(*gathered, base, edge, zed, spk)

    edges = [payz]
    for step in range(1, columns):
        edges.append(exchange(payz, step, columns, "gz"))

    bm, kept = pl.pallas_call(
        ready_kernel,
        in_specs=[VM] * 5,
        out_specs=[VM] * 2,
        out_shape=[sds(nx, 32, 2 * wz, dtype=bf16), sds(nx, wy, wz)],
        scratch_shapes=[pltpu.VMEM((2 * nx, 2 * wz), f32)],
        compiler_params=LIMIT,
        name="ready",
    )(lam, zh, zl, zsp, absorber)

    height = nx * per_plane
    order = steps_of(groups)
    cuts = 2 if nx // sides % 2 == 0 else 1
    *sent, am = pl.pallas_call(
        lambda *refs: lost_kernel(*refs, columns=columns, groups=groups, tail=tail),
        in_specs=[VM] * (5 + columns),
        out_specs=[VM] * (groups + cuts),
        out_shape=[sds(height // (cuts if g == order[-1] else 1), 2 * KZ) for g in range(groups)]
        + [sds(height // cuts, 2 * KZ)] * (cuts - 1)
        + [sds(nx, 32, wy, dtype=bf16)],
        scratch_shapes=[
            pltpu.VMEM((columns, 6 * nx, wy), f32),
            pltpu.VMEM((columns, 4 * nx + EDGE, wy), f32),
        ],
        compiler_params=LIMIT,
        name="lost",
    )(s, spk, kept, bm, place, *edges)

    late = late_of(groups)
    got = [sent[0]] + [exchange(sent[step], step, groups) for step in order[:-1]]
    lasts = [exchange(part, order[-1], groups) for part in [sent[order[-1]]] + sent[groups:]]

    yt, ylast, vol = pl.pallas_call(
        lambda *refs: table_kernel(*refs, tail=tail, norm=norm),
        in_specs=[VM] * 4,
        out_specs=[VM] * 3,
        out_shape=[
            sds(sides, 2, 2 * KY, (groups - late) * rows, dtype=bf16),
            sds(sides, 2 * KY, 3 * late * rows, dtype=bf16),
            sds(2, KY, KZ),
        ],
        scratch_shapes=[
            pltpu.VMEM((groups * rows, KY), f32),
            pltpu.VMEM(owners.shape, jnp.int32),
            pltpu.VMEM(owners.shape, f32),
        ],
        compiler_params=LIMIT,
        name="tables",
    )(listed, owners, jnp.asarray(ytab), volkov_phase)

    damped = pl.pallas_call(
        damp_kernel,
        in_specs=[VM] * 4,
        out_specs=AN,
        out_shape=sds(2, nx, wy, wz),
        scratch_shapes=[
            pltpu.VMEM((nx, 2, wy, wz), f32),
            pltpu.SemaphoreType.DMA((nx, 2)),
        ],
        compiler_params=LIMIT,
        name="damp",
    )(s, kept, am, bm)

    early = pl.pallas_call(
        lambda *refs: early_kernel(*refs, tail=tail),
        in_specs=[VM] * (groups - late + 2),
        out_specs=VM,
        out_shape=sds(nx, KY, 2 * KZ),
        scratch_shapes=[pltpu.VMEM((groups - late, height, 2 * KZ), f32)],
        compiler_params=LIMIT,
        name="early",
    )(yt, jnp.asarray(ztab), *got[: groups - late])

    spectrum = []
    first = 0
    for block in lasts:
        count = block.shape[0] // per_plane
        spectrum = [
            pl.pallas_call(
                lambda *refs, first=first: late_kernel(*refs, tail=tail, first=first),
                in_specs=[VM] * (4 + late) + [AN] * len(spectrum),
                out_specs=AN,
                out_shape=sds(2, nx, KY, KZ),
                scratch_shapes=[
                    pltpu.VMEM((late, *block.shape), f32),
                    pltpu.VMEM((count, 2, KY, KZ), f32),
                    pltpu.SemaphoreType.DMA((count, 2)),
                ],
                input_output_aliases={4 + late: 0} if spectrum else {},
                compiler_params=LIMIT,
                name="late",
            )(ylast, jnp.asarray(ztab), early, vol, *got[groups - late :], block, *far(*spectrum))
        ]
        first = first + count
    (spectrum,) = spectrum
    return damped, spectrum


def solution(mesh):
    placed = (
        P(None, None, "gy", "gz"),
        P(None, "gy", "gz"),
        P(None, "gy", None),
        P(),
        P(),
        P("gz", None, None),
        P("gz", None, None, None),
        P(),
    )
    return jax.shard_map(
        body,
        mesh=mesh,
        in_specs=placed,
        out_specs=(P(None, None, "gy", "gz"), P(None, "gy", "gz", None)),
        check_vma=False,
    )
```

```python
import math

import jax
import jax.numpy as jnp
import numpy as np
from jax import lax
from jax.experimental import pallas as pl
from jax.experimental.pallas import tpu as pltpu
from jax.sharding import PartitionSpec as P


BY = 2
KY = 128
KZ = 128
EDGE = 8
MBLOCK = 4

f32 = jnp.float32
bf16 = jnp.bfloat16
NN = (((1,), (0,)), ((), ()))
NT = (((1,), (1,)), ((), ()))
TN = (((0,), (0,)), ((), ()))


def mm(a, b, dims=NN):
    return lax.dot_general(a, b, dims, preferred_element_type=f32)


def split(a):
    hi = a.astype(bf16)
    return hi, (a - hi.astype(f32)).astype(bf16)


def mm3(a, b, dims=NN):
    return mm(a[0], b[0], dims) + mm(a[0], b[1], dims) + mm(a[1], b[0], dims)


def cmul(a, b):
    return (a[0] * b[0] - a[1] * b[1], a[0] * b[1] + a[1] * b[0])


def cdiv(a, b):
    modulus = b[0] * b[0] + b[1] * b[1]
    return ((a[0] * b[0] + a[1] * b[1]) / modulus, (a[1] * b[0] - a[0] * b[1]) / modulus)


def cadd(a, b):
    return (a[0] + b[0], a[1] + b[1])


def put(hi_ref, lo_ref, rows, cols, value):
    hi, lo = split(value)
    hi_ref[rows, cols] = hi
    lo_ref[rows, cols] = lo


def spikes_of(transposed, link, sweep):
    last = transposed[0].shape[0] - 1
    left = cmul(
        (link[sweep, 0, 0], link[sweep, 0, 1]), (transposed[0][0:1], transposed[1][0:1])
    )
    right = cmul(
        (link[sweep, 1, 0], link[sweep, 1, 1]),
        (transposed[0][last : last + 1], transposed[1][last : last + 1]),
    )
    return left, right


def edge_rows(left, right, lanes):
    last = left[0].shape[1] - 1
    rows = []
    for spike in (left, right):
        for at in (0, last):
            for part in spike:
                rows.append(jnp.broadcast_to(part[:, at : at + 1], (1, lanes)))
    return rows


VM = pl.BlockSpec(memory_space=pltpu.VMEM)
SM = pl.BlockSpec(memory_space=pltpu.SMEM)
AN = pl.BlockSpec(memory_space=pl.ANY)
LIMIT = pltpu.CompilerParams(vmem_limit_bytes=20 << 20)


def far(*values):
    return [pltpu.with_memory_space_constraint(value, pltpu.HBM) for value in values]


def paired_by_bits(groups):
    return groups & (groups - 1) == 0


def slot_of(owner, me, groups):
    return owner ^ me if paired_by_bits(groups) else (owner - me + groups) % groups


def source_of(step, me, groups):
    return me ^ step if paired_by_bits(groups) else (me - step + groups) % groups


def exchange(value, step, groups, axis="gy"):
    pairs = [
        (i, i ^ step if paired_by_bits(groups) else (i + step) % groups) for i in range(groups)
    ]
    return lax.ppermute(value, axis, pairs)


def inner_of(groups):
    bits = groups.bit_length() - 1
    return 1 << (bits // 2)


def row_edges_kernel(
    terms, w, y, col, listed, owners, ps, spk, wv, yv, zv, iv, ov, link, sums, sems, ysem, zsems, lsem
):
    nx, n, width = wv.shape[1:]
    ycopy = pltpu.make_async_copy(y, yv, ysem)
    ycopy.start()
    linked = pltpu.make_async_copy(terms, link, lsem)
    linked.start()
    copies = []
    for x in range(nx):
        copies.append(pltpu.make_async_copy(w.at[:, x], wv.at[:, x], sems.at[x]))
        copies[x].start()
    wz = zv.shape[1]
    rank = lax.axis_index("gz")
    loads = [
        pltpu.make_async_copy(col.at[:, pl.ds(rank * wz, wz), :], zv, zsems.at[0]),
        pltpu.make_async_copy(listed, iv, zsems.at[1]),
        pltpu.make_async_copy(owners, ov, zsems.at[2]),
    ]
    for load in loads:
        load.start()
    ycopy.wait()
    linked.wait()
    rt = yv[0].T
    it = yv[1].T
    left, right = spikes_of((rt, it), link, 0)
    for at, row in enumerate((left[0], left[1], right[0], right[1])):
        spk[at : at + 1, :] = row
    spk[4:8, :] = jnp.zeros((4, n), f32)
    lanes = ps.shape[2]
    count = width // lanes * nx
    for at, row in enumerate(edge_rows(left, right, lanes)):
        ps[0, 4 * count + at : 4 * count + at + 1, :] = row
    coef = [
        (
            jnp.broadcast_to(rt[:, row : row + 1], (n, lanes)),
            jnp.broadcast_to(it[:, row : row + 1], (n, lanes)),
        )
        for row in (0, n - 1)
    ]
    for x in range(nx):
        copies[x].wait()
        for k in range(width // lanes):
            cols = slice(k * lanes, (k + 1) * lanes)
            wr = wv[0, x, :, cols]
            wi = wv[1, x, :, cols]
            for side, (cr, ci) in enumerate(coef):
                real = cr * wr - ci * wi
                imag = cr * wi + ci * wr
                at = 2 * side * count + k * nx + x
                sums[at] = jnp.sum(real.reshape(n // 8, 8, lanes), axis=0)
                sums[at + count] = jnp.sum(imag.reshape(n // 8, 8, lanes), axis=0)
    ps[0, 0 : 4 * count, :] = jnp.sum(sums[...], axis=1)
    for load in loads:
        load.wait()


def join_kernel(*refs):
    *parts, _, out = refs
    for at, part in enumerate(parts):
        out[at] = part[0]


def route(listed, owners, place, tail):
    me = lax.axis_index("gy")
    groups, count = owners.shape
    rows = place.shape[1] // groups
    ny = place.shape[2] // 2
    ids = listed[pl.ds(me, 1), :]
    own = owners[pl.ds(me, 1), :]
    slot = slot_of(own, me, groups)
    hot = (lax.broadcasted_iota(jnp.int32, (groups, count), 0) == own).astype(f32)
    upper = (
        lax.broadcasted_iota(jnp.int32, (count, count), 0)
        < lax.broadcasted_iota(jnp.int32, (count, count), 1)
    ).astype(f32).astype(bf16)
    earlier = mm(hot.astype(bf16), upper)
    rank = jnp.sum(hot * earlier, axis=0, keepdims=True).astype(jnp.int32)
    at = lax.broadcasted_iota(jnp.int32, (groups * rows, count), 0)
    n = lax.broadcasted_iota(jnp.int32, (ny, count), 0)
    for side in range(place.shape[0]):
        total = jnp.zeros((groups * rows, ny), f32)
        for b in range(BY):
            row = rank * BY + b
            if tail is not None and side:
                row = row + jnp.where(row >= tail, 4, 0)
            here = (at == slot * rows + row).astype(f32).astype(bf16)
            there = (n == ids * BY + b).astype(f32).astype(bf16)
            total = total + mm(here, there, NT)
        place[side, :, 0:ny] = total.astype(bf16)
        place[side, :, ny : 2 * ny] = total.astype(bf16)


def solve_rows_kernel(w, y, th, tl, yh, yl):
    nx, n, wz = w.shape[1:]
    yr = y[0]
    yi = y[1]
    for part, value in ((0, (yr, -yi)), (1, (yi, yr))):
        for half in range(2):
            hi, lo = split(value[half])
            yh[part * n : (part + 1) * n, half * n : (half + 1) * n] = hi
            yl[part * n : (part + 1) * n, half * n : (half + 1) * n] = lo
    for x in range(nx):
        wx = split(w[:, x].reshape(2 * n, wz))
        hi, lo = split(mm3((yh[...], yl[...]), wx))
        rows = slice(x * n, (x + 1) * n)
        th[rows, 0:wz] = hi[0:n]
        th[rows, wz : 2 * wz] = hi[n : 2 * n]
        tl[rows, 0:wz] = lo[0:n]
        tl[rows, wz : 2 * wz] = lo[n : 2 * n]


def prepare_kernel(link, zv, iv, ov, after, edge, zsp, zed, zh, zl, place, *, tail):
    wz = zv.shape[1]
    zr = zv[0]
    zi = zv[1]
    rt = zr.T
    it = zi.T
    put(zh, zl, slice(0, wz), slice(0, wz), rt)
    put(zh, zl, slice(0, wz), slice(wz, 2 * wz), it)
    put(zh, zl, slice(wz, 2 * wz), slice(0, wz), -it)
    put(zh, zl, slice(wz, 2 * wz), slice(wz, 2 * wz), rt)
    for at, (row, turned) in enumerate(((0, False), (0, True), (wz - 1, False), (wz - 1, True))):
        edge[at : at + 1, 0:wz] = (zi if turned else zr)[row : row + 1]
        edge[at : at + 1, wz : 2 * wz] = zr[row : row + 1] if turned else -zi[row : row + 1]
    edge[4:8, :] = jnp.zeros((4, 2 * wz), f32)
    left, right = spikes_of((rt, it), link, 1)
    for at, spike in enumerate((left, right)):
        zsp[2 * at : 2 * at + 1, 0:wz] = spike[0]
        zsp[2 * at : 2 * at + 1, wz : 2 * wz] = spike[1]
        zsp[2 * at + 1 : 2 * at + 2, 0:wz] = -spike[1]
        zsp[2 * at + 1 : 2 * at + 2, wz : 2 * wz] = spike[0]
    zsp[4:8, :] = jnp.zeros((4, 2 * wz), f32)
    for at, row in enumerate(edge_rows(left, right, zed.shape[1])):
        zed[at : at + 1, :] = row
    route(iv, ov, place, tail)


def solve_columns_kernel(th, tl, zh, zl, s, base):
    n = base.shape[1]
    nx = base.shape[0] // 4
    wz = s.shape[1] // 2
    block = MBLOCK * n
    for m in range(nx // MBLOCK):
        rows = slice(m * block, (m + 1) * block)
        s[rows, :] = mm3((th[rows, :], tl[rows, :]), (zh[...], zl[...]))
    lane = lax.broadcasted_iota(jnp.int32, (n, 128), 1)
    picked = jnp.zeros((n, 128), f32)
    for at, column in enumerate((0, wz, wz - 1, 2 * wz - 1)):
        for x in range(nx):
            value = s[x * n : (x + 1) * n, column : column + 1]
            picked = jnp.where(lane == at * nx + x, value, picked)
    base[...] = picked.T[0 : 4 * nx]


def chain(gathered, nx, own, keep, index=lambda j: j):
    groups = gathered.shape[0]
    lanes = gathered.shape[2]
    zero = jnp.zeros((nx, lanes), f32)

    def read(j):
        block = gathered[index(j)]
        rows = [block[at * nx : (at + 1) * nx] for at in range(4)]
        edges = [
            jnp.broadcast_to(block[4 * nx + at : 4 * nx + at + 1], (nx, lanes))
            for at in range(EDGE)
        ]
        head, tail = (rows[0], rows[1]), (rows[2], rows[3])
        return head, tail, [(edges[2 * at], edges[2 * at + 1]) for at in range(4)]

    def forward(j, carry):
        coupling, carried = (carry[0], carry[1]), (carry[2], carry[3])
        head, tail, (lead_left, tail_left, lead_right, tail_right) = read(j)
        product = cmul(lead_left, coupling)
        pivot = (1.0 - product[0], -product[1])
        gain = cdiv(tail_left, pivot)
        for at, value in enumerate(coupling + carried + pivot):
            keep[j, at * nx : (at + 1) * nx, :] = value
        coupling_next = cadd(tail_right, cmul(gain, cmul(lead_right, coupling)))
        carried_next = cadd(
            cmul(gain, carried), cadd(tail, cmul(cmul(gain, coupling), head))
        )
        return coupling_next + carried_next

    def solved(j, head_next):
        head, _, (lead_left, _, lead_right, _) = read(j)
        kept = keep[j]
        values = [kept[at * nx : (at + 1) * nx] for at in range(6)]
        coupling, carried, pivot = (
            (values[0], values[1]),
            (values[2], values[3]),
            (values[4], values[5]),
        )
        offset = cdiv(cadd(head, cmul(lead_left, carried)), pivot)
        factor = cdiv(lead_right, pivot)
        value = cadd(offset, cmul(factor, head_next))
        return value, cadd(carried, cmul(coupling, value))

    lax.fori_loop(0, groups, forward, (zero, zero, zero, zero))
    following = lax.fori_loop(
        0,
        groups - 1 - own,
        lambda lap, head_next: solved(groups - 1 - lap, head_next)[0],
        (zero, zero),
    )
    return solved(own, following)[1], following


def row_chain_kernel(*refs):
    *parts, base, edge, zed, spk, lam, pay, keep, gathered = refs
    nx = base.shape[0] // 4
    own = lax.axis_index("gy")
    bits = len(parts) > 1
    for b, part in enumerate(parts):
        for a in range(part.shape[0]):
            gathered[a * len(parts) + b] = part[a]
    count = (gathered.shape[1] - EDGE) // 4
    sides = chain(gathered, count, own, keep, (lambda j: j ^ own) if bits else (lambda j: j))
    stacked = jnp.concatenate(
        [
            jnp.concatenate(
                [part[k : k + nx] for part in side for k in range(0, count, nx)], 1
            )
            for side in sides
        ],
        0,
    )
    lam[...] = stacked
    spikes = ((spk[0:1, :], spk[1:2, :]), (spk[2:3, :], spk[3:4, :]))
    for at in range(2):
        value = [base[(2 * at + part) * nx : (2 * at + part + 1) * nx, :] for part in range(2)]
        moved = [
            jnp.sum(stacked * edge[2 * at + part : 2 * at + part + 1, :], axis=1, keepdims=True)
            for part in range(2)
        ]
        for side in range(2):
            rows = slice(side * nx, (side + 1) * nx)
            value = cadd(value, cmul((moved[0][rows], moved[1][rows]), spikes[side]))
        pay[2 * at * nx : (2 * at + 1) * nx, :] = value[0]
        pay[(2 * at + 1) * nx : (2 * at + 2) * nx, :] = value[1]
    pay[4 * nx : 4 * nx + EDGE, :] = zed[...]


def table_kernel(listed, owners, table, phase, *rest, tail, norm):
    yt, ylast, vol, q, rank, mine = rest
    me = lax.axis_index("gy")
    groups, count = owners.shape
    rows = q.shape[0] // groups
    ny = table.shape[2]
    mine[...] = (owners[...] == me).astype(f32)
    upper = (
        lax.broadcasted_iota(jnp.int32, (count, count), 0)
        < lax.broadcasted_iota(jnp.int32, (count, count), 1)
    ).astype(f32).astype(bf16)
    rank[...] = mm(mine[...].astype(bf16), upper).astype(jnp.int32)
    at = lax.broadcasted_iota(jnp.int32, (rows, count), 0)
    n = lax.broadcasted_iota(jnp.int32, (ny, count), 0)
    order = steps_of(groups)
    for side in range(yt.shape[0]):
        for place, step in enumerate([0] + order):
            g = source_of(step, me, groups)
            own = jnp.broadcast_to(mine[pl.ds(g, 1), :], at.shape)
            total = jnp.zeros((rows, ny), f32)
            for b in range(BY):
                row = rank[pl.ds(g, 1), :] * BY + b
                if tail is not None and side:
                    row = row + jnp.where(row >= tail, 4, 0)
                here = jnp.where(at == row, own, 0.0)
                there = (n == listed[pl.ds(g, 1), :] * BY + b).astype(f32).astype(bf16)
                total = total + mm(here.astype(bf16), there, NT)
            q[place * rows : (place + 1) * rows, :] = total
        cut = (groups - late_of(groups)) * rows
        first = q[0:cut, :].astype(bf16)
        last = q[cut : groups * rows, :].astype(bf16)
        for part in range(2):
            yt[side, part] = mm(table[part], first, NT).astype(bf16)
        hi = mm(table[0], last, NT)
        lo = mm(table[1], last, NT)
        ylast[side] = jnp.concatenate([hi, hi, lo], 1).astype(bf16)
    vol[0] = jnp.cos(phase[...]) * norm
    vol[1] = jnp.sin(phase[...]) * norm


def ready_kernel(lam, zh, zl, zsp, absorber, bm, kept, moved):
    nx = lam.shape[0] // 2
    wz = lam.shape[1] // 2
    moved[...] = mm3(split(lam[...]), (zh[...], zl[...]))
    swapped = jnp.concatenate([-moved[:, wz : 2 * wz], moved[:, 0:wz]], 1)
    for x in range(nx):
        b = jnp.concatenate(
            [
                moved[x : x + 1, :],
                swapped[x : x + 1],
                moved[nx + x : nx + x + 1, :],
                swapped[nx + x : nx + x + 1],
                zsp[0:4, :],
            ],
            0,
        )
        bhi = b.astype(bf16).astype(f32)
        bm[x] = jnp.concatenate([bhi, b - bhi, bhi, jnp.zeros_like(b)], 0).astype(bf16)
        kept[x] = jnp.exp(-absorber[x])


def lost_kernel(s, spk, keep_part, bm, place, *rest, columns, groups, tail):
    parts = rest[:columns]
    am, keep, gathered = rest[-3:]
    sent = rest[columns : columns + groups]
    more = rest[columns + groups : -3]
    final = steps_of(groups)[-1]
    nx, n, wz = keep_part.shape
    own = lax.axis_index("gz")
    bits = paired_by_bits(columns)
    for step, part in enumerate(parts):
        gathered[step] = part[...]

    def index(j):
        return j ^ own if bits else (own - j + columns) % columns

    left, right = chain(gathered, nx, own, keep, index)
    for x in range(nx):
        a = jnp.concatenate(
            [spk[0:4, :]] + [v[x : x + 1] for v in (left[0], left[1], right[0], right[1])], 0
        )
        ahi = a.astype(bf16).astype(f32)
        am[x] = jnp.concatenate([ahi, ahi, a - ahi, jnp.zeros_like(a)], 0).astype(bf16)
    rows = place.shape[1] // groups
    sides = 1 if tail is None else 2
    width = rows if tail is None else 2 * tail + 8
    for step in range(nx // sides):
        parts = []
        for side in range(sides):
            x = step * sides + side
            field = s[x * n : (x + 1) * n, :] + mm(am[x], bm[x], TN)
            kept = keep_part[x]
            folded = []
            for part in range(2):
                value = field[:, part * wz : (part + 1) * wz]
                value = value - value * kept
                folded.append(sum(value[:, k * KZ : (k + 1) * KZ] for k in range(wz // KZ)))
            hi, lo = split(jnp.concatenate(folded, 1))
            parts.append(mm(place[side], jnp.concatenate([hi, lo], 0)))
        for g in range(groups):
            top = g * rows
            at = step * width
            target = sent[g]
            if g == final and at >= target.shape[0]:
                at = at - target.shape[0]
                target = more[0]
            if tail is None:
                target[at : at + rows, :] = parts[0][top : top + rows]
            else:
                target[at : at + tail, :] = parts[0][top : top + tail]
                target[at + tail : at + 2 * tail, :] = parts[1][top : top + tail]
                target[at + 2 * tail : at + 2 * tail + 8, :] = (
                    parts[0][top + tail : top + rows] + parts[1][top + tail : top + rows]
                )


def damp_kernel(s, keep_part, am, bm, damped, dv, sems):
    nx, n, wz = keep_part.shape
    copies = []
    for x in range(nx):
        field = s[x * n : (x + 1) * n, :] + mm(am[x], bm[x], TN)
        kept = keep_part[x]
        for part in range(2):
            dv[x, part] = field[:, part * wz : (part + 1) * wz] * kept
            copies.append(
                pltpu.make_async_copy(dv.at[x, part], damped.at[part, x], sems.at[x, part])
            )
            copies[-1].start()
    for copy in copies:
        copy.wait()


def plane_rows(block, x, rows, tail):
    if tail is None:
        return block[x * rows : (x + 1) * rows, :]
    at = x // 2 * (2 * tail + 8)
    side = x % 2
    return jnp.concatenate(
        [
            block[at + side * tail : at + (side + 1) * tail, :],
            block[at + 2 * tail : at + 2 * tail + 8, :],
        ],
        0,
    )


def combine(u):
    half = u.shape[0] // 2
    real = u[0:half, 0:KZ] - u[half:, KZ:]
    imag = u[0:half, KZ:] + u[half:, 0:KZ]
    return real, imag


def early_kernel(yt, ez, *rest, tail):
    count = len(rest) - 2
    got, (out, moved) = rest[:count], rest[count:]
    rows = yt.shape[3] // count
    sides = 1 if tail is None else 2
    for g in range(count):
        moved[g] = mm3(split(got[g][...]), (ez[0], ez[1]))
    for x in range(out.shape[0]):
        block = jnp.concatenate([plane_rows(moved[g], x, rows, tail) for g in range(count)], 0)
        side = x % sides
        real, imag = combine(mm3((yt[side, 0], yt[side, 1]), split(block)))
        out[x, :, 0:KZ] = real
        out[x, :, KZ:] = imag


def late_kernel(ylast, ez, early, vol, *rest, tail, first):
    out, moved, ov, sems = rest[-4:]
    sources = moved.shape[0]
    height = moved.shape[1]
    count = ov.shape[0]
    rows = ylast.shape[2] // (3 * sources)
    sides = 1 if tail is None else 2
    top = first * height // count
    for at in range(sources):
        got = rest[at]
        block = got[...] if at == sources - 1 else got[top : top + height, :]
        moved[at] = mm3(split(block), (ez[0], ez[1]))
    copies = []
    for x in range(count):
        block = [plane_rows(moved[at], x, rows, tail) for at in range(sources)]
        hi, lo = split(jnp.concatenate(block, 0))
        real, imag = combine(mm(ylast[x % sides], jnp.concatenate([hi, lo, hi], 0)))
        real = real + early[first + x, :, 0:KZ]
        imag = imag + early[first + x, :, KZ:]
        ov[x, 0] = vol[0] * real - vol[1] * imag
        ov[x, 1] = vol[0] * imag + vol[1] * real
        for part in range(2):
            copies.append(
                pltpu.make_async_copy(ov.at[x, part], out.at[part, first + x], sems.at[x, part])
            )
            copies[-1].start()
    for copy in copies:
        copy.wait()


def late_of(groups):
    return min(2, groups - 1)


def steps_of(groups):
    return list(range(1, groups))


def halves(table):
    exact = np.asarray(table, np.float64)
    hi = exact.astype(jnp.bfloat16)
    lo = (exact - hi.astype(np.float64)).astype(jnp.bfloat16)
    return np.stack([hi, lo])


def transform_tables():
    n = np.arange(KY)
    angle = 2.0 * np.pi / KY * (np.outer(n, n) % KY) - np.pi * (n % 2)[None, :]
    ytab = halves(np.concatenate([np.cos(angle), -np.sin(angle)], 0))
    n = np.arange(KZ)
    angle = 2.0 * np.pi / KZ * (np.outer(n, n) % KZ) - np.pi * (n % 2)[:, None]
    er, ei = np.cos(angle), -np.sin(angle)
    ztab = halves(np.block([[er, ei], [-ei, er]]))
    return ytab, ztab


def sds(*shape, dtype=f32):
    return jax.ShapeDtypeStruct(shape, dtype)


def body(
    wavefunction,
    absorber,
    row_inverse,
    column_inverse,
    link_terms,
    shell_blocks,
    owner_map,
    volkov_phase,
):
    nx, wy, wz = wavefunction.shape[1:]
    groups = lax.axis_size("gy")
    columns = lax.axis_size("gz")
    shell = shell_blocks.shape[2]
    capacity = 2 * ((shell + groups - 1) // groups)
    sent = capacity * BY
    paired = sent % 8 == 4 and nx % 2 == 0
    tail = sent - 4 if paired else None
    rows = (sent + 7) // 8 * 8
    sides = 2 if paired else 1
    per_plane = sent if paired else rows
    listed = shell_blocks[0]
    owners = owner_map[0, :, :, 0]
    ytab, ztab = transform_tables()
    norm = 1.0 / math.sqrt(wy * wz)

    tall = 4 * (wz // 128) * nx + EDGE
    pay, spk, wv, yv, zv, iv, ov = pl.pallas_call(
        row_edges_kernel,
        in_specs=[AN] * 6,
        out_specs=[VM] * 7,
        out_shape=[
            sds(1, tall, 128),
            sds(8, wy),
            sds(2, nx, wy, wz),
            sds(2, wy, wy),
            sds(2, wz, wz),
            sds(*listed.shape, dtype=jnp.int32),
            sds(*owners.shape, dtype=jnp.int32),
        ],
        scratch_shapes=[
            pltpu.SMEM(link_terms.shape, f32),
            pltpu.VMEM((tall - EDGE, 8, 128), f32),
            pltpu.SemaphoreType.DMA((nx,)),
            pltpu.SemaphoreType.DMA,
            pltpu.SemaphoreType.DMA((3,)),
            pltpu.SemaphoreType.DMA,
        ],
        compiler_params=LIMIT,
        name="row_edges",
    )(*far(link_terms, wavefunction, row_inverse, column_inverse, listed, owners))

    inner = inner_of(groups) if paired_by_bits(groups) else groups
    outer = groups // inner
    if paired_by_bits(groups):
        lines = [pay]
        for step in range(1, outer):
            lines.append(exchange(pay, step * inner, groups))
    else:
        lines = [lax.all_gather(pay[0], "gy")]

    th, tl = pl.pallas_call(
        solve_rows_kernel,
        in_specs=[VM] * 2,
        out_specs=[VM] * 2,
        out_shape=[sds(nx * wy, 2 * wz, dtype=bf16)] * 2,
        scratch_shapes=[pltpu.VMEM((2 * wy, 2 * wy), bf16)] * 2,
        compiler_params=LIMIT,
        name="solve_rows",
    )(wv, yv)

    first = lines[-1]
    if paired_by_bits(groups):
        joined = pl.pallas_call(
            join_kernel,
            in_specs=[VM] * outer + [AN],
            out_specs=VM,
            out_shape=sds(outer, tall, 128),
            compiler_params=LIMIT,
            name="join",
        )(*lines, th)
        gathered = [joined] + [exchange(joined, step, groups) for step in range(1, inner)]
    else:
        gathered = lines

    edge, zsp, zed, zh, zl, place = pl.pallas_call(
        lambda *refs: prepare_kernel(*refs, tail=tail),
        in_specs=[SM, VM, VM, VM, AN],
        out_specs=[VM] * 6,
        out_shape=[
            sds(8, 2 * wz),
            sds(8, 2 * wz),
            sds(EDGE, wy),
            sds(2 * wz, 2 * wz, dtype=bf16),
            sds(2 * wz, 2 * wz, dtype=bf16),
            sds(sides, groups * rows, 2 * wy, dtype=bf16),
        ],
        compiler_params=LIMIT,
        name="prepare",
    )(*far(link_terms), zv, iv, ov, first)

    s, base = pl.pallas_call(
        solve_columns_kernel,
        in_specs=[VM] * 4,
        out_specs=[VM] * 2,
        out_shape=[sds(nx * wy, 2 * wz), sds(4 * nx, wy)],
        compiler_params=LIMIT,
        name="solve_columns",
    )(th, tl, zh, zl)

    lam, payz = pl.pallas_call(
        row_chain_kernel,
        in_specs=[VM] * (4 + len(gathered)),
        out_specs=[VM] * 2,
        out_shape=[sds(2 * nx, 2 * wz), sds(4 * nx + EDGE, wy)],
        scratch_shapes=[
            pltpu.VMEM((groups, 6 * (wz // 128) * nx, 128), f32),
            pltpu.VMEM((groups, tall, 128), f32),
        ],
        compiler_params=LIMIT,
        name="row_chain",
    )(*gathered, base, edge, zed, spk)

    edges = [payz]
    for step in range(1, columns):
        edges.append(exchange(payz, step, columns, "gz"))

    bm, kept = pl.pallas_call(
        ready_kernel,
        in_specs=[VM] * 5,
        out_specs=[VM] * 2,
        out_shape=[sds(nx, 32, 2 * wz, dtype=bf16), sds(nx, wy, wz)],
        scratch_shapes=[pltpu.VMEM((2 * nx, 2 * wz), f32)],
        compiler_params=LIMIT,
        name="ready",
    )(lam, zh, zl, zsp, absorber)

    height = nx * per_plane
    order = steps_of(groups)
    cuts = 2 if nx // sides % 2 == 0 else 1
    *sent, am = pl.pallas_call(
        lambda *refs: lost_kernel(*refs, columns=columns, groups=groups, tail=tail),
        in_specs=[VM] * (5 + columns),
        out_specs=[VM] * (groups + cuts),
        out_shape=[sds(height // (cuts if g == order[-1] else 1), 2 * KZ) for g in range(groups)]
        + [sds(height // cuts, 2 * KZ)] * (cuts - 1)
        + [sds(nx, 32, wy, dtype=bf16)],
        scratch_shapes=[
            pltpu.VMEM((columns, 6 * nx, wy), f32),
            pltpu.VMEM((columns, 4 * nx + EDGE, wy), f32),
        ],
        compiler_params=LIMIT,
        name="lost",
    )(s, spk, kept, bm, place, *edges)

    late = late_of(groups)
    got = [sent[0]] + [exchange(sent[step], step, groups) for step in order[:-1]]
    lasts = [exchange(part, order[-1], groups) for part in [sent[order[-1]]] + sent[groups:]]

    yt, ylast, vol = pl.pallas_call(
        lambda *refs: table_kernel(*refs, tail=tail, norm=norm),
        in_specs=[VM] * 4,
        out_specs=[VM] * 3,
        out_shape=[
            sds(sides, 2, 2 * KY, (groups - late) * rows, dtype=bf16),
            sds(sides, 2 * KY, 3 * late * rows, dtype=bf16),
            sds(2, KY, KZ),
        ],
        scratch_shapes=[
            pltpu.VMEM((groups * rows, KY), f32),
            pltpu.VMEM(owners.shape, jnp.int32),
            pltpu.VMEM(owners.shape, f32),
        ],
        compiler_params=LIMIT,
        name="tables",
    )(listed, owners, jnp.asarray(ytab), volkov_phase)

    damped = pl.pallas_call(
        damp_kernel,
        in_specs=[VM] * 4,
        out_specs=AN,
        out_shape=sds(2, nx, wy, wz),
        scratch_shapes=[
            pltpu.VMEM((nx, 2, wy, wz), f32),
            pltpu.SemaphoreType.DMA((nx, 2)),
        ],
        compiler_params=LIMIT,
        name="damp",
    )(s, kept, am, bm)

    early = pl.pallas_call(
        lambda *refs: early_kernel(*refs, tail=tail),
        in_specs=[VM] * (groups - late + 2),
        out_specs=VM,
        out_shape=sds(nx, KY, 2 * KZ),
        scratch_shapes=[pltpu.VMEM((groups - late, height, 2 * KZ), f32)],
        compiler_params=LIMIT,
        name="early",
    )(yt, jnp.asarray(ztab), *got[: groups - late])

    spectrum = []
    first = 0
    for block in lasts:
        count = block.shape[0] // per_plane
        spectrum = [
            pl.pallas_call(
                lambda *refs, first=first: late_kernel(*refs, tail=tail, first=first),
                in_specs=[VM] * (4 + late) + [AN] * len(spectrum),
                out_specs=AN,
                out_shape=sds(2, nx, KY, KZ),
                scratch_shapes=[
                    pltpu.VMEM((late, *block.shape), f32),
                    pltpu.VMEM((count, 2, KY, KZ), f32),
                    pltpu.SemaphoreType.DMA((count, 2)),
                ],
                input_output_aliases={4 + late: 0} if spectrum else {},
                compiler_params=LIMIT,
                name="late",
            )(ylast, jnp.asarray(ztab), early, vol, *got[groups - late :], block, *far(*spectrum))
        ]
        first = first + count
    (spectrum,) = spectrum
    return damped, spectrum


def solution(mesh):
    placed = (
        P(None, None, "gy", "gz"),
        P(None, "gy", "gz"),
        P(None, "gy", None),
        P(),
        P(),
        P("gz", None, None),
        P("gz", None, None, None),
        P(),
    )
    return jax.shard_map(
        body,
        mesh=mesh,
        in_specs=placed,
        out_specs=(P(None, None, "gy", "gz"), P(None, "gy", "gz", None)),
        check_vma=False,
    )
```

```python
import math

import jax
import jax.numpy as jnp
import numpy as np
from jax import lax
from jax.experimental import pallas as pl
from jax.experimental.pallas import tpu as pltpu
from jax.sharding import PartitionSpec as P


BY = 2
KY = 128
KZ = 128
EDGE = 8
MBLOCK = 4

f32 = jnp.float32
bf16 = jnp.bfloat16
NN = (((1,), (0,)), ((), ()))
NT = (((1,), (1,)), ((), ()))
TN = (((0,), (0,)), ((), ()))


def mm(a, b, dims=NN):
    return lax.dot_general(a, b, dims, preferred_element_type=f32)


def split(a):
    hi = a.astype(bf16)
    return hi, (a - hi.astype(f32)).astype(bf16)


def mm3(a, b, dims=NN):
    return mm(a[0], b[0], dims) + mm(a[0], b[1], dims) + mm(a[1], b[0], dims)


def cmul(a, b):
    return (a[0] * b[0] - a[1] * b[1], a[0] * b[1] + a[1] * b[0])


def cdiv(a, b):
    modulus = b[0] * b[0] + b[1] * b[1]
    return ((a[0] * b[0] + a[1] * b[1]) / modulus, (a[1] * b[0] - a[0] * b[1]) / modulus)


def cadd(a, b):
    return (a[0] + b[0], a[1] + b[1])


def put(hi_ref, lo_ref, rows, cols, value):
    hi, lo = split(value)
    hi_ref[rows, cols] = hi
    lo_ref[rows, cols] = lo


def spikes_of(transposed, previous, following):
    last = transposed[0].shape[0] - 1
    left = cmul(previous, (transposed[0][0:1], transposed[1][0:1]))
    right = cmul(following, (transposed[0][last : last + 1], transposed[1][last : last + 1]))
    return left, right


def edge_rows(left, right, lanes):
    last = left[0].shape[1] - 1
    rows = []
    for spike in (left, right):
        for at in (0, last):
            for part in spike:
                rows.append(jnp.broadcast_to(part[:, at : at + 1], (1, lanes)))
    return rows


VM = pl.BlockSpec(memory_space=pltpu.VMEM)
SM = pl.BlockSpec(memory_space=pltpu.SMEM)
AN = pl.BlockSpec(memory_space=pl.ANY)
LIMIT = pltpu.CompilerParams(vmem_limit_bytes=20 << 20)


def far(*values):
    return [pltpu.with_memory_space_constraint(value, pltpu.HBM) for value in values]


def paired_by_bits(groups):
    return groups & (groups - 1) == 0


def slot_of(owner, me, groups):
    return owner ^ me if paired_by_bits(groups) else (owner - me + groups) % groups


def source_of(step, me, groups):
    return me ^ step if paired_by_bits(groups) else (me - step + groups) % groups


def exchange(value, step, groups, axis="gy"):
    pairs = [
        (i, i ^ step if paired_by_bits(groups) else (i + step) % groups) for i in range(groups)
    ]
    return lax.ppermute(value, axis, pairs)


def inner_of(groups):
    bits = groups.bit_length() - 1
    return 1 << (bits // 2)


def row_edges_kernel(
    terms, w, y, col, listed, owners, ps, spk, wv, yv, zv, iv, ov, link, sums, sems, ysem, zsems, lsem
):
    nx, n, width = wv.shape[1:]
    ycopy = pltpu.make_async_copy(y, yv, ysem)
    ycopy.start()
    linked = pltpu.make_async_copy(terms, link, lsem)
    linked.start()
    copies = []
    for x in range(nx):
        copies.append(pltpu.make_async_copy(w.at[:, x], wv.at[:, x], sems.at[x]))
        copies[x].start()
    wz = zv.shape[1]
    rank = lax.axis_index("gz")
    loads = [
        pltpu.make_async_copy(col.at[:, pl.ds(rank * wz, wz), :], zv, zsems.at[0]),
        pltpu.make_async_copy(listed, iv, zsems.at[1]),
        pltpu.make_async_copy(owners, ov, zsems.at[2]),
    ]
    for load in loads:
        load.start()
    ycopy.wait()
    linked.wait()
    rt = yv[0].T
    it = yv[1].T
    left, right = spikes_of(
        (rt, it), (link[0, 0, 0], link[0, 0, 1]), (link[0, 1, 0], link[0, 1, 1])
    )
    for at, row in enumerate((left[0], left[1], right[0], right[1])):
        spk[at : at + 1, :] = row
    for at in range(4):
        spk[4 + at : 5 + at, :] = jnp.full((1, n), link[1, at // 2, at % 2], f32)
    lanes = ps.shape[2]
    count = width // lanes * nx
    for at, row in enumerate(edge_rows(left, right, lanes)):
        ps[0, 4 * count + at : 4 * count + at + 1, :] = row
    coef = [
        (
            jnp.broadcast_to(rt[:, row : row + 1], (n, lanes)),
            jnp.broadcast_to(it[:, row : row + 1], (n, lanes)),
        )
        for row in (0, n - 1)
    ]
    for x in range(nx):
        copies[x].wait()
        for k in range(width // lanes):
            cols = slice(k * lanes, (k + 1) * lanes)
            wr = wv[0, x, :, cols]
            wi = wv[1, x, :, cols]
            for side, (cr, ci) in enumerate(coef):
                real = cr * wr - ci * wi
                imag = cr * wi + ci * wr
                at = 2 * side * count + k * nx + x
                sums[at] = jnp.sum(real.reshape(n // 8, 8, lanes), axis=0)
                sums[at + count] = jnp.sum(imag.reshape(n // 8, 8, lanes), axis=0)
    ps[0, 0 : 4 * count, :] = jnp.sum(sums[...], axis=1)
    for load in loads:
        load.wait()


def join_kernel(*refs):
    *parts, _, out = refs
    for at, part in enumerate(parts):
        out[at] = part[0]


def route(listed, owners, place, tail):
    me = lax.axis_index("gy")
    groups, count = owners.shape
    rows = place.shape[1] // groups
    ny = place.shape[2] // 2
    ids = listed[pl.ds(me, 1), :]
    own = owners[pl.ds(me, 1), :]
    slot = slot_of(own, me, groups)
    hot = (lax.broadcasted_iota(jnp.int32, (groups, count), 0) == own).astype(f32)
    upper = (
        lax.broadcasted_iota(jnp.int32, (count, count), 0)
        < lax.broadcasted_iota(jnp.int32, (count, count), 1)
    ).astype(f32).astype(bf16)
    earlier = mm(hot.astype(bf16), upper)
    rank = jnp.sum(hot * earlier, axis=0, keepdims=True).astype(jnp.int32)
    at = lax.broadcasted_iota(jnp.int32, (groups * rows, count), 0)
    n = lax.broadcasted_iota(jnp.int32, (ny, count), 0)
    for side in range(place.shape[0]):
        total = jnp.zeros((groups * rows, ny), f32)
        for b in range(BY):
            row = rank * BY + b
            if tail is not None and side:
                row = row + jnp.where(row >= tail, 4, 0)
            here = (at == slot * rows + row).astype(f32).astype(bf16)
            there = (n == ids * BY + b).astype(f32).astype(bf16)
            total = total + mm(here, there, NT)
        place[side, :, 0:ny] = total.astype(bf16)
        place[side, :, ny : 2 * ny] = total.astype(bf16)


def solve_rows_kernel(w, y, th, tl, yh, yl):
    nx, n, wz = w.shape[1:]
    yr = y[0]
    yi = y[1]
    for part, value in ((0, (yr, -yi)), (1, (yi, yr))):
        for half in range(2):
            hi, lo = split(value[half])
            yh[part * n : (part + 1) * n, half * n : (half + 1) * n] = hi
            yl[part * n : (part + 1) * n, half * n : (half + 1) * n] = lo
    for x in range(nx):
        wx = split(w[:, x].reshape(2 * n, wz))
        hi, lo = split(mm3((yh[...], yl[...]), wx))
        rows = slice(x * n, (x + 1) * n)
        th[rows, 0:wz] = hi[0:n]
        th[rows, wz : 2 * wz] = hi[n : 2 * n]
        tl[rows, 0:wz] = lo[0:n]
        tl[rows, wz : 2 * wz] = lo[n : 2 * n]


def prepare_kernel(spk, zv, iv, ov, after, edge, zsp, zed, zh, zl, place, *, tail):
    wz = zv.shape[1]
    zr = zv[0]
    zi = zv[1]
    rt = zr.T
    it = zi.T
    put(zh, zl, slice(0, wz), slice(0, wz), rt)
    put(zh, zl, slice(0, wz), slice(wz, 2 * wz), it)
    put(zh, zl, slice(wz, 2 * wz), slice(0, wz), -it)
    put(zh, zl, slice(wz, 2 * wz), slice(wz, 2 * wz), rt)
    for at, (row, turned) in enumerate(((0, False), (0, True), (wz - 1, False), (wz - 1, True))):
        edge[at : at + 1, 0:wz] = (zi if turned else zr)[row : row + 1]
        edge[at : at + 1, wz : 2 * wz] = zr[row : row + 1] if turned else -zi[row : row + 1]
    edge[4:8, :] = jnp.zeros((4, 2 * wz), f32)
    terms = [spk[at : at + 1, 0:1] for at in range(4, 8)]
    left, right = spikes_of((rt, it), (terms[0], terms[1]), (terms[2], terms[3]))
    for at, spike in enumerate((left, right)):
        zsp[2 * at : 2 * at + 1, 0:wz] = spike[0]
        zsp[2 * at : 2 * at + 1, wz : 2 * wz] = spike[1]
        zsp[2 * at + 1 : 2 * at + 2, 0:wz] = -spike[1]
        zsp[2 * at + 1 : 2 * at + 2, wz : 2 * wz] = spike[0]
    zsp[4:8, :] = jnp.zeros((4, 2 * wz), f32)
    for at, row in enumerate(edge_rows(left, right, zed.shape[1])):
        zed[at : at + 1, :] = row
    route(iv, ov, place, tail)


def solve_columns_kernel(th, tl, zh, zl, s, base):
    n = base.shape[1]
    nx = base.shape[0] // 4
    wz = s.shape[1] // 2
    block = MBLOCK * n
    for m in range(nx // MBLOCK):
        rows = slice(m * block, (m + 1) * block)
        s[rows, :] = mm3((th[rows, :], tl[rows, :]), (zh[...], zl[...]))
    lane = lax.broadcasted_iota(jnp.int32, (n, 128), 1)
    picked = jnp.zeros((n, 128), f32)
    for at, column in enumerate((0, wz, wz - 1, 2 * wz - 1)):
        for x in range(nx):
            value = s[x * n : (x + 1) * n, column : column + 1]
            picked = jnp.where(lane == at * nx + x, value, picked)
    base[...] = picked.T[0 : 4 * nx]


def chain(gathered, nx, own, keep, index=lambda j: j):
    groups = gathered.shape[0]
    lanes = gathered.shape[2]
    zero = jnp.zeros((nx, lanes), f32)

    def read(j):
        block = gathered[index(j)]
        rows = [block[at * nx : (at + 1) * nx] for at in range(4)]
        edges = [
            jnp.broadcast_to(block[4 * nx + at : 4 * nx + at + 1], (nx, lanes))
            for at in range(EDGE)
        ]
        head, tail = (rows[0], rows[1]), (rows[2], rows[3])
        return head, tail, [(edges[2 * at], edges[2 * at + 1]) for at in range(4)]

    def forward(j, carry):
        coupling, carried = (carry[0], carry[1]), (carry[2], carry[3])
        head, tail, (lead_left, tail_left, lead_right, tail_right) = read(j)
        product = cmul(lead_left, coupling)
        pivot = (1.0 - product[0], -product[1])
        gain = cdiv(tail_left, pivot)
        for at, value in enumerate(coupling + carried + pivot):
            keep[j, at * nx : (at + 1) * nx, :] = value
        coupling_next = cadd(tail_right, cmul(gain, cmul(lead_right, coupling)))
        carried_next = cadd(
            cmul(gain, carried), cadd(tail, cmul(cmul(gain, coupling), head))
        )
        return coupling_next + carried_next

    def solved(j, head_next):
        head, _, (lead_left, _, lead_right, _) = read(j)
        kept = keep[j]
        values = [kept[at * nx : (at + 1) * nx] for at in range(6)]
        coupling, carried, pivot = (
            (values[0], values[1]),
            (values[2], values[3]),
            (values[4], values[5]),
        )
        offset = cdiv(cadd(head, cmul(lead_left, carried)), pivot)
        factor = cdiv(lead_right, pivot)
        value = cadd(offset, cmul(factor, head_next))
        return value, cadd(carried, cmul(coupling, value))

    lax.fori_loop(0, groups, forward, (zero, zero, zero, zero))
    following = lax.fori_loop(
        0,
        groups - 1 - own,
        lambda lap, head_next: solved(groups - 1 - lap, head_next)[0],
        (zero, zero),
    )
    return solved(own, following)[1], following


def row_chain_kernel(*refs):
    *parts, base, edge, zed, spk, lam, pay, keep, gathered = refs
    nx = base.shape[0] // 4
    own = lax.axis_index("gy")
    bits = len(parts) > 1
    for b, part in enumerate(parts):
        for a in range(part.shape[0]):
            gathered[a * len(parts) + b] = part[a]
    count = (gathered.shape[1] - EDGE) // 4
    sides = chain(gathered, count, own, keep, (lambda j: j ^ own) if bits else (lambda j: j))
    stacked = jnp.concatenate(
        [
            jnp.concatenate(
                [part[k : k + nx] for part in side for k in range(0, count, nx)], 1
            )
            for side in sides
        ],
        0,
    )
    lam[...] = stacked
    spikes = ((spk[0:1, :], spk[1:2, :]), (spk[2:3, :], spk[3:4, :]))
    for at in range(2):
        value = [base[(2 * at + part) * nx : (2 * at + part + 1) * nx, :] for part in range(2)]
        moved = [
            jnp.sum(stacked * edge[2 * at + part : 2 * at + part + 1, :], axis=1, keepdims=True)
            for part in range(2)
        ]
        for side in range(2):
            rows = slice(side * nx, (side + 1) * nx)
            value = cadd(value, cmul((moved[0][rows], moved[1][rows]), spikes[side]))
        pay[2 * at * nx : (2 * at + 1) * nx, :] = value[0]
        pay[(2 * at + 1) * nx : (2 * at + 2) * nx, :] = value[1]
    pay[4 * nx : 4 * nx + EDGE, :] = zed[...]


def table_kernel(listed, owners, table, phase, *rest, tail, norm):
    yt, ylast, vol, q, rank, mine = rest
    me = lax.axis_index("gy")
    groups, count = owners.shape
    rows = q.shape[0] // groups
    ny = table.shape[2]
    mine[...] = (owners[...] == me).astype(f32)
    upper = (
        lax.broadcasted_iota(jnp.int32, (count, count), 0)
        < lax.broadcasted_iota(jnp.int32, (count, count), 1)
    ).astype(f32).astype(bf16)
    rank[...] = mm(mine[...].astype(bf16), upper).astype(jnp.int32)
    at = lax.broadcasted_iota(jnp.int32, (rows, count), 0)
    n = lax.broadcasted_iota(jnp.int32, (ny, count), 0)
    order = steps_of(groups)
    for side in range(yt.shape[0]):
        for place, step in enumerate([0] + order):
            g = source_of(step, me, groups)
            own = jnp.broadcast_to(mine[pl.ds(g, 1), :], at.shape)
            total = jnp.zeros((rows, ny), f32)
            for b in range(BY):
                row = rank[pl.ds(g, 1), :] * BY + b
                if tail is not None and side:
                    row = row + jnp.where(row >= tail, 4, 0)
                here = jnp.where(at == row, own, 0.0)
                there = (n == listed[pl.ds(g, 1), :] * BY + b).astype(f32).astype(bf16)
                total = total + mm(here.astype(bf16), there, NT)
            q[place * rows : (place + 1) * rows, :] = total
        cut = (groups - late_of(groups)) * rows
        first = q[0:cut, :].astype(bf16)
        last = q[cut : groups * rows, :].astype(bf16)
        for part in range(2):
            yt[side, part] = mm(table[part], first, NT).astype(bf16)
        hi = mm(table[0], last, NT)
        lo = mm(table[1], last, NT)
        ylast[side] = jnp.concatenate([hi, hi, lo], 1).astype(bf16)
    vol[0] = jnp.cos(phase[...]) * norm
    vol[1] = jnp.sin(phase[...]) * norm


def ready_kernel(lam, zh, zl, zsp, absorber, bm, kept, moved):
    nx = lam.shape[0] // 2
    wz = lam.shape[1] // 2
    moved[...] = mm3(split(lam[...]), (zh[...], zl[...]))
    swapped = jnp.concatenate([-moved[:, wz : 2 * wz], moved[:, 0:wz]], 1)
    for x in range(nx):
        b = jnp.concatenate(
            [
                moved[x : x + 1, :],
                swapped[x : x + 1],
                moved[nx + x : nx + x + 1, :],
                swapped[nx + x : nx + x + 1],
                zsp[0:4, :],
            ],
            0,
        )
        bhi = b.astype(bf16).astype(f32)
        bm[x] = jnp.concatenate([bhi, b - bhi, bhi, jnp.zeros_like(b)], 0).astype(bf16)
        kept[x] = jnp.exp(-absorber[x])


def lost_kernel(s, spk, keep_part, bm, place, *rest, columns, groups, tail):
    parts = rest[:columns]
    am, keep, gathered = rest[-3:]
    sent = rest[columns : columns + groups]
    more = rest[columns + groups : -3]
    final = steps_of(groups)[-1]
    nx, n, wz = keep_part.shape
    own = lax.axis_index("gz")
    bits = paired_by_bits(columns)
    for step, part in enumerate(parts):
        gathered[step] = part[...]

    def index(j):
        return j ^ own if bits else (own - j + columns) % columns

    left, right = chain(gathered, nx, own, keep, index)
    for x in range(nx):
        a = jnp.concatenate(
            [spk[0:4, :]] + [v[x : x + 1] for v in (left[0], left[1], right[0], right[1])], 0
        )
        ahi = a.astype(bf16).astype(f32)
        am[x] = jnp.concatenate([ahi, ahi, a - ahi, jnp.zeros_like(a)], 0).astype(bf16)
    rows = place.shape[1] // groups
    sides = 1 if tail is None else 2
    width = rows if tail is None else 2 * tail + 8
    for step in range(nx // sides):
        parts = []
        for side in range(sides):
            x = step * sides + side
            field = s[x * n : (x + 1) * n, :] + mm(am[x], bm[x], TN)
            kept = keep_part[x]
            folded = []
            for part in range(2):
                value = field[:, part * wz : (part + 1) * wz]
                value = value - value * kept
                folded.append(sum(value[:, k * KZ : (k + 1) * KZ] for k in range(wz // KZ)))
            hi, lo = split(jnp.concatenate(folded, 1))
            parts.append(mm(place[side], jnp.concatenate([hi, lo], 0)))
        for g in range(groups):
            top = g * rows
            at = step * width
            target = sent[g]
            if g == final and at >= target.shape[0]:
                at = at - target.shape[0]
                target = more[0]
            if tail is None:
                target[at : at + rows, :] = parts[0][top : top + rows]
            else:
                target[at : at + tail, :] = parts[0][top : top + tail]
                target[at + tail : at + 2 * tail, :] = parts[1][top : top + tail]
                target[at + 2 * tail : at + 2 * tail + 8, :] = (
                    parts[0][top + tail : top + rows] + parts[1][top + tail : top + rows]
                )


def damp_kernel(s, keep_part, am, bm, damped, dv, sems):
    nx, n, wz = keep_part.shape
    copies = []
    for x in range(nx):
        field = s[x * n : (x + 1) * n, :] + mm(am[x], bm[x], TN)
        kept = keep_part[x]
        for part in range(2):
            dv[x, part] = field[:, part * wz : (part + 1) * wz] * kept
            copies.append(
                pltpu.make_async_copy(dv.at[x, part], damped.at[part, x], sems.at[x, part])
            )
            copies[-1].start()
    for copy in copies:
        copy.wait()


def plane_rows(block, x, rows, tail):
    if tail is None:
        return block[x * rows : (x + 1) * rows, :]
    at = x // 2 * (2 * tail + 8)
    side = x % 2
    return jnp.concatenate(
        [
            block[at + side * tail : at + (side + 1) * tail, :],
            block[at + 2 * tail : at + 2 * tail + 8, :],
        ],
        0,
    )


def combine(u):
    half = u.shape[0] // 2
    real = u[0:half, 0:KZ] - u[half:, KZ:]
    imag = u[0:half, KZ:] + u[half:, 0:KZ]
    return real, imag


def early_kernel(yt, ez, *rest, tail):
    count = len(rest) - 2
    got, (out, moved) = rest[:count], rest[count:]
    rows = yt.shape[3] // count
    sides = 1 if tail is None else 2
    for g in range(count):
        moved[g] = mm3(split(got[g][...]), (ez[0], ez[1]))
    for x in range(out.shape[0]):
        block = jnp.concatenate([plane_rows(moved[g], x, rows, tail) for g in range(count)], 0)
        side = x % sides
        real, imag = combine(mm3((yt[side, 0], yt[side, 1]), split(block)))
        out[x, :, 0:KZ] = real
        out[x, :, KZ:] = imag


def late_kernel(ylast, ez, early, vol, *rest, tail, first):
    out, moved, ov, sems = rest[-4:]
    sources = moved.shape[0]
    height = moved.shape[1]
    count = ov.shape[0]
    rows = ylast.shape[2] // (3 * sources)
    sides = 1 if tail is None else 2
    top = first * height // count
    for at in range(sources):
        got = rest[at]
        block = got[...] if at == sources - 1 else got[top : top + height, :]
        moved[at] = mm3(split(block), (ez[0], ez[1]))
    copies = []
    for x in range(count):
        block = [plane_rows(moved[at], x, rows, tail) for at in range(sources)]
        hi, lo = split(jnp.concatenate(block, 0))
        real, imag = combine(mm(ylast[x % sides], jnp.concatenate([hi, lo, hi], 0)))
        real = real + early[first + x, :, 0:KZ]
        imag = imag + early[first + x, :, KZ:]
        ov[x, 0] = vol[0] * real - vol[1] * imag
        ov[x, 1] = vol[0] * imag + vol[1] * real
        for part in range(2):
            copies.append(
                pltpu.make_async_copy(ov.at[x, part], out.at[part, first + x], sems.at[x, part])
            )
            copies[-1].start()
    for copy in copies:
        copy.wait()


def late_of(groups):
    return min(2, groups - 1)


def steps_of(groups):
    return list(range(1, groups))


def halves(table):
    exact = np.asarray(table, np.float64)
    hi = exact.astype(jnp.bfloat16)
    lo = (exact - hi.astype(np.float64)).astype(jnp.bfloat16)
    return np.stack([hi, lo])


def transform_tables():
    n = np.arange(KY)
    angle = 2.0 * np.pi / KY * (np.outer(n, n) % KY) - np.pi * (n % 2)[None, :]
    ytab = halves(np.concatenate([np.cos(angle), -np.sin(angle)], 0))
    n = np.arange(KZ)
    angle = 2.0 * np.pi / KZ * (np.outer(n, n) % KZ) - np.pi * (n % 2)[:, None]
    er, ei = np.cos(angle), -np.sin(angle)
    ztab = halves(np.block([[er, ei], [-ei, er]]))
    return ytab, ztab


def sds(*shape, dtype=f32):
    return jax.ShapeDtypeStruct(shape, dtype)


def body(
    wavefunction,
    absorber,
    row_inverse,
    column_inverse,
    link_terms,
    shell_blocks,
    owner_map,
    volkov_phase,
):
    nx, wy, wz = wavefunction.shape[1:]
    groups = lax.axis_size("gy")
    columns = lax.axis_size("gz")
    shell = shell_blocks.shape[2]
    capacity = 2 * ((shell + groups - 1) // groups)
    sent = capacity * BY
    paired = sent % 8 == 4 and nx % 2 == 0
    tail = sent - 4 if paired else None
    rows = (sent + 7) // 8 * 8
    sides = 2 if paired else 1
    per_plane = sent if paired else rows
    listed = shell_blocks[0]
    owners = owner_map[0, :, :, 0]
    ytab, ztab = transform_tables()
    norm = 1.0 / math.sqrt(wy * wz)

    tall = 4 * (wz // 128) * nx + EDGE
    pay, spk, wv, yv, zv, iv, ov = pl.pallas_call(
        row_edges_kernel,
        in_specs=[AN] * 6,
        out_specs=[VM] * 7,
        out_shape=[
            sds(1, tall, 128),
            sds(8, wy),
            sds(2, nx, wy, wz),
            sds(2, wy, wy),
            sds(2, wz, wz),
            sds(*listed.shape, dtype=jnp.int32),
            sds(*owners.shape, dtype=jnp.int32),
        ],
        scratch_shapes=[
            pltpu.SMEM(link_terms.shape, f32),
            pltpu.VMEM((tall - EDGE, 8, 128), f32),
            pltpu.SemaphoreType.DMA((nx,)),
            pltpu.SemaphoreType.DMA,
            pltpu.SemaphoreType.DMA((3,)),
            pltpu.SemaphoreType.DMA,
        ],
        compiler_params=LIMIT,
        name="row_edges",
    )(*far(link_terms, wavefunction, row_inverse, column_inverse, listed, owners))

    inner = inner_of(groups) if paired_by_bits(groups) else groups
    outer = groups // inner
    if paired_by_bits(groups):
        lines = [pay]
        for step in range(1, outer):
            lines.append(exchange(pay, step * inner, groups))
    else:
        lines = [lax.all_gather(pay[0], "gy")]

    th, tl = pl.pallas_call(
        solve_rows_kernel,
        in_specs=[VM] * 2,
        out_specs=[VM] * 2,
        out_shape=[sds(nx * wy, 2 * wz, dtype=bf16)] * 2,
        scratch_shapes=[pltpu.VMEM((2 * wy, 2 * wy), bf16)] * 2,
        compiler_params=LIMIT,
        name="solve_rows",
    )(wv, yv)

    first = lines[-1]
    if paired_by_bits(groups):
        joined = pl.pallas_call(
            join_kernel,
            in_specs=[VM] * outer + [AN],
            out_specs=VM,
            out_shape=sds(outer, tall, 128),
            compiler_params=LIMIT,
            name="join",
        )(*lines, th)
        gathered = [joined] + [exchange(joined, step, groups) for step in range(1, inner)]
    else:
        gathered = lines

    edge, zsp, zed, zh, zl, place = pl.pallas_call(
        lambda *refs: prepare_kernel(*refs, tail=tail),
        in_specs=[VM, VM, VM, VM, AN],
        out_specs=[VM] * 6,
        out_shape=[
            sds(8, 2 * wz),
            sds(8, 2 * wz),
            sds(EDGE, wy),
            sds(2 * wz, 2 * wz, dtype=bf16),
            sds(2 * wz, 2 * wz, dtype=bf16),
            sds(sides, groups * rows, 2 * wy, dtype=bf16),
        ],
        compiler_params=LIMIT,
        name="prepare",
    )(spk, zv, iv, ov, first)

    s, base = pl.pallas_call(
        solve_columns_kernel,
        in_specs=[VM] * 4,
        out_specs=[VM] * 2,
        out_shape=[sds(nx * wy, 2 * wz), sds(4 * nx, wy)],
        compiler_params=LIMIT,
        name="solve_columns",
    )(th, tl, zh, zl)

    lam, payz = pl.pallas_call(
        row_chain_kernel,
        in_specs=[VM] * (4 + len(gathered)),
        out_specs=[VM] * 2,
        out_shape=[sds(2 * nx, 2 * wz), sds(4 * nx + EDGE, wy)],
        scratch_shapes=[
            pltpu.VMEM((groups, 6 * (wz // 128) * nx, 128), f32),
            pltpu.VMEM((groups, tall, 128), f32),
        ],
        compiler_params=LIMIT,
        name="row_chain",
    )(*gathered, base, edge, zed, spk)

    edges = [payz]
    for step in range(1, columns):
        edges.append(exchange(payz, step, columns, "gz"))

    bm, kept = pl.pallas_call(
        ready_kernel,
        in_specs=[VM] * 5,
        out_specs=[VM] * 2,
        out_shape=[sds(nx, 32, 2 * wz, dtype=bf16), sds(nx, wy, wz)],
        scratch_shapes=[pltpu.VMEM((2 * nx, 2 * wz), f32)],
        compiler_params=LIMIT,
        name="ready",
    )(lam, zh, zl, zsp, absorber)

    height = nx * per_plane
    order = steps_of(groups)
    cuts = 2 if nx // sides % 2 == 0 else 1
    *sent, am = pl.pallas_call(
        lambda *refs: lost_kernel(*refs, columns=columns, groups=groups, tail=tail),
        in_specs=[VM] * (5 + columns),
        out_specs=[VM] * (groups + cuts),
        out_shape=[sds(height // (cuts if g == order[-1] else 1), 2 * KZ) for g in range(groups)]
        + [sds(height // cuts, 2 * KZ)] * (cuts - 1)
        + [sds(nx, 32, wy, dtype=bf16)],
        scratch_shapes=[
            pltpu.VMEM((columns, 6 * nx, wy), f32),
            pltpu.VMEM((columns, 4 * nx + EDGE, wy), f32),
        ],
        compiler_params=LIMIT,
        name="lost",
    )(s, spk, kept, bm, place, *edges)

    late = late_of(groups)
    got = [sent[0]] + [exchange(sent[step], step, groups) for step in order[:-1]]
    lasts = [exchange(part, order[-1], groups) for part in [sent[order[-1]]] + sent[groups:]]

    yt, ylast, vol = pl.pallas_call(
        lambda *refs: table_kernel(*refs, tail=tail, norm=norm),
        in_specs=[VM] * 4,
        out_specs=[VM] * 3,
        out_shape=[
            sds(sides, 2, 2 * KY, (groups - late) * rows, dtype=bf16),
            sds(sides, 2 * KY, 3 * late * rows, dtype=bf16),
            sds(2, KY, KZ),
        ],
        scratch_shapes=[
            pltpu.VMEM((groups * rows, KY), f32),
            pltpu.VMEM(owners.shape, jnp.int32),
            pltpu.VMEM(owners.shape, f32),
        ],
        compiler_params=LIMIT,
        name="tables",
    )(listed, owners, jnp.asarray(ytab), volkov_phase)

    damped = pl.pallas_call(
        damp_kernel,
        in_specs=[VM] * 4,
        out_specs=AN,
        out_shape=sds(2, nx, wy, wz),
        scratch_shapes=[
            pltpu.VMEM((nx, 2, wy, wz), f32),
            pltpu.SemaphoreType.DMA((nx, 2)),
        ],
        compiler_params=LIMIT,
        name="damp",
    )(s, kept, am, bm)

    early = pl.pallas_call(
        lambda *refs: early_kernel(*refs, tail=tail),
        in_specs=[VM] * (groups - late + 2),
        out_specs=VM,
        out_shape=sds(nx, KY, 2 * KZ),
        scratch_shapes=[pltpu.VMEM((groups - late, height, 2 * KZ), f32)],
        compiler_params=LIMIT,
        name="early",
    )(yt, jnp.asarray(ztab), *got[: groups - late])

    spectrum = []
    first = 0
    for block in lasts:
        count = block.shape[0] // per_plane
        spectrum = [
            pl.pallas_call(
                lambda *refs, first=first: late_kernel(*refs, tail=tail, first=first),
                in_specs=[VM] * (4 + late) + [AN] * len(spectrum),
                out_specs=AN,
                out_shape=sds(2, nx, KY, KZ),
                scratch_shapes=[
                    pltpu.VMEM((late, *block.shape), f32),
                    pltpu.VMEM((count, 2, KY, KZ), f32),
                    pltpu.SemaphoreType.DMA((count, 2)),
                ],
                input_output_aliases={4 + late: 0} if spectrum else {},
                compiler_params=LIMIT,
                name="late",
            )(ylast, jnp.asarray(ztab), early, vol, *got[groups - late :], block, *far(*spectrum))
        ]
        first = first + count
    (spectrum,) = spectrum
    return damped, spectrum


def solution(mesh):
    placed = (
        P(None, None, "gy", "gz"),
        P(None, "gy", "gz"),
        P(None, "gy", None),
        P(),
        P(),
        P("gz", None, None),
        P("gz", None, None, None),
        P(),
    )
    return jax.shard_map(
        body,
        mesh=mesh,
        in_specs=placed,
        out_specs=(P(None, None, "gy", "gz"), P(None, "gy", "gz", None)),
        check_vma=False,
    )
```

```python
import math

import jax
import jax.numpy as jnp
import numpy as np
from jax import lax
from jax.experimental import pallas as pl
from jax.experimental.pallas import tpu as pltpu
from jax.sharding import PartitionSpec as P


BY = 2
KY = 128
KZ = 128
EDGE = 8
MBLOCK = 4

f32 = jnp.float32
bf16 = jnp.bfloat16
NN = (((1,), (0,)), ((), ()))
NT = (((1,), (1,)), ((), ()))
TN = (((0,), (0,)), ((), ()))


def mm(a, b, dims=NN):
    return lax.dot_general(a, b, dims, preferred_element_type=f32)


def split(a):
    hi = a.astype(bf16)
    return hi, (a - hi.astype(f32)).astype(bf16)


def mm3(a, b, dims=NN):
    return mm(a[0], b[0], dims) + mm(a[0], b[1], dims) + mm(a[1], b[0], dims)


def cmul(a, b):
    return (a[0] * b[0] - a[1] * b[1], a[0] * b[1] + a[1] * b[0])


def cdiv(a, b):
    modulus = b[0] * b[0] + b[1] * b[1]
    return ((a[0] * b[0] + a[1] * b[1]) / modulus, (a[1] * b[0] - a[0] * b[1]) / modulus)


def cadd(a, b):
    return (a[0] + b[0], a[1] + b[1])


def put(hi_ref, lo_ref, rows, cols, value):
    hi, lo = split(value)
    hi_ref[rows, cols] = hi
    lo_ref[rows, cols] = lo


def spikes_of(transposed, previous, following):
    last = transposed[0].shape[0] - 1
    left = cmul(previous, (transposed[0][0:1], transposed[1][0:1]))
    right = cmul(following, (transposed[0][last : last + 1], transposed[1][last : last + 1]))
    return left, right


def edge_rows(left, right, lanes):
    last = left[0].shape[1] - 1
    rows = []
    for spike in (left, right):
        for at in (0, last):
            for part in spike:
                rows.append(jnp.broadcast_to(part[:, at : at + 1], (1, lanes)))
    return rows


VM = pl.BlockSpec(memory_space=pltpu.VMEM)
SM = pl.BlockSpec(memory_space=pltpu.SMEM)
AN = pl.BlockSpec(memory_space=pl.ANY)
LIMIT = pltpu.CompilerParams(vmem_limit_bytes=20 << 20)


def far(*values):
    return [pltpu.with_memory_space_constraint(value, pltpu.HBM) for value in values]


def paired_by_bits(groups):
    return groups & (groups - 1) == 0


def slot_of(owner, me, groups):
    return owner ^ me if paired_by_bits(groups) else (owner - me + groups) % groups


def source_of(step, me, groups):
    return me ^ step if paired_by_bits(groups) else (me - step + groups) % groups


def exchange(value, step, groups, axis="gy"):
    pairs = [
        (i, i ^ step if paired_by_bits(groups) else (i + step) % groups) for i in range(groups)
    ]
    return lax.ppermute(value, axis, pairs)


def inner_of(groups):
    bits = groups.bit_length() - 1
    return 1 << (bits // 2)


def row_edges_kernel(
    terms, w, y, col, listed, owners, ps, spk, wv, yv, zv, iv, ov, link, sums, sems, ysem, zsems, lsem
):
    nx, n, width = wv.shape[1:]
    ycopy = pltpu.make_async_copy(y, yv, ysem)
    ycopy.start()
    linked = pltpu.make_async_copy(terms, link, lsem)
    linked.start()
    copies = []
    for x in range(nx):
        copies.append(pltpu.make_async_copy(w.at[:, x], wv.at[:, x], sems.at[x]))
        copies[x].start()
    wz = zv.shape[1]
    rank = lax.axis_index("gz")
    loads = [
        pltpu.make_async_copy(col.at[:, pl.ds(rank * wz, wz), :], zv, zsems.at[0]),
        pltpu.make_async_copy(listed, iv, zsems.at[1]),
        pltpu.make_async_copy(owners, ov, zsems.at[2]),
    ]
    for load in loads:
        load.start()
    ycopy.wait()
    linked.wait()
    rt = yv[0].T
    it = yv[1].T
    left, right = spikes_of(
        (rt, it), (link[0, 0, 0], link[0, 0, 1]), (link[0, 1, 0], link[0, 1, 1])
    )
    for at, row in enumerate((left[0], left[1], right[0], right[1])):
        spk[at : at + 1, :] = row
    for at in range(4):
        spk[4 + at : 5 + at, :] = jnp.full((1, n), link[1, at // 2, at % 2], f32)
    lanes = ps.shape[2]
    count = width // lanes * nx
    for at, row in enumerate(edge_rows(left, right, lanes)):
        ps[0, 4 * count + at : 4 * count + at + 1, :] = row
    coef = [
        (
            jnp.broadcast_to(rt[:, row : row + 1], (n, lanes)),
            jnp.broadcast_to(it[:, row : row + 1], (n, lanes)),
        )
        for row in (0, n - 1)
    ]
    for x in range(nx):
        copies[x].wait()
        for k in range(width // lanes):
            cols = slice(k * lanes, (k + 1) * lanes)
            wr = wv[0, x, :, cols]
            wi = wv[1, x, :, cols]
            for side, (cr, ci) in enumerate(coef):
                real = cr * wr - ci * wi
                imag = cr * wi + ci * wr
                at = 2 * side * count + k * nx + x
                sums[at] = jnp.sum(real.reshape(n // 8, 8, lanes), axis=0)
                sums[at + count] = jnp.sum(imag.reshape(n // 8, 8, lanes), axis=0)
    ps[0, 0 : 4 * count, :] = jnp.sum(sums[...], axis=1)
    for load in loads:
        load.wait()


def join_kernel(*refs):
    *parts, _, out = refs
    for at, part in enumerate(parts):
        out[at] = part[0]


def route(listed, owners, place, tail):
    me = lax.axis_index("gy")
    groups, count = owners.shape
    rows = place.shape[1] // groups
    ny = place.shape[2] // 2
    ids = listed[pl.ds(me, 1), :]
    own = owners[pl.ds(me, 1), :]
    slot = slot_of(own, me, groups)
    hot = (lax.broadcasted_iota(jnp.int32, (groups, count), 0) == own).astype(f32)
    upper = (
        lax.broadcasted_iota(jnp.int32, (count, count), 0)
        < lax.broadcasted_iota(jnp.int32, (count, count), 1)
    ).astype(f32).astype(bf16)
    earlier = mm(hot.astype(bf16), upper)
    rank = jnp.sum(hot * earlier, axis=0, keepdims=True).astype(jnp.int32)
    at = lax.broadcasted_iota(jnp.int32, (groups * rows, count), 0)
    n = lax.broadcasted_iota(jnp.int32, (ny, count), 0)
    for side in range(place.shape[0]):
        total = jnp.zeros((groups * rows, ny), f32)
        for b in range(BY):
            row = rank * BY + b
            if tail is not None and side:
                row = row + jnp.where(row >= tail, 4, 0)
            here = (at == slot * rows + row).astype(f32).astype(bf16)
            there = (n == ids * BY + b).astype(f32).astype(bf16)
            total = total + mm(here, there, NT)
        place[side, :, 0:ny] = total.astype(bf16)
        place[side, :, ny : 2 * ny] = total.astype(bf16)


def solve_rows_kernel(w, y, th, tl, yh, yl):
    nx, n, wz = w.shape[1:]
    yr = y[0]
    yi = y[1]
    for part, value in ((0, (yr, -yi)), (1, (yi, yr))):
        for half in range(2):
            hi, lo = split(value[half])
            yh[part * n : (part + 1) * n, half * n : (half + 1) * n] = hi
            yl[part * n : (part + 1) * n, half * n : (half + 1) * n] = lo
    for x in range(nx):
        wx = split(w[:, x].reshape(2 * n, wz))
        hi, lo = split(mm3((yh[...], yl[...]), wx))
        rows = slice(x * n, (x + 1) * n)
        th[rows, 0:wz] = hi[0:n]
        th[rows, wz : 2 * wz] = hi[n : 2 * n]
        tl[rows, 0:wz] = lo[0:n]
        tl[rows, wz : 2 * wz] = lo[n : 2 * n]


def prepare_kernel(spk, zv, iv, ov, after, edge, zsp, zed, zh, zl, place, *, tail):
    wz = zv.shape[1]
    zr = zv[0]
    zi = zv[1]
    rt = zr.T
    it = zi.T
    put(zh, zl, slice(0, wz), slice(0, wz), rt)
    put(zh, zl, slice(0, wz), slice(wz, 2 * wz), it)
    put(zh, zl, slice(wz, 2 * wz), slice(0, wz), -it)
    put(zh, zl, slice(wz, 2 * wz), slice(wz, 2 * wz), rt)
    for at, (row, turned) in enumerate(((0, False), (0, True), (wz - 1, False), (wz - 1, True))):
        edge[at : at + 1, 0:wz] = (zi if turned else zr)[row : row + 1]
        edge[at : at + 1, wz : 2 * wz] = zr[row : row + 1] if turned else -zi[row : row + 1]
    edge[4:8, :] = jnp.zeros((4, 2 * wz), f32)
    terms = [spk[at : at + 1, 0:1] for at in range(4, 8)]
    left, right = spikes_of((rt, it), (terms[0], terms[1]), (terms[2], terms[3]))
    for at, spike in enumerate((left, right)):
        zsp[2 * at : 2 * at + 1, 0:wz] = spike[0]
        zsp[2 * at : 2 * at + 1, wz : 2 * wz] = spike[1]
        zsp[2 * at + 1 : 2 * at + 2, 0:wz] = -spike[1]
        zsp[2 * at + 1 : 2 * at + 2, wz : 2 * wz] = spike[0]
    zsp[4:8, :] = jnp.zeros((4, 2 * wz), f32)
    for at, row in enumerate(edge_rows(left, right, zed.shape[1])):
        zed[at : at + 1, :] = row
    route(iv, ov, place, tail)


def solve_columns_kernel(th, tl, zh, zl, s, base):
    n = base.shape[1]
    nx = base.shape[0] // 4
    wz = s.shape[1] // 2
    block = MBLOCK * n
    for m in range(nx // MBLOCK):
        rows = slice(m * block, (m + 1) * block)
        s[rows, :] = mm3((th[rows, :], tl[rows, :]), (zh[...], zl[...]))
    lane = lax.broadcasted_iota(jnp.int32, (n, 128), 1)
    picked = jnp.zeros((n, 128), f32)
    for at, column in enumerate((0, wz, wz - 1, 2 * wz - 1)):
        for x in range(nx):
            value = s[x * n : (x + 1) * n, column : column + 1]
            picked = jnp.where(lane == at * nx + x, value, picked)
    base[...] = picked.T[0 : 4 * nx]


def chain(gathered, nx, own, keep, index=lambda j: j):
    groups = gathered.shape[0]
    lanes = gathered.shape[2]
    zero = jnp.zeros((nx, lanes), f32)

    def read(j):
        block = gathered[index(j)]
        rows = [block[at * nx : (at + 1) * nx] for at in range(4)]
        edges = [
            jnp.broadcast_to(block[4 * nx + at : 4 * nx + at + 1], (nx, lanes))
            for at in range(EDGE)
        ]
        head, tail = (rows[0], rows[1]), (rows[2], rows[3])
        return head, tail, [(edges[2 * at], edges[2 * at + 1]) for at in range(4)]

    def forward(j, carry):
        coupling, carried = (carry[0], carry[1]), (carry[2], carry[3])
        head, tail, (lead_left, tail_left, lead_right, tail_right) = read(j)
        product = cmul(lead_left, coupling)
        pivot = (1.0 - product[0], -product[1])
        gain = cdiv(tail_left, pivot)
        for at, value in enumerate(coupling + carried + pivot):
            keep[j, at * nx : (at + 1) * nx, :] = value
        coupling_next = cadd(tail_right, cmul(gain, cmul(lead_right, coupling)))
        carried_next = cadd(
            cmul(gain, carried), cadd(tail, cmul(cmul(gain, coupling), head))
        )
        return coupling_next + carried_next

    def solved(j, head_next):
        head, _, (lead_left, _, lead_right, _) = read(j)
        kept = keep[j]
        values = [kept[at * nx : (at + 1) * nx] for at in range(6)]
        coupling, carried, pivot = (
            (values[0], values[1]),
            (values[2], values[3]),
            (values[4], values[5]),
        )
        offset = cdiv(cadd(head, cmul(lead_left, carried)), pivot)
        factor = cdiv(lead_right, pivot)
        value = cadd(offset, cmul(factor, head_next))
        return value, cadd(carried, cmul(coupling, value))

    lax.fori_loop(0, groups, forward, (zero, zero, zero, zero))
    following = lax.fori_loop(
        0,
        groups - 1 - own,
        lambda lap, head_next: solved(groups - 1 - lap, head_next)[0],
        (zero, zero),
    )
    return solved(own, following)[1], following


def row_chain_kernel(*refs):
    *parts, base, edge, zed, spk, lam, pay, keep, gathered = refs
    nx = base.shape[0] // 4
    own = lax.axis_index("gy")
    bits = len(parts) > 1
    for b, part in enumerate(parts):
        for a in range(part.shape[0]):
            gathered[a * len(parts) + b] = part[a]
    count = (gathered.shape[1] - EDGE) // 4
    sides = chain(gathered, count, own, keep, (lambda j: j ^ own) if bits else (lambda j: j))
    stacked = jnp.concatenate(
        [
            jnp.concatenate(
                [part[k : k + nx] for part in side for k in range(0, count, nx)], 1
            )
            for side in sides
        ],
        0,
    )
    lam[...] = stacked
    spikes = ((spk[0:1, :], spk[1:2, :]), (spk[2:3, :], spk[3:4, :]))
    for at in range(2):
        value = [base[(2 * at + part) * nx : (2 * at + part + 1) * nx, :] for part in range(2)]
        moved = [
            jnp.sum(stacked * edge[2 * at + part : 2 * at + part + 1, :], axis=1, keepdims=True)
            for part in range(2)
        ]
        for side in range(2):
            rows = slice(side * nx, (side + 1) * nx)
            value = cadd(value, cmul((moved[0][rows], moved[1][rows]), spikes[side]))
        pay[2 * at * nx : (2 * at + 1) * nx, :] = value[0]
        pay[(2 * at + 1) * nx : (2 * at + 2) * nx, :] = value[1]
    pay[4 * nx : 4 * nx + EDGE, :] = zed[...]


def table_kernel(listed, owners, table, phase, *rest, tail, norm):
    yt, ylast, vol, q, rank, mine = rest
    me = lax.axis_index("gy")
    groups, count = owners.shape
    rows = q.shape[0] // groups
    ny = table.shape[2]
    mine[...] = (owners[...] == me).astype(f32)
    upper = (
        lax.broadcasted_iota(jnp.int32, (count, count), 0)
        < lax.broadcasted_iota(jnp.int32, (count, count), 1)
    ).astype(f32).astype(bf16)
    rank[...] = mm(mine[...].astype(bf16), upper).astype(jnp.int32)
    at = lax.broadcasted_iota(jnp.int32, (rows, count), 0)
    n = lax.broadcasted_iota(jnp.int32, (ny, count), 0)
    order = steps_of(groups)
    for side in range(yt.shape[0]):
        for place, step in enumerate([0] + order):
            g = source_of(step, me, groups)
            own = jnp.broadcast_to(mine[pl.ds(g, 1), :], at.shape)
            total = jnp.zeros((rows, ny), f32)
            for b in range(BY):
                row = rank[pl.ds(g, 1), :] * BY + b
                if tail is not None and side:
                    row = row + jnp.where(row >= tail, 4, 0)
                here = jnp.where(at == row, own, 0.0)
                there = (n == listed[pl.ds(g, 1), :] * BY + b).astype(f32).astype(bf16)
                total = total + mm(here.astype(bf16), there, NT)
            q[place * rows : (place + 1) * rows, :] = total
        cut = (groups - late_of()) * rows
        first = q[0:cut, :].astype(bf16)
        last = q[cut : groups * rows, :].astype(bf16)
        for part in range(2):
            yt[side, part] = mm(table[part], first, NT).astype(bf16)
        hi = mm(table[0], last, NT)
        lo = mm(table[1], last, NT)
        ylast[side] = jnp.concatenate([hi, hi, lo], 1).astype(bf16)
    vol[0] = jnp.cos(phase[...]) * norm
    vol[1] = jnp.sin(phase[...]) * norm


def ready_kernel(lam, zh, zl, zsp, absorber, bm, kept, moved):
    nx = lam.shape[0] // 2
    wz = lam.shape[1] // 2
    moved[...] = mm3(split(lam[...]), (zh[...], zl[...]))
    swapped = jnp.concatenate([-moved[:, wz : 2 * wz], moved[:, 0:wz]], 1)
    for x in range(nx):
        b = jnp.concatenate(
            [
                moved[x : x + 1, :],
                swapped[x : x + 1],
                moved[nx + x : nx + x + 1, :],
                swapped[nx + x : nx + x + 1],
                zsp[0:4, :],
            ],
            0,
        )
        bhi = b.astype(bf16).astype(f32)
        bm[x] = jnp.concatenate([bhi, b - bhi, bhi, jnp.zeros_like(b)], 0).astype(bf16)
        kept[x] = jnp.exp(-absorber[x])


def lost_kernel(s, spk, keep_part, bm, place, *rest, columns, groups, tail):
    parts = rest[:columns]
    am, keep, gathered = rest[-3:]
    sent = rest[columns : columns + groups]
    more = rest[columns + groups : -3]
    final = steps_of(groups)[-1]
    nx, n, wz = keep_part.shape
    own = lax.axis_index("gz")
    bits = paired_by_bits(columns)
    for step, part in enumerate(parts):
        gathered[step] = part[...]

    def index(j):
        return j ^ own if bits else (own - j + columns) % columns

    left, right = chain(gathered, nx, own, keep, index)
    for x in range(nx):
        a = jnp.concatenate(
            [spk[0:4, :]] + [v[x : x + 1] for v in (left[0], left[1], right[0], right[1])], 0
        )
        ahi = a.astype(bf16).astype(f32)
        am[x] = jnp.concatenate([ahi, ahi, a - ahi, jnp.zeros_like(a)], 0).astype(bf16)
    rows = place.shape[1] // groups
    sides = 1 if tail is None else 2
    width = rows if tail is None else 2 * tail + 8
    for step in range(nx // sides):
        parts = []
        for side in range(sides):
            x = step * sides + side
            field = s[x * n : (x + 1) * n, :] + mm(am[x], bm[x], TN)
            kept = keep_part[x]
            folded = []
            for part in range(2):
                value = field[:, part * wz : (part + 1) * wz]
                value = value - value * kept
                folded.append(sum(value[:, k * KZ : (k + 1) * KZ] for k in range(wz // KZ)))
            hi, lo = split(jnp.concatenate(folded, 1))
            parts.append(mm(place[side], jnp.concatenate([hi, lo], 0)))
        for g in range(groups):
            top = g * rows
            at = step * width
            target = sent[g]
            if g == final and at >= target.shape[0]:
                at = at - target.shape[0]
                target = more[0]
            if tail is None:
                target[at : at + rows, :] = parts[0][top : top + rows]
            else:
                target[at : at + tail, :] = parts[0][top : top + tail]
                target[at + tail : at + 2 * tail, :] = parts[1][top : top + tail]
                target[at + 2 * tail : at + 2 * tail + 8, :] = (
                    parts[0][top + tail : top + rows] + parts[1][top + tail : top + rows]
                )


def damp_kernel(s, keep_part, am, bm, damped, dv, sems):
    nx, n, wz = keep_part.shape
    copies = []
    for x in range(nx):
        field = s[x * n : (x + 1) * n, :] + mm(am[x], bm[x], TN)
        kept = keep_part[x]
        for part in range(2):
            dv[x, part] = field[:, part * wz : (part + 1) * wz] * kept
            copies.append(
                pltpu.make_async_copy(dv.at[x, part], damped.at[part, x], sems.at[x, part])
            )
            copies[-1].start()
    for copy in copies:
        copy.wait()


def plane_rows(block, x, rows, tail):
    if tail is None:
        return block[x * rows : (x + 1) * rows, :]
    at = x // 2 * (2 * tail + 8)
    side = x % 2
    return jnp.concatenate(
        [
            block[at + side * tail : at + (side + 1) * tail, :],
            block[at + 2 * tail : at + 2 * tail + 8, :],
        ],
        0,
    )


def combine(u):
    half = u.shape[0] // 2
    real = u[0:half, 0:KZ] - u[half:, KZ:]
    imag = u[0:half, KZ:] + u[half:, 0:KZ]
    return real, imag


def early_kernel(yt, ez, *rest, tail):
    count = len(rest) - 2
    got, (out, moved) = rest[:count], rest[count:]
    rows = yt.shape[3] // count
    sides = 1 if tail is None else 2
    for g in range(count):
        moved[g] = mm3(split(got[g][...]), (ez[0], ez[1]))
    for x in range(out.shape[0]):
        block = jnp.concatenate([plane_rows(moved[g], x, rows, tail) for g in range(count)], 0)
        side = x % sides
        real, imag = combine(mm3((yt[side, 0], yt[side, 1]), split(block)))
        out[x, :, 0:KZ] = real
        out[x, :, KZ:] = imag


def late_kernel(ylast, ez, early, vol, *rest, tail, first):
    out, moved, ov, sems = rest[-4:]
    sources = moved.shape[0]
    height = moved.shape[1]
    count = ov.shape[0]
    rows = ylast.shape[2] // (3 * sources)
    sides = 1 if tail is None else 2
    top = first * height // count
    for at in range(sources):
        got = rest[at]
        block = got[...] if at == sources - 1 else got[top : top + height, :]
        moved[at] = mm3(split(block), (ez[0], ez[1]))
    copies = []
    for x in range(count):
        block = [plane_rows(moved[at], x, rows, tail) for at in range(sources)]
        hi, lo = split(jnp.concatenate(block, 0))
        real, imag = combine(mm(ylast[x % sides], jnp.concatenate([hi, lo, hi], 0)))
        real = real + early[first + x, :, 0:KZ]
        imag = imag + early[first + x, :, KZ:]
        ov[x, 0] = vol[0] * real - vol[1] * imag
        ov[x, 1] = vol[0] * imag + vol[1] * real
        for part in range(2):
            copies.append(
                pltpu.make_async_copy(ov.at[x, part], out.at[part, first + x], sems.at[x, part])
            )
            copies[-1].start()
    for copy in copies:
        copy.wait()


def late_of():
    return 1


def steps_of(groups):
    return list(range(1, groups))


def halves(table):
    exact = np.asarray(table, np.float64)
    hi = exact.astype(jnp.bfloat16)
    lo = (exact - hi.astype(np.float64)).astype(jnp.bfloat16)
    return np.stack([hi, lo])


def transform_tables():
    n = np.arange(KY)
    angle = 2.0 * np.pi / KY * (np.outer(n, n) % KY) - np.pi * (n % 2)[None, :]
    ytab = halves(np.concatenate([np.cos(angle), -np.sin(angle)], 0))
    n = np.arange(KZ)
    angle = 2.0 * np.pi / KZ * (np.outer(n, n) % KZ) - np.pi * (n % 2)[:, None]
    er, ei = np.cos(angle), -np.sin(angle)
    ztab = halves(np.block([[er, ei], [-ei, er]]))
    return ytab, ztab


def sds(*shape, dtype=f32):
    return jax.ShapeDtypeStruct(shape, dtype)


def body(
    wavefunction,
    absorber,
    row_inverse,
    column_inverse,
    link_terms,
    shell_blocks,
    owner_map,
    volkov_phase,
):
    nx, wy, wz = wavefunction.shape[1:]
    groups = lax.axis_size("gy")
    columns = lax.axis_size("gz")
    shell = shell_blocks.shape[2]
    capacity = 2 * ((shell + groups - 1) // groups)
    sent = capacity * BY
    paired = sent % 8 == 4 and nx % 2 == 0
    tail = sent - 4 if paired else None
    rows = (sent + 7) // 8 * 8
    sides = 2 if paired else 1
    per_plane = sent if paired else rows
    listed = shell_blocks[0]
    owners = owner_map[0, :, :, 0]
    ytab, ztab = transform_tables()
    norm = 1.0 / math.sqrt(wy * wz)

    tall = 4 * (wz // 128) * nx + EDGE
    pay, spk, wv, yv, zv, iv, ov = pl.pallas_call(
        row_edges_kernel,
        in_specs=[AN] * 6,
        out_specs=[VM] * 7,
        out_shape=[
            sds(1, tall, 128),
            sds(8, wy),
            sds(2, nx, wy, wz),
            sds(2, wy, wy),
            sds(2, wz, wz),
            sds(*listed.shape, dtype=jnp.int32),
            sds(*owners.shape, dtype=jnp.int32),
        ],
        scratch_shapes=[
            pltpu.SMEM(link_terms.shape, f32),
            pltpu.VMEM((tall - EDGE, 8, 128), f32),
            pltpu.SemaphoreType.DMA((nx,)),
            pltpu.SemaphoreType.DMA,
            pltpu.SemaphoreType.DMA((3,)),
            pltpu.SemaphoreType.DMA,
        ],
        compiler_params=LIMIT,
        name="row_edges",
    )(*far(link_terms, wavefunction, row_inverse, column_inverse, listed, owners))

    inner = inner_of(groups) if paired_by_bits(groups) else groups
    outer = groups // inner
    if paired_by_bits(groups):
        lines = [pay]
        for step in range(1, outer):
            lines.append(exchange(pay, step * inner, groups))
    else:
        lines = [lax.all_gather(pay[0], "gy")]

    th, tl = pl.pallas_call(
        solve_rows_kernel,
        in_specs=[VM] * 2,
        out_specs=[VM] * 2,
        out_shape=[sds(nx * wy, 2 * wz, dtype=bf16)] * 2,
        scratch_shapes=[pltpu.VMEM((2 * wy, 2 * wy), bf16)] * 2,
        compiler_params=LIMIT,
        name="solve_rows",
    )(wv, yv)

    first = lines[-1]
    if paired_by_bits(groups):
        joined = pl.pallas_call(
            join_kernel,
            in_specs=[VM] * outer + [AN],
            out_specs=VM,
            out_shape=sds(outer, tall, 128),
            compiler_params=LIMIT,
            name="join",
        )(*lines, th)
        gathered = [joined] + [exchange(joined, step, groups) for step in range(1, inner)]
    else:
        gathered = lines

    edge, zsp, zed, zh, zl, place = pl.pallas_call(
        lambda *refs: prepare_kernel(*refs, tail=tail),
        in_specs=[VM, VM, VM, VM, AN],
        out_specs=[VM] * 6,
        out_shape=[
            sds(8, 2 * wz),
            sds(8, 2 * wz),
            sds(EDGE, wy),
            sds(2 * wz, 2 * wz, dtype=bf16),
            sds(2 * wz, 2 * wz, dtype=bf16),
            sds(sides, groups * rows, 2 * wy, dtype=bf16),
        ],
        compiler_params=LIMIT,
        name="prepare",
    )(spk, zv, iv, ov, first)

    s, base = pl.pallas_call(
        solve_columns_kernel,
        in_specs=[VM] * 4,
        out_specs=[VM] * 2,
        out_shape=[sds(nx * wy, 2 * wz), sds(4 * nx, wy)],
        compiler_params=LIMIT,
        name="solve_columns",
    )(th, tl, zh, zl)

    lam, payz = pl.pallas_call(
        row_chain_kernel,
        in_specs=[VM] * (4 + len(gathered)),
        out_specs=[VM] * 2,
        out_shape=[sds(2 * nx, 2 * wz), sds(4 * nx + EDGE, wy)],
        scratch_shapes=[
            pltpu.VMEM((groups, 6 * (wz // 128) * nx, 128), f32),
            pltpu.VMEM((groups, tall, 128), f32),
        ],
        compiler_params=LIMIT,
        name="row_chain",
    )(*gathered, base, edge, zed, spk)

    edges = [payz]
    for step in range(1, columns):
        edges.append(exchange(payz, step, columns, "gz"))

    bm, kept = pl.pallas_call(
        ready_kernel,
        in_specs=[VM] * 5,
        out_specs=[VM] * 2,
        out_shape=[sds(nx, 32, 2 * wz, dtype=bf16), sds(nx, wy, wz)],
        scratch_shapes=[pltpu.VMEM((2 * nx, 2 * wz), f32)],
        compiler_params=LIMIT,
        name="ready",
    )(lam, zh, zl, zsp, absorber)

    height = nx * per_plane
    order = steps_of(groups)
    cuts = 2 if nx // sides % 2 == 0 else 1
    *sent, am = pl.pallas_call(
        lambda *refs: lost_kernel(*refs, columns=columns, groups=groups, tail=tail),
        in_specs=[VM] * (5 + columns),
        out_specs=[VM] * (groups + cuts),
        out_shape=[sds(height // (cuts if g == order[-1] else 1), 2 * KZ) for g in range(groups)]
        + [sds(height // cuts, 2 * KZ)] * (cuts - 1)
        + [sds(nx, 32, wy, dtype=bf16)],
        scratch_shapes=[
            pltpu.VMEM((columns, 6 * nx, wy), f32),
            pltpu.VMEM((columns, 4 * nx + EDGE, wy), f32),
        ],
        compiler_params=LIMIT,
        name="lost",
    )(s, spk, kept, bm, place, *edges)

    late = late_of()
    got = [sent[0]] + [exchange(sent[step], step, groups) for step in order[:-1]]
    lasts = [exchange(part, order[-1], groups) for part in [sent[order[-1]]] + sent[groups:]]

    yt, ylast, vol = pl.pallas_call(
        lambda *refs: table_kernel(*refs, tail=tail, norm=norm),
        in_specs=[VM] * 4,
        out_specs=[VM] * 3,
        out_shape=[
            sds(sides, 2, 2 * KY, (groups - late) * rows, dtype=bf16),
            sds(sides, 2 * KY, 3 * late * rows, dtype=bf16),
            sds(2, KY, KZ),
        ],
        scratch_shapes=[
            pltpu.VMEM((groups * rows, KY), f32),
            pltpu.VMEM(owners.shape, jnp.int32),
            pltpu.VMEM(owners.shape, f32),
        ],
        compiler_params=LIMIT,
        name="tables",
    )(listed, owners, jnp.asarray(ytab), volkov_phase)

    damped = pl.pallas_call(
        damp_kernel,
        in_specs=[VM] * 4,
        out_specs=AN,
        out_shape=sds(2, nx, wy, wz),
        scratch_shapes=[
            pltpu.VMEM((nx, 2, wy, wz), f32),
            pltpu.SemaphoreType.DMA((nx, 2)),
        ],
        compiler_params=LIMIT,
        name="damp",
    )(s, kept, am, bm)

    early = pl.pallas_call(
        lambda *refs: early_kernel(*refs, tail=tail),
        in_specs=[VM] * (groups - late + 2),
        out_specs=VM,
        out_shape=sds(nx, KY, 2 * KZ),
        scratch_shapes=[pltpu.VMEM((groups - late, height, 2 * KZ), f32)],
        compiler_params=LIMIT,
        name="early",
    )(yt, jnp.asarray(ztab), *got[: groups - late])

    spectrum = []
    first = 0
    for block in lasts:
        count = block.shape[0] // per_plane
        spectrum = [
            pl.pallas_call(
                lambda *refs, first=first: late_kernel(*refs, tail=tail, first=first),
                in_specs=[VM] * (4 + late) + [AN] * len(spectrum),
                out_specs=AN,
                out_shape=sds(2, nx, KY, KZ),
                scratch_shapes=[
                    pltpu.VMEM((late, *block.shape), f32),
                    pltpu.VMEM((count, 2, KY, KZ), f32),
                    pltpu.SemaphoreType.DMA((count, 2)),
                ],
                input_output_aliases={4 + late: 0} if spectrum else {},
                compiler_params=LIMIT,
                name="late",
            )(ylast, jnp.asarray(ztab), early, vol, *got[groups - late :], block, *far(*spectrum))
        ]
        first = first + count
    (spectrum,) = spectrum
    return damped, spectrum


def solution(mesh):
    placed = (
        P(None, None, "gy", "gz"),
        P(None, "gy", "gz"),
        P(None, "gy", None),
        P(),
        P(),
        P("gz", None, None),
        P("gz", None, None, None),
        P(),
    )
    return jax.shard_map(
        body,
        mesh=mesh,
        in_specs=placed,
        out_specs=(P(None, None, "gy", "gz"), P(None, "gy", "gz", None)),
        check_vma=False,
    )
```
